128 devices in a mesh: tp: 4 (over x), dp: 32 (over z, y, core).
Axes of the slice: x: 4, y: 4, z: 4, core: 2. Of those that a mesh axis runs over, the one named last changes fastest.
Arguments:
- hidden: bfloat16 [2048, 896], P('dp')
- norm_w: bfloat16 [896], replicated
- emb_table: bfloat16 [151936, 896], P('tp')
- teacher: bfloat16 [2048, 151936], P('dp', 'tp')
- loss_mask: int32 [2048], P('dp')
Outputs:
- output 1: float32 [], replicated
- output 2: bfloat16 [2048, 896], P('dp')
- output 3: float32 [151936, 896], P('tp', 'dp')
- output 4: float32 [896], replicated
All inputs are finite; a program needn't handle non-finite values.
Results may differ from the reference program's by a relative error of at most 0.001.
Values sent between devices are 32-bit elements.
A program may use at most 1 GiB of HBM per device.

```python
import jax
import jax.numpy as jnp
from jax import lax

MODEL_DIM = 896
VOCAB_SIZE = 151936
TOK_DEV = 64
DP_SHARDS = 32
TOKENS = TOK_DEV * DP_SHARDS
SOFT_CAP = 30.0
NORM_EPS = 1e-6


def setup_inputs(seed: int = 0) -> dict:
    base_key = jax.random.key(seed)
    key_list = jax.random.split(base_key, 6)
    hidden = jax.random.normal(key_list[0], (TOKENS, MODEL_DIM), jnp.float32)
    norm_w = 0.5 * jax.random.normal(key_list[1], (MODEL_DIM,), jnp.float32)
    mean_dir = jax.random.normal(key_list[2], (MODEL_DIM,), jnp.float32)
    emb_noise = jax.random.normal(key_list[3], (VOCAB_SIZE, MODEL_DIM), jnp.float32)
    emb_table = (18.0 * mean_dir[None, :] + 1.5 * emb_noise) * (MODEL_DIM ** -0.5)
    teacher = 2.0 * jax.random.normal(key_list[4], (TOKENS, VOCAB_SIZE), jnp.float32)
    lengths = jax.random.randint(key_list[5], (DP_SHARDS,), 1, TOK_DEV + 1)
    lengths = jnp.where(jnp.arange(DP_SHARDS) == 0, TOK_DEV, lengths)
    loss_mask = (jnp.arange(TOK_DEV)[None, :] < lengths[:, None]).astype(jnp.int32)
    return {'hidden': hidden.astype(jnp.bfloat16), 'norm_w': norm_w.astype(jnp.bfloat16), 'emb_table': emb_table.astype(jnp.bfloat16), 'teacher': teacher.astype(jnp.bfloat16), 'loss_mask': loss_mask.reshape(TOKENS)}


def rms_norm(hid_f32, scale_f32):
    inv_rms = lax.rsqrt(jnp.mean(hid_f32 * hid_f32, axis=-1, keepdims=True) + NORM_EPS)
    return hid_f32 * inv_rms * (1.0 + scale_f32)


def reference(hidden, norm_w, emb_table, teacher, loss_mask):
    mask_f32 = loss_mask.astype(jnp.float32)
    weights = mask_f32 / jnp.sum(mask_f32)
    scale_f32 = norm_w.astype(jnp.float32)

    def block_step(acc_state, blk_inputs):
        emb_acc, scale_acc = acc_state
        hid_blk, teach_blk, weight_blk = blk_inputs
        normed_f32, norm_pull = jax.vjp(rms_norm, hid_blk.astype(jnp.float32), scale_f32)
        normed = normed_f32.astype(jnp.bfloat16)
        raw_logit = jnp.dot(normed, emb_table.T, preferred_element_type=jnp.float32)
        tanh_val = jnp.tanh(raw_logit / SOFT_CAP)
        capped = SOFT_CAP * tanh_val
        log_stu = jax.nn.log_softmax(capped, axis=-1)
        log_tea = jax.nn.log_softmax(teach_blk.astype(jnp.float32), axis=-1)
        prob_tea = jnp.exp(log_tea)
        kl_tok = jnp.sum(prob_tea * (log_tea - log_stu), axis=-1)
        loss_part = jnp.sum(weight_blk * kl_tok)
        d_raw = ((jnp.exp(log_stu) - prob_tea) * weight_blk[:, None] * (1.0 - tanh_val * tanh_val)).astype(jnp.bfloat16)
        grad_normed = jnp.dot(d_raw, emb_table, preferred_element_type=jnp.float32)
        emb_acc = emb_acc + jnp.dot(d_raw.T, normed, preferred_element_type=jnp.float32)
        grad_hid, grad_scale = norm_pull(grad_normed)
        return (emb_acc, scale_acc + grad_scale), (loss_part, grad_hid.astype(jnp.bfloat16))

    blocks_in = (hidden.reshape(DP_SHARDS, TOK_DEV, MODEL_DIM), teacher.reshape(DP_SHARDS, TOK_DEV, VOCAB_SIZE), weights.reshape(DP_SHARDS, TOK_DEV))
    start_acc = (jnp.zeros((VOCAB_SIZE, MODEL_DIM), jnp.float32), jnp.zeros((MODEL_DIM,), jnp.float32))
    final_acc, per_block = lax.scan(block_step, start_acc, blocks_in)
    d_emb, d_norm_w = final_acc
    loss_parts, grad_hid = per_block
    return jnp.sum(loss_parts), grad_hid.reshape(TOKENS, MODEL_DIM), d_emb, d_norm_w
```

```python
import jax
import jax.numpy as jnp
from jax import lax
from jax.sharding import PartitionSpec as P

SOFT_CAP = 30.0
NORM_EPS = 1e-6


def solution(mesh):
    dp_n = mesh.shape['dp']

    def device_fn(hid_loc, norm_w, emb_loc, teach_loc, mask_loc):
        tok, dim = hid_loc.shape
        vloc = emb_loc.shape[0]
        vsub = vloc // dp_n
        dp_i = lax.axis_index('dp')
        x = hid_loc.astype(jnp.float32)
        scale = 1.0 + norm_w.astype(jnp.float32)
        inv = lax.rsqrt(jnp.mean(x * x, axis=-1, keepdims=True) + NORM_EPS)
        xs = x * inv
        xs_all = lax.all_gather(xs, 'dp', axis=0, tiled=True)
        g_all = (xs_all * scale).astype(jnp.bfloat16)

        t32 = teach_loc.astype(jnp.float32)
        t_x = lax.all_to_all(t32, 'dp', split_axis=1, concat_axis=0, tiled=True)
        m_loc = jnp.max(t32, axis=-1)
        t_sh = t32 - m_loc[:, None]
        t_exp = jnp.exp(t_sh)
        tea = lax.all_gather(jnp.stack([m_loc, jnp.sum(t_exp, axis=-1), jnp.sum(t_exp * t_sh, axis=-1)], axis=0), 'tp')
        t_max = jnp.max(tea[:, 0], axis=0)
        shift = tea[:, 0] - t_max
        fac = jnp.exp(shift)
        s_one = jnp.sum(fac * tea[:, 1], axis=0)
        s_two = jnp.sum(fac * (tea[:, 2] + shift * tea[:, 1]), axis=0)
        log_s = jnp.log(s_one)
        neg_ent = s_two / s_one - log_s
        lse_tea = t_max + log_s
        mask_f32 = mask_loc.astype(jnp.float32)
        small = lax.all_gather(jnp.stack([lse_tea, mask_f32], axis=0), 'dp', axis=1, tiled=True)
        weight = small[1] / jnp.sum(small[1])
        lse_all = small[0]

        emb_sub = lax.dynamic_slice_in_dim(emb_loc, dp_i * vsub, vsub, axis=0)
        raw = jnp.einsum('nd,vd->nv', g_all, emb_sub, preferred_element_type=jnp.float32)
        th = jnp.tanh(raw / SOFT_CAP)
        z = SOFT_CAP * th
        e_s = jnp.exp(z)
        sum_s = lax.psum(jnp.sum(e_s, axis=-1), ('tp', 'dp'))
        p_t = jnp.exp(t_x - lse_all[:, None])
        d_raw = ((e_s / sum_s[:, None] - p_t) * weight[:, None] * (1.0 - th * th)).astype(jnp.bfloat16)
        cross = jnp.sum(jnp.sum(p_t * z, axis=-1) * weight)
        demb_t = jnp.einsum('nd,nv->dv', g_all, d_raw, preferred_element_type=jnp.float32)
        grad_emb = lax.all_to_all(demb_t, 'dp', split_axis=0, concat_axis=1, tiled=True).T
        dg_part = jnp.dot(d_raw, emb_sub, preferred_element_type=jnp.float32)
        dg = lax.psum(lax.psum_scatter(dg_part, 'dp', scatter_dimension=0, tiled=True), 'tp')

        w_loc = mask_f32 / jnp.sum(small[1])
        lse_stu = jnp.log(lax.dynamic_slice_in_dim(sum_s, dp_i * tok, tok))
        own = jnp.sum(w_loc * (neg_ent + lse_stu)) / 4.0
        dw_loc = jnp.sum(dg * xs, axis=0)
        dxs = dg * scale
        dx = inv * dxs - x * (inv * inv * inv) * (jnp.sum(dxs * x, axis=-1, keepdims=True) / dim)
        fin = lax.psum(jnp.concatenate([dw_loc / 4.0, (own - cross)[None]]), ('tp', 'dp'))
        return fin[dim], dx.astype(jnp.bfloat16), grad_emb, fin[:dim]

    return jax.shard_map(device_fn, mesh=mesh, in_specs=(P('dp', None), P(None), P('tp', None), P('dp', 'tp'), P('dp')), out_specs=(P(), P('dp', None), P('tp', 'dp'), P(None)), check_vma=False)
```

```python
import functools

import jax
import jax.numpy as jnp
from jax import lax
from jax.experimental import pallas as pl
from jax.experimental.pallas import tpu as pltpu
from jax.sharding import PartitionSpec as P

SOFT_CAP = 30.0
NORM_EPS = 1e-6
SUB = 256
SLOTS = 3
MESH = pl.DeviceIdType.MESH
NT = (((1,), (1,)), ((), ()))
NN = (((1,), (0,)), ((), ()))


def body(cfg, hid, nw, mask, emb, teach, o_emb, o_dh, o_dw, gbuf,
         t_stage, th_buf, t_recv, tb, e_slot, e_sub, g_all, g_t, gin, dr_loc, r_blk, dr_blk, de_st,
         m_buf, acc, st_tp, st_t, st_dp, st_all, dg_tp, dw_dp, xs_buf, gl_buf,
         tb_sem, es_sem, sub_sem, gl_sem, gin_sem, loc_sem, snd_s, rcv_s, t_snd, t_rcv, de_snd, de_rcv):
    tp_n, dp_n, ny = cfg
    tok, dim = hid.shape
    vloc = emb.shape[0]
    win = t_recv.shape[2]
    n_sub = win // SUB
    n_ch = t_stage.shape[1] // win
    tail = vloc - (n_ch - 1) * win
    chips = dp_n // 2
    nz = chips // ny
    rq = tok // tp_n
    cpad = de_st.shape[1] // dp_n
    cols = dim // dp_n
    last = n_ch - 1
    tp_i = lax.axis_index('tp')
    dp_i = lax.axis_index('dp')
    chip = dp_i // 2
    core = dp_i % 2

    def peer_chip(k):
        j = (k * 5) % chips
        return ((chip // ny + j // ny) % nz) * ny + (chip % ny + j % ny) % ny

    def peer(k):
        return peer_chip(k // 2) * 2 + (core + k % 2) % 2

    def active(dev, s):
        return dev * win + s * SUB < vloc

    def n_act(s):
        return sum(1 for d in range(dp_n) if d * win + s * SUB < vloc)

    barrier = pltpu.get_barrier_semaphore()

    @pl.loop(1, dp_n)
    def _(k):
        pl.semaphore_signal(barrier, inc=1, device_id={'dp': peer(k)}, device_id_type=MESH)

    @pl.loop(1, tp_n)
    def _(k):
        pl.semaphore_signal(barrier, inc=1, device_id={'tp': (tp_i + k) % tp_n}, device_id_type=MESH)

    def tb_copy(r):
        return pltpu.make_async_copy(teach.at[pl.ds(r * 16, 16)], tb.at[r % 2], tb_sem.at[r % 2])

    tb_copy(0).start()
    tb_copy(1).start()

    def e_copy(i, slot, rows):
        return pltpu.make_async_copy(emb.at[pl.ds(pl.multiple_of(i * win, 16), rows)],
                                     e_slot.at[slot, pl.ds(0, rows)], es_sem.at[slot])

    def e_start(i):
        @pl.when(i < last)
        def _():
            e_copy(i, i % SLOTS, win).start()

        @pl.when(i == last)
        def _():
            e_copy(i, i % SLOTS, tail).start()

    def e_wait(i):
        @pl.when(i < last)
        def _():
            e_copy(i, i % SLOTS, win).wait()

        @pl.when(i == last)
        def _():
            e_copy(i, i % SLOTS, tail).wait()

    def sub_copy(rows):
        return pltpu.make_async_copy(emb.at[pl.ds(pl.multiple_of(dp_i * win, 16), rows)],
                                     e_sub.at[pl.ds(0, rows)], sub_sem)

    @pl.when(dp_i < last)
    def _():
        sub_copy(win).start()

    @pl.when(dp_i == last)
    def _():
        sub_copy(tail).start()

    x = hid[...].astype(jnp.float32)
    scale = 1.0 + nw[...].astype(jnp.float32)
    inv = lax.rsqrt(jnp.mean(x * x, axis=-1, keepdims=True) + NORM_EPS)
    xs = x * inv
    xs_buf[...] = xs.reshape(tp_n, rq, dim)
    gl_buf[...] = (xs * scale).astype(jnp.bfloat16)

    own_g = pltpu.make_async_copy(xs_buf.at[tp_i], gbuf.at[chip, core, tp_i], gl_sem)
    own_g.start()

    pl.semaphore_wait(barrier, dp_n - 1 + tp_n - 1)

    pieces = [(c0, min(1024, vloc - c0)) for c0 in range(0, vloc, 1024)]
    full_p = vloc // 1024

    t_stage[:, pl.ds(vloc // 128 * 128, n_ch * win - vloc // 128 * 128)] = jnp.zeros(
        (tok, n_ch * win - vloc // 128 * 128), jnp.float32)
    for r in range(tok // 16):
        tb_copy(r).wait()
        rows = pl.ds(r * 16, 16)

        def conv(c0, width, mx):
            v = tb[r % 2, :, pl.ds(c0, width)].astype(jnp.float32)
            t_stage[rows, pl.ds(c0, width)] = v
            return v

        def step(i, mx):
            v = conv(pl.multiple_of(i * 1024, 128), 1024, mx)
            for q in range(8):
                mx = jnp.maximum(mx, v[:, q * 128:(q + 1) * 128])
            return mx

        mx = lax.fori_loop(0, full_p, step, jnp.full((16, 128), -jnp.inf, jnp.float32))
        m1 = jnp.max(mx, axis=-1, keepdims=True)
        if full_p * 1024 < vloc:
            v = conv(full_p * 1024, vloc - full_p * 1024, None)
            m1 = jnp.maximum(m1, jnp.max(v, axis=-1, keepdims=True))
        m_buf[rows, :] = jnp.broadcast_to(m1, (16, 128))
        if r + 2 < tok // 16:
            tb_copy(r + 2).start()

    for i in range(SLOTS):
        e_start(i)

    def ga_copy(pc):
        return pltpu.make_async_remote_copy(xs_buf.at[tp_i], gbuf.at[chip, core, tp_i], snd_s.at[0], rcv_s.at[0],
                                            device_id={'dp': pc * 2 + core}, device_id_type=MESH)

    @pl.loop(1, chips)
    def _(k):
        ga_copy(peer_chip(k)).start()

    def t_copy(dev, s):
        lane = pl.multiple_of(dev * win + s * SUB, SUB)
        return pltpu.make_async_remote_copy(t_stage.at[:, pl.ds(lane, SUB)], t_recv.at[dp_i, :, pl.ds(s * SUB, SUB)],
                                            t_snd.at[s], t_rcv.at[s], device_id={'dp': dev}, device_id_type=MESH)

    for s in range(n_sub):
        @pl.loop(1, dp_n)
        def _(k, s=s):
            dev = peer(k)

            @pl.when(active(dev, s))
            def _():
                t_copy(dev, s).start()

        @pl.when(active(dp_i, s))
        def _(s=s):
            lane = pl.multiple_of(dp_i * win + s * SUB, SUB)
            t_recv[dp_i, :, pl.ds(s * SUB, SUB)] = t_stage[:, pl.ds(lane, SUB)]

    own_g.wait()
    pltpu.make_async_remote_copy(gbuf.at[pl.ds(0, chips - 1), 0, 0], gbuf.at[pl.ds(0, chips - 1), 0, 0], snd_s.at[0],
                                 rcv_s.at[0], device_id={'dp': dp_i}, device_id_type=MESH).wait_recv()

    def gb_copy(q):
        return pltpu.make_async_remote_copy(gbuf.at[:, core, tp_i], gbuf.at[:, core, tp_i], snd_s.at[1],
                                            rcv_s.at[1], device_id={'tp': q}, device_id_type=MESH)

    @pl.loop(1, tp_n)
    def _(k):
        gb_copy((tp_i + k) % tp_n).start()

    acc[...] = jnp.zeros_like(acc)
    lanes = lax.broadcasted_iota(jnp.int32, (tok, 128), 1)

    @pl.loop(0, n_ch)
    def _(i):
        e_wait(i)
        base = pl.multiple_of(i * win, SUB)
        th_buf[:, pl.ds(base, win)] = lax.dot_general(gl_buf[...], e_slot[i % SLOTS], NT,
                                                      preferred_element_type=jnp.float32)

        @pl.when(i + SLOTS < n_ch)
        def _():
            e_start(i + SLOTS)

        m_l = m_buf[...]
        a_s, a_1, a_2, a_x = acc[0], acc[1], acc[2], acc[3]
        for q in range(win // 128):
            at = pl.ds(pl.multiple_of(base + q * 128, 128), 128)
            th = jnp.tanh(th_buf[:, at] * (1.0 / SOFT_CAP))
            th_buf[:, at] = th
            z = SOFT_CAP * th
            ok = base + q * 128 + lanes < vloc
            e_s = jnp.where(ok, jnp.exp(z), 0.0)
            sh = t_stage[:, at] - m_l
            e_t = jnp.where(ok, jnp.exp(sh), 0.0)
            sh = jnp.where(ok, sh, 0.0)
            a_s = a_s + e_s
            a_1 = a_1 + e_t
            a_2 = a_2 + e_t * sh
            a_x = a_x + e_t * jnp.where(ok, z, 0.0)
        acc[0] = a_s
        acc[1] = a_1
        acc[2] = a_2
        acc[3] = a_x

    for i in range(SLOTS):
        e_start(i)

    parts = [m_buf[:, 0:1]] + [jnp.sum(acc[j], axis=-1, keepdims=True) for j in (1, 2, 3, 0)]
    tile = jnp.zeros((tok, 128), jnp.float32)
    for j, v in enumerate(parts):
        tile = jnp.where(lanes == j, v, tile)
    st_tp[tp_i] = tile

    def st_copy(q):
        return pltpu.make_async_remote_copy(st_tp.at[tp_i], st_tp.at[tp_i], snd_s.at[2], rcv_s.at[2],
                                            device_id={'tp': q}, device_id_type=MESH)

    @pl.loop(1, tp_n)
    def _(k):
        st_copy((tp_i + k) % tp_n).start()

    sib = chip * 2 + (core + 1) % 2
    gb_wait = pltpu.make_async_remote_copy(gbuf.at[:, 0, pl.ds(0, tp_n - 1)], gbuf.at[:, 0, pl.ds(0, tp_n - 1)],
                                           snd_s.at[1], rcv_s.at[1], device_id={'dp': dp_i}, device_id_type=MESH)
    gb_wait.wait_recv()
    gc_copy = pltpu.make_async_remote_copy(gbuf.at[:, core], gbuf.at[:, core], snd_s.at[3], rcv_s.at[3],
                                           device_id={'dp': sib}, device_id_type=MESH)
    gc_copy.start()

    st_wait = pltpu.make_async_remote_copy(st_tp.at[pl.ds(0, tp_n - 1)], st_tp.at[pl.ds(0, tp_n - 1)], snd_s.at[2],
                                           rcv_s.at[2], device_id={'dp': dp_i}, device_id_type=MESH)
    st_wait.wait_recv()
    t_max = st_tp[0][:, 0:1]
    for q in range(1, tp_n):
        t_max = jnp.maximum(t_max, st_tp[q][:, 0:1])
    s_1 = s_2 = s_x = s_s = jnp.zeros((tok, 1), jnp.float32)
    for q in range(tp_n):
        v = st_tp[q]
        shift = v[:, 0:1] - t_max
        fac = jnp.exp(shift)
        s_1 = s_1 + fac * v[:, 1:2]
        s_2 = s_2 + fac * (v[:, 2:3] + shift * v[:, 1:2])
        s_x = s_x + fac * v[:, 3:4]
        s_s = s_s + v[:, 4:5]
    log_1 = jnp.log(s_1)
    kl = (s_2 - s_x) / s_1 - log_1 + jnp.log(s_s)
    lse_t = t_max + log_1
    inv_s = 1.0 / s_s
    m_loc = mask[...]
    tile = jnp.where(lanes == 0, lse_t, jnp.where(lanes == 1, inv_s, jnp.where(lanes == 2, m_loc, 0.0)))
    tile = jnp.concatenate([tile, jnp.zeros((128 - tok, 128), jnp.float32)], axis=0).T
    st_dp[dp_i] = tile[0:8]

    def sd_copy(dev):
        return pltpu.make_async_remote_copy(st_dp.at[dp_i], st_dp.at[dp_i], snd_s.at[4], rcv_s.at[4],
                                            device_id={'dp': dev}, device_id_type=MESH)

    @pl.loop(1, dp_n)
    def _(k):
        sd_copy(peer(k)).start()

    sd_wait = pltpu.make_async_remote_copy(st_dp.at[pl.ds(0, dp_n - 1)], st_dp.at[pl.ds(0, dp_n - 1)], snd_s.at[4],
                                           rcv_s.at[4], device_id={'dp': dp_i}, device_id_type=MESH)
    sd_wait.wait_recv()
    m_cnt = jnp.sum(jnp.sum(st_dp[...], axis=0)[2:3, :], axis=-1, keepdims=True)
    w_loc = m_loc / m_cnt

    @pl.loop(0, dp_n)
    def _(d):
        v = jnp.concatenate([st_dp[d], jnp.zeros((120, 128), jnp.float32)], axis=0).T
        st_all[d] = v[0:tok]

    dg_tp[tp_i] = jnp.zeros((tok, dim), jnp.float32)

    @pl.loop(0, n_ch)
    def _(i):
        e_wait(i)
        base = pl.multiple_of(i * win, SUB)
        for q in range(win // 128):
            at = pl.ds(pl.multiple_of(base + q * 128, 128), 128)
            th = th_buf[:, at]
            p_s = jnp.exp(SOFT_CAP * th) * inv_s
            p_t = jnp.exp(t_stage[:, at] - lse_t)
            d = (p_s - p_t) * w_loc * (1.0 - th * th)
            ok = base + q * 128 + lanes < vloc
            dr_loc[:, pl.ds(q * 128, 128)] = jnp.where(ok, d, 0.0).astype(jnp.bfloat16)
        dg_tp[tp_i] += lax.dot_general(dr_loc[...], e_slot[i % SLOTS], NN, preferred_element_type=jnp.float32)

        @pl.when(i + SLOTS < n_ch)
        def _():
            e_start(i + SLOTS)

    def dg_copy(q):
        return pltpu.make_async_remote_copy(dg_tp.at[tp_i], dg_tp.at[tp_i], snd_s.at[5], rcv_s.at[5],
                                            device_id={'tp': q}, device_id_type=MESH)

    @pl.loop(1, tp_n)
    def _(k):
        dg_copy((tp_i + k) % tp_n).start()

    gc_copy.wait()

    def gin_copy(d):
        return pltpu.make_async_copy(gbuf.at[d // 2, d % 2], gin.at[d % 2], gin_sem.at[d % 2])

    gin_copy(0).start()
    gin_copy(1).start()

    for d in range(dp_n):
        gin_copy(d).wait()
        gv = (gin[d % 2].reshape(tok, dim) * scale)
        g_all[pl.ds(d * tok, tok), :] = gv.astype(jnp.bfloat16)
        if d + 2 < dp_n:
            gin_copy(d + 2).start()

    for d in range(0, dp_n, 2):
        gv = g_all[pl.ds(d * tok, 2 * tok), :].astype(jnp.float32).T
        for c in range(dp_n):
            gc = gv[c * cols:(c + 1) * cols]
            if cpad != cols:
                gc = jnp.concatenate([gc, jnp.zeros((cpad - cols, 2 * tok), jnp.float32)], axis=0)
            g_t[pl.ds(c * cpad, cpad), pl.ds(d * tok, 2 * tok)] = gc.astype(jnp.bfloat16)

    dg_wait = pltpu.make_async_remote_copy(dg_tp.at[pl.ds(0, tp_n - 1)], dg_tp.at[pl.ds(0, tp_n - 1)], snd_s.at[5],
                                           rcv_s.at[5], device_id={'dp': dp_i}, device_id_type=MESH)
    dg_wait.wait_recv()
    dg = dg_tp[0]
    for q in range(1, tp_n):
        dg = dg + dg_tp[q]
    x = hid[...].astype(jnp.float32)
    inv = lax.rsqrt(jnp.mean(x * x, axis=-1, keepdims=True) + NORM_EPS)
    dxs = dg * scale
    o_dh[...] = (inv * dxs - x * (inv * inv * inv * (jnp.sum(dxs * x, axis=-1, keepdims=True) / dim))).astype(jnp.bfloat16)
    dw = jnp.sum(dg * (x * inv), axis=0, keepdims=True)
    dw_dp[dp_i] = jnp.broadcast_to(jnp.sum(w_loc * kl, axis=0, keepdims=True), (8, 128))
    for j in range(dim // 128):
        dw_dp[dp_i, pl.ds(j, 1), :] = dw[:, j * 128:(j + 1) * 128]

    def dw_copy(dev):
        return pltpu.make_async_remote_copy(dw_dp.at[dp_i], dw_dp.at[dp_i], snd_s.at[6], rcv_s.at[6],
                                            device_id={'dp': dev}, device_id_type=MESH)

    @pl.loop(1, dp_n)
    def _(k):
        dw_copy(peer(k)).start()

    @pl.when(dp_i < last)
    def _():
        sub_copy(win).wait()

    @pl.when(dp_i == last)
    def _():
        sub_copy(tail).wait()

    row_n = 4 * tok

    def de_copy(dev, s):
        lane = pl.multiple_of(dp_i * win + s * SUB, SUB)
        return pltpu.make_async_remote_copy(de_st.at[s % 2, pl.ds(pl.multiple_of(dev * cpad, 8), cpad)],
                                            o_emb.at[:, pl.ds(lane, SUB)], de_snd.at[s % 2], de_rcv,
                                            device_id={'dp': dev}, device_id_type=MESH)

    def de_local(s):
        lane = pl.multiple_of(dp_i * win + s * SUB, SUB)
        return pltpu.make_async_copy(de_st.at[s % 2, pl.ds(pl.multiple_of(dp_i * cpad, 8), cpad)],
                                     o_emb.at[:, pl.ds(lane, SUB)], loc_sem.at[s % 2])

    def de_wait(s):
        @pl.when(active(dp_i, s))
        def _():
            pltpu.make_async_remote_copy(de_st.at[s % 2, pl.ds(0, (dp_n - 1) * cpad)],
                                         de_st.at[s % 2, pl.ds(0, (dp_n - 1) * cpad)], de_snd.at[s % 2], de_rcv,
                                         device_id={'dp': dp_i}, device_id_type=MESH).wait_send()
            de_local(s).wait()

    for s in range(n_sub):
        if s >= 2:
            de_wait(s - 2)

        @pl.when(active(dp_i, s))
        def _(s=s):
            part = t_recv.at[pl.ds(0, dp_n - 1), :, pl.ds(s * SUB, SUB)]
            pltpu.make_async_remote_copy(part, part, t_snd.at[s], t_rcv.at[s], device_id={'dp': dp_i},
                                         device_id_type=MESH).wait_recv()

            @pl.loop(0, dp_n // 4)
            def _(b):
                rows = pl.ds(pl.multiple_of(b * row_n, row_n), row_n)
                r_blk[...] = lax.dot_general(g_all[rows, :], e_sub[pl.ds(s * SUB, SUB), :], NT,
                                             preferred_element_type=jnp.float32)
                for q in range(row_n // 32):
                    d = b * 4 + q * 32 // tok
                    off = q * 32 % tok
                    th = jnp.tanh(r_blk[pl.ds(q * 32, 32), :] * (1.0 / SOFT_CAP))
                    sv = st_all[d, pl.ds(off, 32), :]
                    p_s = jnp.exp(SOFT_CAP * th) * sv[:, 1:2]
                    p_t = jnp.exp(t_recv[d, pl.ds(off, 32), pl.ds(s * SUB, SUB)] - sv[:, 0:1])
                    dv = (p_s - p_t) * (sv[:, 2:3] / m_cnt) * (1.0 - th * th)
                    dr_blk[pl.ds(pl.multiple_of(b * row_n + q * 32, 32), 32), :] = dv.astype(jnp.bfloat16)

            @pl.loop(0, de_st.shape[1] // 256)
            def _(b):
                rows = pl.ds(pl.multiple_of(b * 256, 256), 256)
                de_st[s % 2, rows, :] = lax.dot_general(g_t[rows, :], dr_blk[...], NN,
                                                        preferred_element_type=jnp.float32)

            @pl.loop(1, dp_n)
            def _(k):
                de_copy(peer(k), s).start()

            de_local(s).start()

    dw_wait = pltpu.make_async_remote_copy(dw_dp.at[pl.ds(0, dp_n - 1)], dw_dp.at[pl.ds(0, dp_n - 1)], snd_s.at[6],
                                           rcv_s.at[6], device_id={'dp': dp_i}, device_id_type=MESH)
    dw_wait.wait_recv()
    tot = dw_dp[0]
    for d in range(1, dp_n):
        tot = tot + dw_dp[d]
    o_dw[...] = tot

    ga_wait = pltpu.make_async_remote_copy(gbuf.at[pl.ds(0, chips - 1), 0, 0], gbuf.at[pl.ds(0, chips - 1), 0, 0],
                                           snd_s.at[0], rcv_s.at[0], device_id={'dp': dp_i}, device_id_type=MESH)
    for w in (ga_wait, gb_wait, st_wait, sd_wait, dg_wait, dw_wait):
        w.wait_send()

    def t_drain(s, n):
        pltpu.make_async_remote_copy(t_stage.at[:, pl.ds(0, n * SUB)], t_stage.at[:, pl.ds(0, n * SUB)], t_snd.at[s],
                                     t_rcv.at[s], device_id={'dp': dp_i}, device_id_type=MESH).wait_send()

    for s in range(n_sub):
        @pl.when(active(dp_i, s))
        def _(s=s):
            t_drain(s, n_act(s) - 1)

        @pl.when(jnp.logical_not(active(dp_i, s)))
        def _(s=s):
            t_drain(s, n_act(s))

    for s in range(max(0, n_sub - 2), n_sub):
        de_wait(s)

    total = sum(n_act(s) for s in range(n_sub))
    tail_n = -(-tail // SUB)

    def de_drain(n):
        part = o_emb.at[:, pl.ds(0, n * SUB)]
        pltpu.make_async_remote_copy(part, part, de_snd.at[0], de_rcv, device_id={'dp': dp_i},
                                     device_id_type=MESH).wait_recv()

    @pl.when(dp_i < last)
    def _():
        de_drain(total - n_sub)

    @pl.when(dp_i == last)
    def _():
        de_drain(total - tail_n)

    @pl.when(dp_i > last)
    def _():
        de_drain(total)


def solution(mesh):
    tp_n, dp_n = mesh.shape['tp'], mesh.shape['dp']
    ny = 4 if dp_n >= 32 else 1

    def device_fn(hid_loc, norm_w, emb_loc, teach_loc, mask_loc):
        tok, dim = hid_loc.shape
        vloc = emb_loc.shape[0]
        win = -(-vloc // (dp_n * SUB)) * SUB
        n_ch = -(-vloc // win)
        cols = dim // dp_n
        cpad = -(-cols // 8) * 8
        rq = tok // tp_n
        f32, bf16 = jnp.float32, jnp.bfloat16
        vm, dma = pltpu.VMEM, pltpu.SemaphoreType.DMA
        any_s, vm_s = pl.BlockSpec(memory_space=pl.ANY), pl.BlockSpec(memory_space=pltpu.VMEM)
        wide = n_ch * win
        o_emb, o_dh, o_dw, _ = pl.pallas_call(
            functools.partial(body, (tp_n, dp_n, ny)),
            out_shape=(jax.ShapeDtypeStruct((cpad, wide), f32), jax.ShapeDtypeStruct((tok, dim), bf16),
                       jax.ShapeDtypeStruct((8, 128), f32),
                       jax.ShapeDtypeStruct((dp_n // 2, 2, tp_n, rq, dim), f32)),
            in_specs=[vm_s, vm_s, vm_s, any_s, any_s],
            out_specs=(any_s, vm_s, vm_s, any_s),
            scratch_shapes=[
                vm((tok, wide), f32), vm((tok, wide), f32), vm((dp_n, tok, win), f32), vm((2, 16, vloc), bf16),
                vm((SLOTS, win, dim), bf16), vm((win, dim), bf16), vm((dp_n * tok, dim), bf16),
                vm((dp_n * cpad, dp_n * tok), bf16), vm((2, tp_n, rq, dim), f32), vm((tok, win), bf16),
                vm((4 * tok, SUB), f32), vm((dp_n * tok, SUB), bf16), vm((2, dp_n * cpad, SUB), f32),
                vm((tok, 128), f32), vm((4, tok, 128), f32), vm((tp_n, tok, 128), f32), vm((8, 128), f32),
                vm((dp_n, 8, 128), f32), vm((dp_n, tok, 128), f32), vm((tp_n, tok, dim), f32),
                vm((dp_n, 8, 128), f32), vm((tp_n, rq, dim), f32), vm((tok, dim), bf16),
                dma((2,)), dma((SLOTS,)), dma, dma, dma((2,)), dma((2,)), dma((7,)), dma((7,)),
                dma((win // SUB,)), dma((win // SUB,)), dma((2,)), dma,
            ],
            compiler_params=pltpu.CompilerParams(collective_id=0, has_side_effects=True,
                                                 vmem_limit_bytes=66_000_000),
            name='head',
        )(hid_loc, norm_w.reshape(1, dim), mask_loc.astype(f32).reshape(tok, 1), emb_loc, teach_loc)
        return o_dw[7, 0], o_dh, o_emb[:cols, :vloc].T, o_dw.reshape(-1)[:dim]

    return jax.shard_map(device_fn, mesh=mesh, in_specs=(P('dp', None), P(None), P('tp', None), P('dp', 'tp'), P('dp')),
                         out_specs=(P(), P('dp', None), P('tp', 'dp'), P(None)), check_vma=False)
```

```python
import functools

import jax
import jax.numpy as jnp
from jax import lax
from jax.experimental import pallas as pl
from jax.experimental.pallas import tpu as pltpu
from jax.sharding import PartitionSpec as P

SOFT_CAP = 30.0
NORM_EPS = 1e-6
SUB = 256
SLOTS = 3
MESH = pl.DeviceIdType.MESH
NT = (((1,), (1,)), ((), ()))
NN = (((1,), (0,)), ((), ()))


def body(cfg, hid, nw, mask, emb, teach, o_emb, o_dh, o_dw, gbuf,
         t_stage, th_buf, t_recv, tb, e_slot, e_sub, g_all, g_t, gin, dr_loc, r_blk, dr_blk, de_st,
         rl_t, rl_e, m_buf, acc, st_tp, st_t, st_dp, st_all, dg_tp, dw_dp, xs_buf, gl_buf,
         tb_sem, es_sem, sub_sem, gl_sem, gin_sem, loc_sem, snd_s, rcv_s, t_snd, t_rcv, de_snd, de_rcv, rt_rcv, rt_snd, re_rcv, re_snd):
    tp_n, dp_n, ny = cfg
    tok, dim = hid.shape
    vloc = emb.shape[0]
    win = t_recv.shape[2]
    n_sub = win // SUB
    n_ch = t_stage.shape[1] // win
    tail = vloc - (n_ch - 1) * win
    chips = dp_n // 2
    nz = chips // ny
    rq = tok // tp_n
    cpad = de_st.shape[1] // dp_n
    cols = dim // dp_n
    last = n_ch - 1
    tp_i = lax.axis_index('tp')
    dp_i = lax.axis_index('dp')
    chip = dp_i // 2
    core = dp_i % 2

    def offset(k):
        j = (k // 2 * 5) % chips
        return j // ny, j % ny, k % 2

    def device(dz, dy, dc):
        return (((chip // ny + dz + nz) % nz) * ny + (chip % ny + dy + ny) % ny) * 2 + (core + dc) % 2

    def peer_chip(k):
        dz, dy, _ = offset(2 * k)
        return device(dz, dy, 0) // 2

    def peer(k):
        return device(*offset(k))

    def is_two(v, n):
        return (v // 2) * (1 - v % 2) if n == 4 else 0 * v

    def far(k):
        dz, dy, _ = offset(k)
        return is_two(dz, nz) + is_two(dy, ny)

    def hops(k):
        dz, dy, dc = offset(k)
        tz, ty = is_two(dz, nz), is_two(dy, ny)
        slot = 2 * (tz * dy + (1 - tz) * (4 + (dz + 1) // 2)) + dc
        rz, ry = (1 - 2 * dc) * tz, (1 - 2 * dc) * ty
        return slot, (rz, ry), (dz - rz, dy - ry, dc)

    def each_far(f):
        if nz == 4 or ny == 4:
            @pl.loop(1, dp_n)
            def _(k):
                pl.when(far(k) > 0)(functools.partial(f, k))

    def each_near(f):
        @pl.loop(1, dp_n)
        def _(k):
            pl.when(far(k) == 0)(functools.partial(f, k))

    def active(dev, s):
        return dev * win + s * SUB < vloc

    def n_act(s):
        return sum(1 for d in range(dp_n) if d * win + s * SUB < vloc)

    barrier = pltpu.get_barrier_semaphore()

    @pl.loop(1, dp_n)
    def _(k):
        pl.semaphore_signal(barrier, inc=1, device_id={'dp': peer(k)}, device_id_type=MESH)

    @pl.loop(1, tp_n)
    def _(k):
        pl.semaphore_signal(barrier, inc=1, device_id={'tp': (tp_i + k) % tp_n}, device_id_type=MESH)

    def tb_copy(r):
        return pltpu.make_async_copy(teach.at[pl.ds(r * 16, 16)], tb.at[r % 2], tb_sem.at[r % 2])

    tb_copy(0).start()
    tb_copy(1).start()

    def e_copy(i, slot, rows):
        return pltpu.make_async_copy(emb.at[pl.ds(pl.multiple_of(i * win, 16), rows)],
                                     e_slot.at[slot, pl.ds(0, rows)], es_sem.at[slot])

    def e_start(i):
        @pl.when(i < last)
        def _():
            e_copy(i, i % SLOTS, win).start()

        @pl.when(i == last)
        def _():
            e_copy(i, i % SLOTS, tail).start()

    def e_wait(i):
        @pl.when(i < last)
        def _():
            e_copy(i, i % SLOTS, win).wait()

        @pl.when(i == last)
        def _():
            e_copy(i, i % SLOTS, tail).wait()

    def sub_copy(rows):
        return pltpu.make_async_copy(emb.at[pl.ds(pl.multiple_of(dp_i * win, 16), rows)],
                                     e_sub.at[pl.ds(0, rows)], sub_sem)

    @pl.when(dp_i < last)
    def _():
        sub_copy(win).start()

    @pl.when(dp_i == last)
    def _():
        sub_copy(tail).start()

    x = hid[...].astype(jnp.float32)
    scale = 1.0 + nw[...].astype(jnp.float32)
    inv = lax.rsqrt(jnp.mean(x * x, axis=-1, keepdims=True) + NORM_EPS)
    xs = x * inv
    xs_buf[...] = xs.reshape(tp_n, rq, dim)
    gl_buf[...] = (xs * scale).astype(jnp.bfloat16)

    own_g = pltpu.make_async_copy(xs_buf.at[tp_i], gbuf.at[chip, core, tp_i], gl_sem)
    own_g.start()

    pl.semaphore_wait(barrier, dp_n - 1 + tp_n - 1)

    pieces = [(c0, min(1024, vloc - c0)) for c0 in range(0, vloc, 1024)]
    full_p = vloc // 1024

    t_stage[:, pl.ds(vloc // 128 * 128, n_ch * win - vloc // 128 * 128)] = jnp.zeros(
        (tok, n_ch * win - vloc // 128 * 128), jnp.float32)
    for r in range(tok // 16):
        tb_copy(r).wait()
        rows = pl.ds(r * 16, 16)

        def conv(c0, width, mx):
            v = tb[r % 2, :, pl.ds(c0, width)].astype(jnp.float32)
            t_stage[rows, pl.ds(c0, width)] = v
            return v

        def step(i, mx):
            v = conv(pl.multiple_of(i * 1024, 128), 1024, mx)
            for q in range(8):
                mx = jnp.maximum(mx, v[:, q * 128:(q + 1) * 128])
            return mx

        mx = lax.fori_loop(0, full_p, step, jnp.full((16, 128), -jnp.inf, jnp.float32))
        m1 = jnp.max(mx, axis=-1, keepdims=True)
        if full_p * 1024 < vloc:
            v = conv(full_p * 1024, vloc - full_p * 1024, None)
            m1 = jnp.maximum(m1, jnp.max(v, axis=-1, keepdims=True))
        m_buf[rows, :] = jnp.broadcast_to(m1, (16, 128))
        if r + 2 < tok // 16:
            tb_copy(r + 2).start()

    for i in range(SLOTS):
        e_start(i)

    def ga_copy(pc):
        return pltpu.make_async_remote_copy(xs_buf.at[tp_i], gbuf.at[chip, core, tp_i], snd_s.at[0], rcv_s.at[0],
                                            device_id={'dp': pc * 2 + core}, device_id_type=MESH)

    @pl.loop(1, chips)
    def _(k):
        ga_copy(peer_chip(k)).start()

    def t_copy(dev, s, k):
        lane = pl.multiple_of(dev * win + s * SUB, SUB)
        return pltpu.make_async_remote_copy(t_stage.at[:, pl.ds(lane, SUB)], t_recv.at[dp_i, :, pl.ds(s * SUB, SUB)],
                                            t_snd.at[k], t_rcv.at[s], device_id={'dp': dev}, device_id_type=MESH)

    def t_first(k):
        slot, (rz, ry), _ = hops(k)
        dev = peer(k)
        lane = pl.multiple_of(dev * win, SUB)

        @pl.when(active(dev, 0))
        def _():
            pltpu.make_async_remote_copy(t_stage.at[:, pl.ds(lane, win)], rl_t.at[slot], t_snd.at[k], rt_rcv.at[slot],
                                         device_id={'dp': device(rz, ry, 0)}, device_id_type=MESH).start()

    each_far(t_first)

    for s in range(n_sub):
        def t_near(k, s=s):
            dev = peer(k)

            @pl.when(active(dev, s))
            def _():
                t_copy(dev, s, k).start()

        each_near(t_near)

        @pl.when(active(dp_i, s))
        def _(s=s):
            lane = pl.multiple_of(dp_i * win + s * SUB, SUB)
            t_recv[dp_i, :, pl.ds(s * SUB, SUB)] = t_stage[:, pl.ds(lane, SUB)]

    own_g.wait()
    pltpu.make_async_remote_copy(gbuf.at[pl.ds(0, chips - 1), 0, 0], gbuf.at[pl.ds(0, chips - 1), 0, 0], snd_s.at[0],
                                 rcv_s.at[0], device_id={'dp': dp_i}, device_id_type=MESH).wait_recv()

    def gb_copy(q):
        return pltpu.make_async_remote_copy(gbuf.at[:, core, tp_i], gbuf.at[:, core, tp_i], snd_s.at[1],
                                            rcv_s.at[1], device_id={'tp': q}, device_id_type=MESH)

    @pl.loop(1, tp_n)
    def _(k):
        gb_copy((tp_i + k) % tp_n).start()

    acc[...] = jnp.zeros_like(acc)
    lanes = lax.broadcasted_iota(jnp.int32, (tok, 128), 1)

    @pl.loop(0, n_ch)
    def _(i):
        e_wait(i)
        base = pl.multiple_of(i * win, SUB)
        th_buf[:, pl.ds(base, win)] = lax.dot_general(gl_buf[...], e_slot[i % SLOTS], NT,
                                                      preferred_element_type=jnp.float32)

        @pl.when(i + SLOTS < n_ch)
        def _():
            e_start(i + SLOTS)

        m_l = m_buf[...]
        a_s, a_1, a_2, a_x = acc[0], acc[1], acc[2], acc[3]
        for q in range(win // 128):
            at = pl.ds(pl.multiple_of(base + q * 128, 128), 128)
            th = jnp.tanh(th_buf[:, at] * (1.0 / SOFT_CAP))
            th_buf[:, at] = th
            z = SOFT_CAP * th
            ok = base + q * 128 + lanes < vloc
            e_s = jnp.where(ok, jnp.exp(z), 0.0)
            sh = t_stage[:, at] - m_l
            e_t = jnp.where(ok, jnp.exp(sh), 0.0)
            sh = jnp.where(ok, sh, 0.0)
            a_s = a_s + e_s
            a_1 = a_1 + e_t
            a_2 = a_2 + e_t * sh
            a_x = a_x + e_t * jnp.where(ok, z, 0.0)
        acc[0] = a_s
        acc[1] = a_1
        acc[2] = a_2
        acc[3] = a_x

    for i in range(SLOTS):
        e_start(i)

    parts = [m_buf[:, 0:1]] + [jnp.sum(acc[j], axis=-1, keepdims=True) for j in (1, 2, 3, 0)]
    tile = jnp.zeros((tok, 128), jnp.float32)
    for j, v in enumerate(parts):
        tile = jnp.where(lanes == j, v, tile)
    st_tp[tp_i] = tile

    def st_copy(q):
        return pltpu.make_async_remote_copy(st_tp.at[tp_i], st_tp.at[tp_i], snd_s.at[2], rcv_s.at[2],
                                            device_id={'tp': q}, device_id_type=MESH)

    @pl.loop(1, tp_n)
    def _(k):
        st_copy((tp_i + k) % tp_n).start()

    def t_arrived(k):
        slot, _, end = hops(k)

        @pl.when(active(device(*end), 0))
        def _():
            pltpu.make_async_remote_copy(rl_t.at[slot], rl_t.at[slot], t_snd.at[0], rt_rcv.at[slot],
                                         device_id={'dp': dp_i}, device_id_type=MESH).wait_recv()

    each_far(t_arrived)

    for s in range(n_sub):
        def t_second(k, s=s):
            slot, (rz, ry), end = hops(k)
            dev = device(*end)
            part = pl.ds(s * SUB, SUB)

            @pl.when(active(dev, s))
            def _():
                pltpu.make_async_remote_copy(rl_t.at[slot, :, part], t_recv.at[device(-rz, -ry, 0), :, part],
                                             rt_snd.at[slot], t_rcv.at[s], device_id={'dp': dev},
                                             device_id_type=MESH).start()

        each_far(t_second)

    sib = chip * 2 + (core + 1) % 2
    gb_wait = pltpu.make_async_remote_copy(gbuf.at[:, 0, pl.ds(0, tp_n - 1)], gbuf.at[:, 0, pl.ds(0, tp_n - 1)],
                                           snd_s.at[1], rcv_s.at[1], device_id={'dp': dp_i}, device_id_type=MESH)
    gb_wait.wait_recv()
    gc_copy = pltpu.make_async_remote_copy(gbuf.at[:, core], gbuf.at[:, core], snd_s.at[3], rcv_s.at[3],
                                           device_id={'dp': sib}, device_id_type=MESH)
    gc_copy.start()

    st_wait = pltpu.make_async_remote_copy(st_tp.at[pl.ds(0, tp_n - 1)], st_tp.at[pl.ds(0, tp_n - 1)], snd_s.at[2],
                                           rcv_s.at[2], device_id={'dp': dp_i}, device_id_type=MESH)
    st_wait.wait_recv()
    t_max = st_tp[0][:, 0:1]
    for q in range(1, tp_n):
        t_max = jnp.maximum(t_max, st_tp[q][:, 0:1])
    s_1 = s_2 = s_x = s_s = jnp.zeros((tok, 1), jnp.float32)
    for q in range(tp_n):
        v = st_tp[q]
        shift = v[:, 0:1] - t_max
        fac = jnp.exp(shift)
        s_1 = s_1 + fac * v[:, 1:2]
        s_2 = s_2 + fac * (v[:, 2:3] + shift * v[:, 1:2])
        s_x = s_x + fac * v[:, 3:4]
        s_s = s_s + v[:, 4:5]
    log_1 = jnp.log(s_1)
    kl = (s_2 - s_x) / s_1 - log_1 + jnp.log(s_s)
    lse_t = t_max + log_1
    inv_s = 1.0 / s_s
    m_loc = mask[...]
    tile = jnp.where(lanes == 0, lse_t, jnp.where(lanes == 1, inv_s, jnp.where(lanes == 2, m_loc, 0.0)))
    tile = jnp.concatenate([tile, jnp.zeros((128 - tok, 128), jnp.float32)], axis=0).T
    st_dp[dp_i] = tile[0:8]

    def sd_copy(dev):
        return pltpu.make_async_remote_copy(st_dp.at[dp_i], st_dp.at[dp_i], snd_s.at[4], rcv_s.at[4],
                                            device_id={'dp': dev}, device_id_type=MESH)

    @pl.loop(1, dp_n)
    def _(k):
        sd_copy(peer(k)).start()

    sd_wait = pltpu.make_async_remote_copy(st_dp.at[pl.ds(0, dp_n - 1)], st_dp.at[pl.ds(0, dp_n - 1)], snd_s.at[4],
                                           rcv_s.at[4], device_id={'dp': dp_i}, device_id_type=MESH)
    sd_wait.wait_recv()
    m_cnt = jnp.sum(jnp.sum(st_dp[...], axis=0)[2:3, :], axis=-1, keepdims=True)
    w_loc = m_loc / m_cnt

    @pl.loop(0, dp_n)
    def _(d):
        v = jnp.concatenate([st_dp[d], jnp.zeros((120, 128), jnp.float32)], axis=0).T
        st_all[d] = v[0:tok]

    dg_tp[tp_i] = jnp.zeros((tok, dim), jnp.float32)

    @pl.loop(0, n_ch)
    def _(i):
        e_wait(i)
        base = pl.multiple_of(i * win, SUB)
        for q in range(win // 128):
            at = pl.ds(pl.multiple_of(base + q * 128, 128), 128)
            th = th_buf[:, at]
            p_s = jnp.exp(SOFT_CAP * th) * inv_s
            p_t = jnp.exp(t_stage[:, at] - lse_t)
            d = (p_s - p_t) * w_loc * (1.0 - th * th)
            ok = base + q * 128 + lanes < vloc
            dr_loc[:, pl.ds(q * 128, 128)] = jnp.where(ok, d, 0.0).astype(jnp.bfloat16)
        dg_tp[tp_i] += lax.dot_general(dr_loc[...], e_slot[i % SLOTS], NN, preferred_element_type=jnp.float32)

        @pl.when(i + SLOTS < n_ch)
        def _():
            e_start(i + SLOTS)

    def dg_copy(q):
        return pltpu.make_async_remote_copy(dg_tp.at[tp_i], dg_tp.at[tp_i], snd_s.at[5], rcv_s.at[5],
                                            device_id={'tp': q}, device_id_type=MESH)

    @pl.loop(1, tp_n)
    def _(k):
        dg_copy((tp_i + k) % tp_n).start()

    gc_copy.wait()

    def gin_copy(d):
        return pltpu.make_async_copy(gbuf.at[d // 2, d % 2], gin.at[d % 4], gin_sem.at[d % 4])

    for d in range(min(4, dp_n)):
        gin_copy(d).start()

    for d in range(dp_n):
        gin_copy(d).wait()
        gv = (gin[d % 4].reshape(tok, dim) * scale)
        g_all[pl.ds(d * tok, tok), :] = gv.astype(jnp.bfloat16)
        if d + 4 < dp_n:
            gin_copy(d + 4).start()

    for d in range(0, dp_n, 2):
        gv = g_all[pl.ds(d * tok, 2 * tok), :].astype(jnp.float32).T
        for c in range(dp_n):
            gc = gv[c * cols:(c + 1) * cols]
            if cpad != cols:
                gc = jnp.concatenate([gc, jnp.zeros((cpad - cols, 2 * tok), jnp.float32)], axis=0)
            g_t[pl.ds(c * cpad, cpad), pl.ds(d * tok, 2 * tok)] = gc.astype(jnp.bfloat16)

    dg_wait = pltpu.make_async_remote_copy(dg_tp.at[pl.ds(0, tp_n - 1)], dg_tp.at[pl.ds(0, tp_n - 1)], snd_s.at[5],
                                           rcv_s.at[5], device_id={'dp': dp_i}, device_id_type=MESH)
    dg_wait.wait_recv()
    dg = dg_tp[0]
    for q in range(1, tp_n):
        dg = dg + dg_tp[q]
    x = hid[...].astype(jnp.float32)
    inv = lax.rsqrt(jnp.mean(x * x, axis=-1, keepdims=True) + NORM_EPS)
    dxs = dg * scale
    o_dh[...] = (inv * dxs - x * (inv * inv * inv * (jnp.sum(dxs * x, axis=-1, keepdims=True) / dim))).astype(jnp.bfloat16)
    dw = jnp.sum(dg * (x * inv), axis=0, keepdims=True)
    dw_dp[dp_i] = jnp.broadcast_to(jnp.sum(w_loc * kl, axis=0, keepdims=True), (8, 128))
    for j in range(dim // 128):
        dw_dp[dp_i, pl.ds(j, 1), :] = dw[:, j * 128:(j + 1) * 128]

    def dw_copy(dev):
        return pltpu.make_async_remote_copy(dw_dp.at[dp_i], dw_dp.at[dp_i], snd_s.at[6], rcv_s.at[6],
                                            device_id={'dp': dev}, device_id_type=MESH)

    @pl.loop(1, dp_n)
    def _(k):
        dw_copy(peer(k)).start()

    @pl.when(dp_i < last)
    def _():
        sub_copy(win).wait()

    @pl.when(dp_i == last)
    def _():
        sub_copy(tail).wait()

    row_n = 4 * tok

    def de_copy(dev, s):
        lane = pl.multiple_of(dp_i * win + s * SUB, SUB)
        return pltpu.make_async_remote_copy(de_st.at[s % 2, pl.ds(pl.multiple_of(dev * cpad, 8), cpad)],
                                            o_emb.at[:, pl.ds(lane, SUB)], de_snd.at[s % 2], de_rcv,
                                            device_id={'dp': dev}, device_id_type=MESH)

    def de_first(k, s):
        slot, (rz, ry), _ = hops(k)
        pltpu.make_async_remote_copy(de_st.at[s % 2, pl.ds(pl.multiple_of(peer(k) * cpad, 8), cpad)], rl_e.at[slot, s],
                                     de_snd.at[s % 2], re_rcv.at[slot, s], device_id={'dp': device(rz, ry, 0)},
                                     device_id_type=MESH).start()

    def de_forward(s):
        def go(k):
            slot, (rz, ry), end = hops(k)
            src = device(-rz, -ry, 0)

            @pl.when(active(src, s))
            def _():
                lane = pl.multiple_of(src * win + s * SUB, SUB)
                pltpu.make_async_remote_copy(rl_e.at[slot, s], rl_e.at[slot, s], de_snd.at[0], re_rcv.at[slot, s],
                                             device_id={'dp': dp_i}, device_id_type=MESH).wait_recv()
                pltpu.make_async_remote_copy(rl_e.at[slot, s], o_emb.at[:, pl.ds(lane, SUB)], re_snd.at[slot], de_rcv,
                                             device_id={'dp': device(*end)}, device_id_type=MESH).start()

        each_far(go)

    def de_local(s):
        lane = pl.multiple_of(dp_i * win + s * SUB, SUB)
        return pltpu.make_async_copy(de_st.at[s % 2, pl.ds(pl.multiple_of(dp_i * cpad, 8), cpad)],
                                     o_emb.at[:, pl.ds(lane, SUB)], loc_sem.at[s % 2])

    def de_wait(s):
        @pl.when(active(dp_i, s))
        def _():
            pltpu.make_async_remote_copy(de_st.at[s % 2, pl.ds(0, (dp_n - 1) * cpad)],
                                         de_st.at[s % 2, pl.ds(0, (dp_n - 1) * cpad)], de_snd.at[s % 2], de_rcv,
                                         device_id={'dp': dp_i}, device_id_type=MESH).wait_send()
            de_local(s).wait()

    for s in range(n_sub):
        if s >= 2:
            de_wait(s - 2)

        @pl.when(active(dp_i, s))
        def _(s=s):
            part = t_recv.at[pl.ds(0, dp_n - 1), :, pl.ds(s * SUB, SUB)]
            pltpu.make_async_remote_copy(part, part, t_snd.at[0], t_rcv.at[s], device_id={'dp': dp_i},
                                         device_id_type=MESH).wait_recv()

            @pl.loop(0, dp_n // 4)
            def _(b):
                rows = pl.ds(pl.multiple_of(b * row_n, row_n), row_n)
                r_blk[...] = lax.dot_general(g_all[rows, :], e_sub[pl.ds(s * SUB, SUB), :], NT,
                                             preferred_element_type=jnp.float32)
                for q in range(row_n // 32):
                    d = b * 4 + q * 32 // tok
                    off = q * 32 % tok
                    th = jnp.tanh(r_blk[pl.ds(q * 32, 32), :] * (1.0 / SOFT_CAP))
                    sv = st_all[d, pl.ds(off, 32), :]
                    p_s = jnp.exp(SOFT_CAP * th) * sv[:, 1:2]
                    p_t = jnp.exp(t_recv[d, pl.ds(off, 32), pl.ds(s * SUB, SUB)] - sv[:, 0:1])
                    dv = (p_s - p_t) * (sv[:, 2:3] / m_cnt) * (1.0 - th * th)
                    dr_blk[pl.ds(pl.multiple_of(b * row_n + q * 32, 32), 32), :] = dv.astype(jnp.bfloat16)

            @pl.loop(0, de_st.shape[1] // 256)
            def _(b):
                rows = pl.ds(pl.multiple_of(b * 256, 256), 256)
                de_st[s % 2, rows, :] = lax.dot_general(g_t[rows, :], dr_blk[...], NN,
                                                        preferred_element_type=jnp.float32)

            each_far(lambda k: de_first(k, s))
            each_near(lambda k: de_copy(peer(k), s).start())

            de_local(s).start()

        if s >= 1:
            de_forward(s - 1)

    de_forward(n_sub - 1)

    dw_wait = pltpu.make_async_remote_copy(dw_dp.at[pl.ds(0, dp_n - 1)], dw_dp.at[pl.ds(0, dp_n - 1)], snd_s.at[6],
                                           rcv_s.at[6], device_id={'dp': dp_i}, device_id_type=MESH)
    dw_wait.wait_recv()
    tot = dw_dp[0]
    for d in range(1, dp_n):
        tot = tot + dw_dp[d]
    o_dw[...] = tot

    ga_wait = pltpu.make_async_remote_copy(gbuf.at[pl.ds(0, chips - 1), 0, 0], gbuf.at[pl.ds(0, chips - 1), 0, 0],
                                           snd_s.at[0], rcv_s.at[0], device_id={'dp': dp_i}, device_id_type=MESH)
    for w in (ga_wait, gb_wait, st_wait, sd_wait, dg_wait, dw_wait):
        w.wait_send()

    tail_n = -(-tail // SUB)

    def drain(ref, sem):
        pltpu.make_async_remote_copy(ref, ref, sem, t_rcv.at[0], device_id={'dp': dp_i}, device_id_type=MESH).wait_send()

    def t_near_drain(k):
        dev = peer(k)
        pl.when(dev < last)(lambda: drain(t_stage.at[:, pl.ds(0, win)], t_snd.at[k]))
        pl.when(dev == last)(lambda: drain(t_stage.at[:, pl.ds(0, tail_n * SUB)], t_snd.at[k]))

    def far_drain(k):
        slot, (rz, ry), end = hops(k)
        dev = device(*end)
        src = device(-rz, -ry, 0)
        pl.when(peer(k) <= last)(lambda: drain(t_stage.at[:, pl.ds(0, win)], t_snd.at[k]))
        pl.when(dev < last)(lambda: drain(rl_t.at[slot], rt_snd.at[slot]))
        pl.when(dev == last)(lambda: drain(rl_t.at[slot, :, pl.ds(0, tail_n * SUB)], rt_snd.at[slot]))
        pl.when(src < last)(lambda: drain(rl_e.at[slot], re_snd.at[slot]))
        pl.when(src == last)(lambda: drain(rl_e.at[slot, pl.ds(0, tail_n)], re_snd.at[slot]))

    each_near(t_near_drain)
    each_far(far_drain)

    for s in range(max(0, n_sub - 2), n_sub):
        de_wait(s)

    total = sum(n_act(s) for s in range(n_sub))

    def de_drain(n):
        part = o_emb.at[:, pl.ds(0, n * SUB)]
        pltpu.make_async_remote_copy(part, part, de_snd.at[0], de_rcv, device_id={'dp': dp_i},
                                     device_id_type=MESH).wait_recv()

    @pl.when(dp_i < last)
    def _():
        de_drain(total - n_sub)

    @pl.when(dp_i == last)
    def _():
        de_drain(total - tail_n)

    @pl.when(dp_i > last)
    def _():
        de_drain(total)


def solution(mesh):
    tp_n, dp_n = mesh.shape['tp'], mesh.shape['dp']
    ny = 4 if dp_n >= 32 else 1

    def device_fn(hid_loc, norm_w, emb_loc, teach_loc, mask_loc):
        tok, dim = hid_loc.shape
        vloc = emb_loc.shape[0]
        win = -(-vloc // (dp_n * SUB)) * SUB
        n_ch = -(-vloc // win)
        cols = dim // dp_n
        cpad = -(-cols // 8) * 8
        rq = tok // tp_n
        f32, bf16 = jnp.float32, jnp.bfloat16
        vm, dma = pltpu.VMEM, pltpu.SemaphoreType.DMA
        any_s, vm_s = pl.BlockSpec(memory_space=pl.ANY), pl.BlockSpec(memory_space=pltpu.VMEM)
        wide = n_ch * win
        nz = dp_n // 2 // ny
        n_rl = 2 * (nz * ny - (nz - (nz == 4)) * (ny - (ny == 4)))
        o_emb, o_dh, o_dw, _ = pl.pallas_call(
            functools.partial(body, (tp_n, dp_n, ny)),
            out_shape=(jax.ShapeDtypeStruct((cpad, wide), f32), jax.ShapeDtypeStruct((tok, dim), bf16),
                       jax.ShapeDtypeStruct((8, 128), f32),
                       jax.ShapeDtypeStruct((dp_n // 2, 2, tp_n, rq, dim), f32)),
            in_specs=[vm_s, vm_s, vm_s, any_s, any_s],
            out_specs=(any_s, vm_s, vm_s, any_s),
            scratch_shapes=[
                vm((tok, wide), f32), vm((tok, wide), f32), vm((dp_n, tok, win), f32), vm((2, 16, vloc), bf16),
                vm((SLOTS, win, dim), bf16), vm((win, dim), bf16), vm((dp_n * tok, dim), bf16),
                vm((dp_n * cpad, dp_n * tok), bf16), vm((4, tp_n, rq, dim), f32), vm((tok, win), bf16),
                vm((4 * tok, SUB), f32), vm((dp_n * tok, SUB), bf16), vm((2, dp_n * cpad, SUB), f32),
                vm((n_rl, tok, win), f32), vm((n_rl, win // SUB, cpad, SUB), f32),
                vm((tok, 128), f32), vm((4, tok, 128), f32), vm((tp_n, tok, 128), f32), vm((8, 128), f32),
                vm((dp_n, 8, 128), f32), vm((dp_n, tok, 128), f32), vm((tp_n, tok, dim), f32),
                vm((dp_n, 8, 128), f32), vm((tp_n, rq, dim), f32), vm((tok, dim), bf16),
                dma((2,)), dma((SLOTS,)), dma, dma, dma((4,)), dma((2,)), dma((7,)), dma((7,)),
                dma((dp_n,)), dma((win // SUB,)), dma((2,)), dma,
                dma((n_rl,)), dma((n_rl,)), dma((n_rl, win // SUB)), dma((n_rl,)),
            ],
            compiler_params=pltpu.CompilerParams(collective_id=0, has_side_effects=True,
                                                 vmem_limit_bytes=67_000_000),
            name='head',
        )(hid_loc, norm_w.reshape(1, dim), mask_loc.astype(f32).reshape(tok, 1), emb_loc, teach_loc)
        return o_dw[7, 0], o_dh, o_emb[:cols, :vloc].T, o_dw.reshape(-1)[:dim]

    return jax.shard_map(device_fn, mesh=mesh, in_specs=(P('dp', None), P(None), P('tp', None), P('dp', 'tp'), P('dp')),
                         out_specs=(P(), P('dp', None), P('tp', 'dp'), P(None)), check_vma=False)
```

```python
import functools

import jax
import jax.numpy as jnp
from jax import lax
from jax.experimental import pallas as pl
from jax.experimental.pallas import tpu as pltpu
from jax.sharding import PartitionSpec as P

SOFT_CAP = 30.0
NORM_EPS = 1e-6
SUB = 256
ODD = (1, 3)
CORES = (0, 1)
SLOTS = 3
MESH = pl.DeviceIdType.MESH
NT = (((1,), (1,)), ((), ()))
NN = (((1,), (0,)), ((), ()))


def halves(j):
    return j // 2, j % 2


def way_of(d):
    return 1 - 2 * d


def m8(o, j):
    return o * 8 + j


def m2(o, dc):
    return o * 2 + dc


def body(cfg, hid, nw, mask, emb, teach, o_emb, o_dh, o_dw, gbuf, w1, r_a, r_b,
         t_stage, th_buf, t_recv, tb, e_slot, e_sub, g_all, g_t, gin, dr_loc, r_blk, dr_blk, de_st,
         e_1, e_a, e_b, mc_dp, m_buf, acc, st_tp, st_t, st_dp, st_all, dg_tp, dw_dp, xs_buf, gl_buf,
         tb_sem, es_sem, sub_sem, gl_sem, gin_sem, loc_sem, snd_s, rcv_s, t_rcv, de_snd, de_rcv, e1_rcv, ea_rcv, eb_rcv, e1_snd, e2_snd, eb_snd,
         w1_rcv, ra_rcv, rb_rcv, s1_snd, sa_snd, s2_snd, sb_snd):
    tp_n, dp_n, ny = cfg
    tok, dim = hid.shape
    vloc = emb.shape[0]
    win = t_recv.shape[2]
    n_sub = win // SUB
    n_ch = t_stage.shape[1] // win
    tail = vloc - (n_ch - 1) * win
    chips = dp_n // 2
    nz = chips // ny
    rq = tok // tp_n
    cpad = de_st.shape[1] // dp_n
    cols = dim // dp_n
    last = n_ch - 1
    tail_n = -(-tail // SUB)
    tp_i = lax.axis_index('tp')
    dp_i = lax.axis_index('dp')
    chip = dp_i // 2
    core = dp_i % 2

    zc, yc = chip // ny, chip % ny
    a_c, b_c = zc + core * (yc - zc), yc + core * (zc - yc)
    sa, sb = ny - core * (ny - 1), 1 + core * (ny - 1)

    def dev_ab(oa, ob, dc):
        return 2 * (((a_c + oa + 4) % 4) * sa + ((b_c + ob + 4) % 4) * sb) + (core + dc) % 2

    def dev_a(oa):
        return dev_ab(oa, 0, 0)

    def dev_b(ob):
        return dev_ab(0, ob, 0)

    def peer(k):
        j = (k // 2 * 5) % chips
        return ((zc + j // ny) % nz * ny + (yc + j % ny) % ny) * 2 + (core + k % 2) % 2

    def active(dev, s):
        return dev * win + s * SUB < vloc

    def n_act(s):
        return sum(1 for d in range(dp_n) if d * win + s * SUB < vloc)

    sib = chip * 2 + (core + 1) % 2

    def push(src, dst, snd, rcv, dev, axis='dp'):
        return pltpu.make_async_remote_copy(src, dst, snd, rcv, device_id={axis: dev}, device_id_type=MESH)

    def got(ref, sem):
        push(ref, ref, gl_sem, sem, dp_i).wait_recv()

    def sent(ref, sem):
        push(ref, ref, sem, gl_sem, dp_i).wait_send()

    def to_plane(buf, ch):
        @pl.loop(1, dp_n)
        def _(k):
            push(buf.at[dp_i], buf.at[dp_i], snd_s.at[ch], rcv_s.at[ch], peer(k)).start()

    def to_tp(ref, ch):
        @pl.loop(1, tp_n)
        def _(k):
            push(ref, ref, snd_s.at[ch], rcv_s.at[ch], (tp_i + k) % tp_n, 'tp').start()

    def others(buf):
        return buf.at[pl.ds(0, buf.shape[0] - 1)]

    barrier = pltpu.get_barrier_semaphore()

    @pl.loop(1, dp_n)
    def _(k):
        pl.semaphore_signal(barrier, inc=1, device_id={'dp': peer(k)}, device_id_type=MESH)

    @pl.loop(1, tp_n)
    def _(k):
        pl.semaphore_signal(barrier, inc=1, device_id={'tp': (tp_i + k) % tp_n}, device_id_type=MESH)

    def tb_copy(r):
        return pltpu.make_async_copy(teach.at[pl.ds(r * 16, 16)], tb.at[r % 2], tb_sem.at[r % 2])

    tb_copy(0).start()
    tb_copy(1).start()

    def e_copy(i, slot, rows):
        return pltpu.make_async_copy(emb.at[pl.ds(pl.multiple_of(i * win, 16), rows)],
                                     e_slot.at[slot, pl.ds(0, rows)], es_sem.at[slot])

    def e_start(i):
        @pl.when(i < last)
        def _():
            e_copy(i, i % SLOTS, win).start()

        @pl.when(i == last)
        def _():
            e_copy(i, i % SLOTS, tail).start()

    def e_wait(i):
        @pl.when(i < last)
        def _():
            e_copy(i, i % SLOTS, win).wait()

        @pl.when(i == last)
        def _():
            e_copy(i, i % SLOTS, tail).wait()

    def sub_copy(rows):
        return pltpu.make_async_copy(emb.at[pl.ds(pl.multiple_of(dp_i * win, 16), rows)],
                                     e_sub.at[pl.ds(0, rows)], sub_sem)

    @pl.when(dp_i < last)
    def _():
        sub_copy(win).start()

    @pl.when(dp_i == last)
    def _():
        sub_copy(tail).start()

    x = hid[...].astype(jnp.float32)
    scale = 1.0 + nw[...].astype(jnp.float32)
    inv = lax.rsqrt(jnp.mean(x * x, axis=-1, keepdims=True) + NORM_EPS)
    xs = x * inv
    xs_buf[...] = xs.reshape(tp_n, rq, dim)
    gl_buf[...] = (xs * scale).astype(jnp.bfloat16)

    own_g = pltpu.make_async_copy(xs_buf.at[tp_i], gbuf.at[chip, core, tp_i], gl_sem)
    own_g.start()

    m_loc = mask[...]
    mc_dp[dp_i] = jnp.broadcast_to(jnp.sum(m_loc, axis=0, keepdims=True), (8, 128))
    pl.semaphore_wait(barrier, dp_n - 1 + tp_n - 1)

    @pl.loop(1, chips)
    def _(k):
        push(xs_buf.at[tp_i], gbuf.at[chip, core, tp_i], snd_s.at[0], rcv_s.at[0], peer(2 * k)).start()


    to_plane(mc_dp, 7)

    pieces = [(c0, min(1024, vloc - c0)) for c0 in range(0, vloc, 1024)]
    full_p = vloc // 1024

    t_stage[:, pl.ds(vloc // 128 * 128, n_ch * win - vloc // 128 * 128)] = jnp.zeros(
        (tok, n_ch * win - vloc // 128 * 128), jnp.float32)
    for r in range(tok // 16):
        tb_copy(r).wait()
        rows = pl.ds(r * 16, 16)

        def conv(c0, width, mx):
            v = tb[r % 2, :, pl.ds(c0, width)].astype(jnp.float32)
            t_stage[rows, pl.ds(c0, width)] = v
            return v

        def step(i, mx):
            v = conv(pl.multiple_of(i * 1024, 128), 1024, mx)
            for q in range(8):
                mx = jnp.maximum(mx, v[:, q * 128:(q + 1) * 128])
            return mx

        mx = lax.fori_loop(0, full_p, step, jnp.full((16, 128), -jnp.inf, jnp.float32))
        m1 = jnp.max(mx, axis=-1, keepdims=True)
        if full_p * 1024 < vloc:
            v = conv(full_p * 1024, vloc - full_p * 1024, None)
            m1 = jnp.maximum(m1, jnp.max(v, axis=-1, keepdims=True))
        m_buf[rows, :] = jnp.broadcast_to(m1, (16, 128))
        if r + 2 < tok // 16:
            tb_copy(r + 2).start()

    for i in range(SLOTS):
        e_start(i)

    def t_win(dev):
        return t_stage.at[:, pl.ds(pl.multiple_of(dev * win, SUB), win)]

    def two_first(j):
        dest = dev_ab(2, *halves(j))
        hop = dev_a(way_of(j // 4))
        pl.when(dest <= last)(lambda: push(t_win(dest), r_a.at[j], s1_snd.at[16 + j], ra_rcv.at[j], hop).start())

    def one_first(o, j):
        dest = dev_ab(o, *halves(j))

        @pl.when(dest <= last)
        def _():
            pl.when(j < 2)(lambda: push(t_win(dest), t_recv.at[dp_i], s1_snd.at[m8(o, j)], t_rcv, dest).start())
            pl.when(j >= 2)(lambda: push(t_win(dest), w1.at[o, j], s1_snd.at[m8(o, j)], w1_rcv.at[m8(o, j)],
                                         dev_a(o)).start())

    def two_second(j):
        sign = way_of(j // 4)
        dest = dev_ab(sign, *halves(j))

        @pl.when(dest <= last)
        def _():
            got(r_a.at[j], ra_rcv.at[j])
            pl.when(j < 2)(lambda: push(r_a.at[j], t_recv.at[dev_a(-sign)], sa_snd.at[j], t_rcv, dest).start())
            pl.when(j >= 2)(lambda: push(r_a.at[j], w1.at[2, j], sa_snd.at[j], w1_rcv.at[16 + j],
                                         dev_a(sign)).start())

    def across(o, j):
        db, dc = halves(j)
        dest = dev_ab(0, db, dc)

        @pl.when(dest <= last)
        def _():
            if o == 0:
                src = t_win(dest)
            else:
                src = w1.at[o, j]
                got(src, w1_rcv.at[m8(o, j)])
            pl.when(db != 2)(lambda: push(src, t_recv.at[dev_a(-o)], s2_snd.at[m8(o, j)], t_rcv, dest).start())
            pl.when(db == 2)(lambda: push(src, r_b.at[m2(o, dc)], s2_snd.at[m8(o, j)], rb_rcv.at[m2(o, dc)],
                                          dev_b(way_of(dc))).start())

    def across_second(o, dc):
        sign = way_of(dc)
        dest = dev_ab(0, sign, dc)

        @pl.when(dest <= last)
        def _():
            got(r_b.at[m2(o, dc)], rb_rcv.at[m2(o, dc)])
            push(r_b.at[m2(o, dc)], t_recv.at[dev_ab(-o, -sign, 0)], sb_snd.at[m2(o, dc)], t_rcv, dest).start()

    @pl.loop(0, 4)
    def _(j):
        two_first(j)
        two_first(j + 4)

    @pl.loop(0, 8)
    def _(j):
        one_first(1, j)
        one_first(3, j)

    pl.when(sib <= last)(lambda: push(t_win(sib), t_recv.at[dp_i], s1_snd.at[1], t_rcv, sib).start())

    @pl.when(dp_i <= last)
    def _():
        t_recv[dp_i] = t_stage[:, pl.ds(pl.multiple_of(dp_i * win, SUB), win)]

    acc[...] = jnp.zeros_like(acc)
    lanes = lax.broadcasted_iota(jnp.int32, (tok, 128), 1)

    @pl.loop(0, n_ch)
    def _(i):
        e_wait(i)
        base = pl.multiple_of(i * win, SUB)
        th_buf[:, pl.ds(base, win)] = lax.dot_general(gl_buf[...], e_slot[i % SLOTS], NT,
                                                      preferred_element_type=jnp.float32)

        @pl.when(i + SLOTS < n_ch)
        def _():
            e_start(i + SLOTS)

        m_l = m_buf[...]
        a_s, a_1, a_2, a_x = acc[0], acc[1], acc[2], acc[3]
        for q in range(win // 128):
            at = pl.ds(pl.multiple_of(base + q * 128, 128), 128)
            th = jnp.tanh(th_buf[:, at] * (1.0 / SOFT_CAP))
            th_buf[:, at] = th
            z = SOFT_CAP * th
            ok = base + q * 128 + lanes < vloc
            e_s = jnp.where(ok, jnp.exp(z), 0.0)
            sh = t_stage[:, at] - m_l
            e_t = jnp.where(ok, jnp.exp(sh), 0.0)
            sh = jnp.where(ok, sh, 0.0)
            a_s = a_s + e_s
            a_1 = a_1 + e_t
            a_2 = a_2 + e_t * sh
            a_x = a_x + e_t * jnp.where(ok, z, 0.0)
        acc[0] = a_s
        acc[1] = a_1
        acc[2] = a_2
        acc[3] = a_x

    for i in range(SLOTS):
        e_start(i)

    parts = [m_buf[:, 0:1]] + [jnp.sum(acc[j], axis=-1, keepdims=True) for j in (1, 2, 3, 0)]
    tile = jnp.zeros((tok, 128), jnp.float32)
    for j, v in enumerate(parts):
        tile = jnp.where(lanes == j, v, tile)
    st_tp[tp_i] = tile

    to_tp(st_tp.at[tp_i], 2)
    got(others(st_tp), rcv_s.at[2])
    t_max = st_tp[0][:, 0:1]
    for q in range(1, tp_n):
        t_max = jnp.maximum(t_max, st_tp[q][:, 0:1])
    s_1 = s_2 = s_x = s_s = jnp.zeros((tok, 1), jnp.float32)
    for q in range(tp_n):
        v = st_tp[q]
        shift = v[:, 0:1] - t_max
        fac = jnp.exp(shift)
        s_1 = s_1 + fac * v[:, 1:2]
        s_2 = s_2 + fac * (v[:, 2:3] + shift * v[:, 1:2])
        s_x = s_x + fac * v[:, 3:4]
        s_s = s_s + v[:, 4:5]
    log_1 = jnp.log(s_1)
    kl = (s_2 - s_x) / s_1 - log_1 + jnp.log(s_s)
    lse_t = t_max + log_1
    inv_s = 1.0 / s_s
    tile = jnp.where(lanes == 0, lse_t, jnp.where(lanes == 1, inv_s, jnp.where(lanes == 2, m_loc, 0.0)))
    tile = jnp.concatenate([tile, jnp.zeros((128 - tok, 128), jnp.float32)], axis=0).T
    st_dp[dp_i] = tile[0:8]

    to_plane(st_dp, 4)

    own_g.wait()
    a_part = gbuf.at[pl.ds(0, chips - 1), 0, 0]
    got(a_part, rcv_s.at[0])
    to_tp(gbuf.at[:, core, tp_i], 1)

    @pl.loop(0, 8)
    def _(j):
        two_second(j)

    @pl.loop(2, 8)
    def _(j):
        across(0, j)

    got(others(mc_dp), rcv_s.at[7])
    m_cnt = jnp.sum(mc_dp[...], axis=0)[0:1, 0:1]
    w_loc = m_loc / m_cnt

    dg_tp[tp_i] = jnp.zeros((tok, dim), jnp.float32)

    @pl.loop(0, n_ch)
    def _(i):
        e_wait(i)
        base = pl.multiple_of(i * win, SUB)
        for q in range(win // 128):
            at = pl.ds(pl.multiple_of(base + q * 128, 128), 128)
            th = th_buf[:, at]
            p_s = jnp.exp(SOFT_CAP * th) * inv_s
            p_t = jnp.exp(t_stage[:, at] - lse_t)
            d = (p_s - p_t) * w_loc * (1.0 - th * th)
            ok = base + q * 128 + lanes < vloc
            dr_loc[:, pl.ds(q * 128, 128)] = jnp.where(ok, d, 0.0).astype(jnp.bfloat16)
        dg_tp[tp_i] += lax.dot_general(dr_loc[...], e_slot[i % SLOTS], NN, preferred_element_type=jnp.float32)

        @pl.when(i + SLOTS < n_ch)
        def _():
            e_start(i + SLOTS)

    to_tp(dg_tp.at[tp_i], 5)

    for o in ODD:
        @pl.loop(2, 8)
        def _(j, o=o):
            across(o, j)

    b_part = gbuf.at[:, 0, pl.ds(0, tp_n - 1)]
    got(b_part, rcv_s.at[1])
    gc_copy = push(gbuf.at[:, core], gbuf.at[:, core], snd_s.at[3], rcv_s.at[3], sib)
    gc_copy.start()

    for o in (2,):
        @pl.loop(2, 8)
        def _(j, o=o):
            across(o, j)

    gc_copy.wait()

    def gin_copy(d):
        return pltpu.make_async_copy(gbuf.at[d // 2, d % 2], gin.at[d % 4], gin_sem.at[d % 4])

    for d in range(min(4, dp_n)):
        gin_copy(d).start()

    for d in range(dp_n):
        gin_copy(d).wait()
        gv = (gin[d % 4].reshape(tok, dim) * scale)
        g_all[pl.ds(d * tok, tok), :] = gv.astype(jnp.bfloat16)
        if d + 4 < dp_n:
            gin_copy(d + 4).start()

    for d in range(0, dp_n, 2):
        gv = g_all[pl.ds(d * tok, 2 * tok), :].astype(jnp.float32).T
        for c in range(dp_n):
            gc = gv[c * cols:(c + 1) * cols]
            if cpad != cols:
                gc = jnp.concatenate([gc, jnp.zeros((cpad - cols, 2 * tok), jnp.float32)], axis=0)
            g_t[pl.ds(c * cpad, cpad), pl.ds(d * tok, 2 * tok)] = gc.astype(jnp.bfloat16)

    got(others(dg_tp), rcv_s.at[5])
    dg = dg_tp[0]
    for q in range(1, tp_n):
        dg = dg + dg_tp[q]
    x = hid[...].astype(jnp.float32)
    inv = lax.rsqrt(jnp.mean(x * x, axis=-1, keepdims=True) + NORM_EPS)
    dxs = dg * scale
    o_dh[...] = (inv * dxs - x * (inv * inv * inv * (jnp.sum(dxs * x, axis=-1, keepdims=True) / dim))).astype(jnp.bfloat16)
    dw = jnp.sum(dg * (x * inv), axis=0, keepdims=True)
    dw_dp[dp_i] = jnp.broadcast_to(jnp.sum(w_loc * kl, axis=0, keepdims=True), (8, 128))
    for j in range(dim // 128):
        dw_dp[dp_i, pl.ds(j, 1), :] = dw[:, j * 128:(j + 1) * 128]

    to_plane(dw_dp, 6)

    got(others(st_dp), rcv_s.at[4])

    @pl.loop(0, dp_n)
    def _(d):
        v = jnp.concatenate([st_dp[d], jnp.zeros((120, 128), jnp.float32)], axis=0).T
        st_all[d] = v[0:tok]

    for o in (0, 1, 3, 2):
        for dc in CORES:
            across_second(o, dc)

    @pl.when(dp_i < last)
    def _():
        sub_copy(win).wait()

    @pl.when(dp_i == last)
    def _():
        sub_copy(tail).wait()

    row_n = 4 * tok

    def de_src(dev, s):
        return de_st.at[s % 2, pl.ds(pl.multiple_of(dev * cpad, 8), cpad)]

    def de_dst(origin, s):
        return o_emb.at[:, pl.ds(pl.multiple_of(origin * win + s * SUB, SUB), SUB)]

    def de_local(s):
        return pltpu.make_async_copy(de_src(dp_i, s), de_dst(dp_i, s), loc_sem.at[s % 2])

    def de_first(s):
        snd = de_snd.at[s % 2]

        @pl.loop(0, 4)
        def _(j):
            for way in CORES:
                dest = dev_ab(2, *halves(j + 4 * way))
                push(de_src(dest, s), e_a.at[way, s, j], snd, ea_rcv.at[way, s], dev_a(way_of(way))).start()

        @pl.loop(0, 8)
        def _(j):
            for o in ODD:
                dest = dev_ab(o, *halves(j))
                src = de_src(dest, s)
                pl.when(j < 2)(lambda: push(src, de_dst(dp_i, s), snd, de_rcv, dest).start())
                pl.when(j >= 2)(lambda: push(src, e_1.at[o, s, j - 2], snd, e1_rcv.at[o, s], dev_a(o)).start())

        push(de_src(sib, s), de_dst(dp_i, s), snd, de_rcv, sib).start()
        de_turn(0, s, snd)
        de_local(s).start()

    def de_turn(o, s, snd):
        @pl.loop(2, 8)
        def _(j):
            db, dc = halves(j)
            dest = dev_ab(0, db, dc)
            src = e_1.at[o, s, j - 2] if o else de_src(dest, s)
            pl.when(db != 2)(lambda: push(src, de_dst(dev_a(-o), s), snd, de_rcv, dest).start())
            pl.when(db == 2)(lambda: push(src, e_b.at[o, dc, s], snd, eb_rcv.at[o, dc, s],
                                          dev_b(way_of(dc))).start())

    def de_two(s):
        for way in CORES:
            sign = way_of(way)
            origin = dev_a(-sign)

            @pl.when(active(origin, s))
            def _():
                got(e_a.at[way, s], ea_rcv.at[way, s])

                @pl.loop(0, 4)
                def _(j):
                    jj = j + 4 * way
                    dest = dev_ab(sign, *halves(jj))
                    src, snd = e_a.at[way, s, j], e2_snd.at[way]
                    pl.when(jj < 2)(lambda: push(src, de_dst(origin, s), snd, de_rcv, dest).start())
                    pl.when(jj >= 2)(lambda: push(src, e_1.at[2, s, jj - 2], snd, e1_rcv.at[2, s],
                                                  dev_a(sign)).start())

    def de_across(o, s):
        @pl.when(active(dev_a(-o), s))
        def _():
            got(e_1.at[o, s], e1_rcv.at[o, s])
            de_turn(o, s, e1_snd.at[o])

    def de_last(o, s):
        for dc in CORES:
            sign = way_of(dc)
            origin = dev_ab(-o, -sign, 0)

            @pl.when(active(origin, s))
            def _():
                src = e_b.at[o, dc, s]
                got(src, eb_rcv.at[o, dc, s])
                push(src, de_dst(origin, s), eb_snd.at[o, dc], de_rcv, dev_ab(0, sign, dc)).start()

    def de_step(k):
        def run(f, s, *o):
            if 0 <= s < n_sub:
                f(*o, s)

        run(de_two, k - 1)
        run(de_across, k - 1, 1)
        run(de_across, k - 1, 3)
        run(de_across, k - 2, 2)
        for o in (0, 1, 3):
            run(de_last, k - 2, o)
        run(de_last, k - 3, 2)

    def de_wait(s):
        @pl.when(active(dp_i, s))
        def _():
            sent(de_st.at[s % 2, pl.ds(0, (dp_n - 1) * cpad)], de_snd.at[s % 2])
            de_local(s).wait()

    pl.when(dp_i <= last)(lambda: got(t_recv.at[pl.ds(0, dp_n - 1)], t_rcv))

    for s in range(n_sub):
        if s >= 2:
            de_wait(s - 2)

        @pl.when(active(dp_i, s))
        def _(s=s):
            @pl.loop(0, dp_n // 4)
            def _(b):
                rows = pl.ds(pl.multiple_of(b * row_n, row_n), row_n)
                r_blk[...] = lax.dot_general(g_all[rows, :], e_sub[pl.ds(s * SUB, SUB), :], NT,
                                             preferred_element_type=jnp.float32)
                for q in range(row_n // 32):
                    d = b * 4 + q * 32 // tok
                    off = q * 32 % tok
                    th = jnp.tanh(r_blk[pl.ds(q * 32, 32), :] * (1.0 / SOFT_CAP))
                    sv = st_all[d, pl.ds(off, 32), :]
                    p_s = jnp.exp(SOFT_CAP * th) * sv[:, 1:2]
                    p_t = jnp.exp(t_recv[d, pl.ds(off, 32), pl.ds(s * SUB, SUB)] - sv[:, 0:1])
                    dv = (p_s - p_t) * (sv[:, 2:3] / m_cnt) * (1.0 - th * th)
                    dr_blk[pl.ds(pl.multiple_of(b * row_n + q * 32, 32), 32), :] = dv.astype(jnp.bfloat16)

            @pl.loop(0, de_st.shape[1] // 256)
            def _(b):
                rows = pl.ds(pl.multiple_of(b * 256, 256), 256)
                de_st[s % 2, rows, :] = lax.dot_general(g_t[rows, :], dr_blk[...], NN,
                                                        preferred_element_type=jnp.float32)

            de_first(s)

        de_step(s)

    for s in range(n_sub, n_sub + 3):
        de_step(s)

    got(others(dw_dp), rcv_s.at[6])
    tot = dw_dp[0]
    for d in range(1, dp_n):
        tot = tot + dw_dp[d]
    o_dw[...] = tot

    sent(a_part, snd_s.at[0])
    sent(b_part, snd_s.at[1])
    for buf, ch in ((st_tp, 2), (st_dp, 4), (dg_tp, 5), (dw_dp, 6), (mc_dp, 7)):
        sent(others(buf), snd_s.at[ch])

    one = t_recv.at[0]

    @pl.loop(0, 8)
    def _(j):
        for o in (1, 2, 3):
            pl.when(dev_ab(o, *halves(j)) <= last)(lambda o=o: sent(one, s1_snd.at[m8(o, j)]))
        pl.when(dev_ab(way_of(j // 4), *halves(j)) <= last)(lambda: sent(one, sa_snd.at[j]))

    pl.when(sib <= last)(lambda: sent(one, s1_snd.at[1]))

    @pl.loop(2, 8)
    def _(j):
        for o in range(4):
            pl.when(dev_ab(0, *halves(j)) <= last)(lambda o=o: sent(one, s2_snd.at[m8(o, j)]))

    for o in range(4):
        for dc in CORES:
            pl.when(dev_ab(0, way_of(dc), dc) <= last)(lambda o=o, dc=dc: sent(one, sb_snd.at[m2(o, dc)]))

    def e_sent(origin, part, sem):
        pl.when(origin < last)(lambda: sent(part(n_sub), sem))
        pl.when(origin == last)(lambda: sent(part(tail_n), sem))

    for way in CORES:
        e_sent(dev_ab(2 * way - 1, 0, 0), lambda n, way=way: e_a.at[way, pl.ds(0, n)], e2_snd.at[way])
    for o in range(4):
        if o:
            e_sent(dev_a(-o), lambda n, o=o: e_1.at[o, pl.ds(0, n)], e1_snd.at[o])
        for dc in CORES:
            e_sent(dev_ab(-o, 2 * dc - 1, 0), lambda n, o=o, dc=dc: e_b.at[o, dc, pl.ds(0, n)], eb_snd.at[o, dc])

    for s in range(max(0, n_sub - 2), n_sub):
        de_wait(s)

    total = sum(n_act(s) for s in range(n_sub))

    def de_drain(n):
        got(o_emb.at[:, pl.ds(0, n * SUB)], de_rcv)

    @pl.when(dp_i < last)
    def _():
        de_drain(total - n_sub)

    @pl.when(dp_i == last)
    def _():
        de_drain(total - tail_n)

    @pl.when(dp_i > last)
    def _():
        de_drain(total)


def solution(mesh):
    tp_n, dp_n = mesh.shape['tp'], mesh.shape['dp']
    ny = 4 if dp_n >= 32 else 1

    def device_fn(hid_loc, norm_w, emb_loc, teach_loc, mask_loc):
        tok, dim = hid_loc.shape
        vloc = emb_loc.shape[0]
        win = -(-vloc // (dp_n * SUB)) * SUB
        n_ch = -(-vloc // win)
        cols = dim // dp_n
        cpad = -(-cols // 8) * 8
        rq = tok // tp_n
        f32, bf16 = jnp.float32, jnp.bfloat16
        vm, dma = pltpu.VMEM, pltpu.SemaphoreType.DMA
        any_s, vm_s = pl.BlockSpec(memory_space=pl.ANY), pl.BlockSpec(memory_space=pltpu.VMEM)
        wide = n_ch * win
        n_sub = win // SUB
        o_emb, o_dh, o_dw = pl.pallas_call(
            functools.partial(body, (tp_n, dp_n, ny)),
            out_shape=(jax.ShapeDtypeStruct((cpad, wide), f32), jax.ShapeDtypeStruct((tok, dim), bf16),
                       jax.ShapeDtypeStruct((8, 128), f32),
                       jax.ShapeDtypeStruct((dp_n // 2, 2, tp_n, rq, dim), f32),
                       jax.ShapeDtypeStruct((4, 8, tok, win), f32), jax.ShapeDtypeStruct((8, tok, win), f32),
                       jax.ShapeDtypeStruct((8, tok, win), f32)),
            in_specs=[vm_s, vm_s, vm_s, any_s, any_s],
            out_specs=(any_s, vm_s, vm_s, any_s, any_s, any_s, any_s),
            scratch_shapes=[
                vm((tok, wide), f32), vm((tok, wide), f32), vm((dp_n, tok, win), f32), vm((2, 16, vloc), bf16),
                vm((SLOTS, win, dim), bf16), vm((win, dim), bf16), vm((dp_n * tok, dim), bf16),
                vm((dp_n * cpad, dp_n * tok), bf16), vm((4, tp_n, rq, dim), f32), vm((tok, win), bf16),
                vm((4 * tok, SUB), f32), vm((dp_n * tok, SUB), bf16), vm((2, dp_n * cpad, SUB), f32),
                vm((4, n_sub, 6, cpad, SUB), f32),
                vm((2, n_sub, 4, cpad, SUB), f32), vm((4, 2, n_sub, cpad, SUB), f32), vm((dp_n, 8, 128), f32),
                vm((tok, 128), f32), vm((4, tok, 128), f32), vm((tp_n, tok, 128), f32), vm((8, 128), f32),
                vm((dp_n, 8, 128), f32), vm((dp_n, tok, 128), f32), vm((tp_n, tok, dim), f32),
                vm((dp_n, 8, 128), f32), vm((tp_n, rq, dim), f32), vm((tok, dim), bf16),
                dma((2,)), dma((SLOTS,)), dma, dma, dma((4,)), dma((2,)), dma((8,)), dma((8,)),
                dma, dma((2,)), dma, dma((4, n_sub)), dma((2, n_sub)), dma((4, 2, n_sub)), dma((4,)), dma((2,)),
                dma((4, 2)),
                dma((32,)), dma((8,)), dma((8,)), dma((32,)), dma((8,)), dma((32,)), dma((8,)),
            ],
            compiler_params=pltpu.CompilerParams(collective_id=0, has_side_effects=True,
                                                 vmem_limit_bytes=67_000_000),
            name='head',
        )(hid_loc, norm_w.reshape(1, dim), mask_loc.astype(f32).reshape(tok, 1), emb_loc, teach_loc)[:3]
        return o_dw[7, 0], o_dh, o_emb[:cols, :vloc].T, o_dw.reshape(-1)[:dim]

    return jax.shard_map(device_fn, mesh=mesh, in_specs=(P('dp', None), P(None), P('tp', None), P('dp', 'tp'), P('dp')),
                         out_specs=(P(), P('dp', None), P('tp', 'dp'), P(None)), check_vma=False)
```

```python
import functools

import jax
import jax.numpy as jnp
from jax import lax
from jax.experimental import pallas as pl
from jax.experimental.pallas import tpu as pltpu
from jax.sharding import PartitionSpec as P

SOFT_CAP = 30.0
NORM_EPS = 1e-6
SUB = 256
ODD = (1, 3)
CORES = (0, 1)
SLOTS = 3
MESH = pl.DeviceIdType.MESH
NT = (((1,), (1,)), ((), ()))
NN = (((1,), (0,)), ((), ()))


def col(v, j):
    return v[:, j:j + 1]


def halves(j):
    return j // 2, j % 2


def way_of(d):
    return 1 - 2 * d


def m8(o, j):
    return o * 8 + j


def m2(o, dc):
    return o * 2 + dc


def body(cfg, hid, nw, mask, emb, teach, o_emb, o_dh, o_dw, gbuf, w1, r_a, r_b,
         t_stage, th_buf, t_recv, tb, e_slot, e_sub, g_all, g_t, gin, dr_loc, r_blk, dr_blk, de_st,
         e_1, e_a, e_b, mc_dp, m_buf, acc, st_tp, st_t, st_dp, st_all, dg_tp, dw_dp, xs_buf, gl_buf,
         tb_sem, es_sem, sub_sem, gl_sem, gin_sem, loc_sem, snd_s, rcv_s, t_rcv, de_snd, de_rcv, b_snd, b_rcv, e1_rcv, ea_rcv, eb_rcv, e1_snd, e2_snd, eb_snd,
         w1_rcv, ra_rcv, rb_rcv, s1_snd, sa_snd, s2_snd, sb_snd):
    tp_n, dp_n, ny = cfg
    tok, dim = hid.shape
    vloc = emb.shape[0]
    win = t_recv.shape[2]
    n_sub = win // SUB
    n_ch = t_stage.shape[1] // win
    tail = vloc - (n_ch - 1) * win
    chips = dp_n // 2
    nz = chips // ny
    rq = tok // tp_n
    cpad = de_st.shape[1] // dp_n
    cols = dim // dp_n
    last = n_ch - 1
    tail_n = -(-tail // SUB)
    tp_i = lax.axis_index('tp')
    dp_i = lax.axis_index('dp')
    chip = dp_i // 2
    core = dp_i % 2

    zc, yc = chip // ny, chip % ny
    a_c, b_c = zc + core * (yc - zc), yc + core * (zc - yc)
    sa, sb = ny - core * (ny - 1), 1 + core * (ny - 1)

    def dev_ab(oa, ob, dc):
        return 2 * (((a_c + oa + 4) % 4) * sa + ((b_c + ob + 4) % 4) * sb) + (core + dc) % 2

    def dev_a(oa):
        return dev_ab(oa, 0, 0)

    def dev_b(ob):
        return dev_ab(0, ob, 0)

    def peer(k):
        j = (k // 2 * 5) % chips
        return ((zc + j // ny) % nz * ny + (yc + j % ny) % ny) * 2 + (core + k % 2) % 2

    def active(dev, s):
        return dev * win + s * SUB < vloc

    def n_act(s):
        return sum(1 for d in range(dp_n) if d * win + s * SUB < vloc)

    sib = chip * 2 + (core + 1) % 2

    def push(src, dst, snd, rcv, dev, axis='dp'):
        return pltpu.make_async_remote_copy(src, dst, snd, rcv, device_id={axis: dev}, device_id_type=MESH)

    def got(ref, sem):
        push(ref, ref, gl_sem, sem, dp_i).wait_recv()

    def sent(ref, sem):
        push(ref, ref, sem, gl_sem, dp_i).wait_send()

    def to_plane(buf, ch):
        @pl.loop(1, dp_n)
        def _(k):
            push(buf.at[dp_i], buf.at[dp_i], snd_s.at[ch], rcv_s.at[ch], peer(k)).start()

    def to_tp(ref, ch):
        @pl.loop(1, tp_n)
        def _(k):
            push(ref, ref, snd_s.at[ch], rcv_s.at[ch], (tp_i + k) % tp_n, 'tp').start()

    def others(buf):
        return buf.at[pl.ds(0, buf.shape[0] - 1)]

    barrier = pltpu.get_barrier_semaphore()

    @pl.loop(1, dp_n)
    def _(k):
        pl.semaphore_signal(barrier, inc=1, device_id={'dp': peer(k)}, device_id_type=MESH)

    @pl.loop(1, tp_n)
    def _(k):
        pl.semaphore_signal(barrier, inc=1, device_id={'tp': (tp_i + k) % tp_n}, device_id_type=MESH)

    def tb_copy(r):
        return pltpu.make_async_copy(teach.at[pl.ds(r * 16, 16)], tb.at[r % 2], tb_sem.at[r % 2])

    tb_copy(0).start()
    tb_copy(1).start()

    def e_copy(i, slot, rows):
        return pltpu.make_async_copy(emb.at[pl.ds(pl.multiple_of(i * win, 16), rows)],
                                     e_slot.at[slot, pl.ds(0, rows)], es_sem.at[slot])

    def e_start(i):
        @pl.when(i < last)
        def _():
            e_copy(i, i % SLOTS, win).start()

        @pl.when(i == last)
        def _():
            e_copy(i, i % SLOTS, tail).start()

    def e_wait(i):
        @pl.when(i < last)
        def _():
            e_copy(i, i % SLOTS, win).wait()

        @pl.when(i == last)
        def _():
            e_copy(i, i % SLOTS, tail).wait()

    def sub_copy(rows):
        return pltpu.make_async_copy(emb.at[pl.ds(pl.multiple_of(dp_i * win, 16), rows)],
                                     e_sub.at[pl.ds(0, rows)], sub_sem)

    @pl.when(dp_i < last)
    def _():
        sub_copy(win).start()

    @pl.when(dp_i == last)
    def _():
        sub_copy(tail).start()

    x = hid[...].astype(jnp.float32)
    scale = 1.0 + nw[...].astype(jnp.float32)
    inv = lax.rsqrt(jnp.mean(x * x, axis=-1, keepdims=True) + NORM_EPS)
    xs = x * inv
    xs_buf[...] = xs.reshape(tp_n, rq, dim)
    gl_buf[...] = (xs * scale).astype(jnp.bfloat16)

    own_g = pltpu.make_async_copy(xs_buf.at[tp_i], gbuf.at[chip, core, tp_i], gl_sem)
    own_g.start()

    m_loc = mask[...]
    mc_dp[dp_i] = jnp.broadcast_to(jnp.sum(m_loc, axis=0, keepdims=True), (8, 128))
    pl.semaphore_wait(barrier, dp_n - 1 + tp_n - 1)

    @pl.loop(1, chips)
    def _(k):
        push(xs_buf.at[tp_i], gbuf.at[chip, core, tp_i], snd_s.at[0], rcv_s.at[0], peer(2 * k)).start()


    to_plane(mc_dp, 7)

    pieces = [(c0, min(1024, vloc - c0)) for c0 in range(0, vloc, 1024)]
    full_p = vloc // 1024

    t_stage[:, pl.ds(vloc // 128 * 128, n_ch * win - vloc // 128 * 128)] = jnp.zeros(
        (tok, n_ch * win - vloc // 128 * 128), jnp.float32)
    for r in range(tok // 16):
        tb_copy(r).wait()
        rows = pl.ds(r * 16, 16)

        def conv(c0, width, mx):
            v = tb[r % 2, :, pl.ds(c0, width)].astype(jnp.float32)
            t_stage[rows, pl.ds(c0, width)] = v
            return v

        def step(i, mx):
            v = conv(pl.multiple_of(i * 1024, 128), 1024, mx)
            for q in range(8):
                mx = jnp.maximum(mx, v[:, q * 128:(q + 1) * 128])
            return mx

        mx = lax.fori_loop(0, full_p, step, jnp.full((16, 128), -jnp.inf, jnp.float32))
        m1 = jnp.max(mx, axis=-1, keepdims=True)
        if full_p * 1024 < vloc:
            v = conv(full_p * 1024, vloc - full_p * 1024, None)
            m1 = jnp.maximum(m1, jnp.max(v, axis=-1, keepdims=True))
        m_buf[rows, :] = jnp.broadcast_to(m1, (16, 128))
        if r + 2 < tok // 16:
            tb_copy(r + 2).start()

    for i in range(SLOTS):
        e_start(i)

    def t_win(dev):
        return t_stage.at[:, pl.ds(pl.multiple_of(dev * win, SUB), win)]

    def two_first(j):
        dest = dev_ab(2, *halves(j))
        hop = dev_a(way_of(j // 4))
        pl.when(dest <= last)(lambda: push(t_win(dest), r_a.at[j], s1_snd.at[16 + j], ra_rcv.at[j], hop).start())

    def one_first(o, j):
        dest = dev_ab(o, *halves(j))

        @pl.when(dest <= last)
        def _():
            pl.when(j < 2)(lambda: push(t_win(dest), t_recv.at[dp_i], s1_snd.at[m8(o, j)], t_rcv, dest).start())
            pl.when(j >= 2)(lambda: push(t_win(dest), w1.at[o, j], s1_snd.at[m8(o, j)], w1_rcv.at[m8(o, j)],
                                         dev_a(o)).start())

    def two_second(j):
        sign = way_of(j // 4)
        dest = dev_ab(sign, *halves(j))

        @pl.when(dest <= last)
        def _():
            got(r_a.at[j], ra_rcv.at[j])
            pl.when(j < 2)(lambda: push(r_a.at[j], t_recv.at[dev_a(-sign)], sa_snd.at[j], t_rcv, dest).start())
            pl.when(j >= 2)(lambda: push(r_a.at[j], w1.at[2, j], sa_snd.at[j], w1_rcv.at[16 + j],
                                         dev_a(sign)).start())

    def across(o, j):
        db, dc = halves(j)
        dest = dev_ab(0, db, dc)

        @pl.when(dest <= last)
        def _():
            if o == 0:
                src = t_win(dest)
            else:
                src = w1.at[o, j]
                got(src, w1_rcv.at[m8(o, j)])
            pl.when(db != 2)(lambda: push(src, t_recv.at[dev_a(-o)], s2_snd.at[m8(o, j)], t_rcv, dest).start())
            pl.when(db == 2)(lambda: push(src, r_b.at[m2(o, dc)], s2_snd.at[m8(o, j)], rb_rcv.at[m2(o, dc)],
                                          dev_b(way_of(dc))).start())

    def across_second(o, dc):
        sign = way_of(dc)
        dest = dev_ab(0, sign, dc)

        @pl.when(dest <= last)
        def _():
            got(r_b.at[m2(o, dc)], rb_rcv.at[m2(o, dc)])
            push(r_b.at[m2(o, dc)], t_recv.at[dev_ab(-o, -sign, 0)], sb_snd.at[m2(o, dc)], t_rcv, dest).start()

    def turn(o):
        @pl.loop(2, 8)
        def _(j):
            across(o, j)

    @pl.loop(0, 4)
    def _(j):
        two_first(j)
        two_first(j + 4)

    @pl.loop(0, 8)
    def _(j):
        one_first(1, j)
        one_first(3, j)

    pl.when(sib <= last)(lambda: push(t_win(sib), t_recv.at[dp_i], s1_snd.at[1], t_rcv, sib).start())

    @pl.when(dp_i <= last)
    def _():
        t_recv[dp_i] = t_stage[:, pl.ds(pl.multiple_of(dp_i * win, SUB), win)]

    a_part = gbuf.at[pl.ds(0, chips - 1), 0, 0]
    up, down = (tp_i + 1) % tp_n, (tp_i + tp_n - 1) % tp_n
    half = chips // 2

    def rows_first():
        own_g.wait()
        got(a_part, rcv_s.at[0])
        own = gbuf.at[:, core, tp_i]
        push(own, own, b_snd.at[0], b_rcv.at[0], up, 'tp').start()
        push(own, own, b_snd.at[1], b_rcv.at[1], down, 'tp').start()

    def rows_second():
        for way in CORES:
            got(gbuf.at[:, 0, 0], b_rcv.at[way])
        lo, hi = gbuf.at[pl.ds(0, half), core, down], gbuf.at[pl.ds(half, half), core, up]
        push(lo, lo, b_snd.at[2], b_rcv.at[2], up, 'tp').start()
        push(hi, hi, b_snd.at[3], b_rcv.at[3], down, 'tp').start()

    b_half = gbuf.at[pl.ds(0, half), 0, 0]

    def rows_sibling():
        for way in CORES:
            got(b_half, b_rcv.at[2 + way])
        gc_copy.start()

    gc_copy = push(gbuf.at[:, core], gbuf.at[:, core], snd_s.at[3], rcv_s.at[3], sib)

    acc[...] = jnp.zeros_like(acc)
    lanes = lax.broadcasted_iota(jnp.int32, (tok, 128), 1)

    @pl.loop(0, n_ch)
    def _(i):
        pl.when(i == n_ch // 4)(rows_first)
        e_wait(i)
        base = pl.multiple_of(i * win, SUB)
        th_buf[:, pl.ds(base, win)] = lax.dot_general(gl_buf[...], e_slot[i % SLOTS], NT,
                                                      preferred_element_type=jnp.float32)

        @pl.when(i + SLOTS < n_ch)
        def _():
            e_start(i + SLOTS)

        m_l = m_buf[...]
        a_s, a_1, a_2, a_x = acc[0], acc[1], acc[2], acc[3]
        for q in range(win // 128):
            at = pl.ds(pl.multiple_of(base + q * 128, 128), 128)
            th = jnp.tanh(th_buf[:, at] * (1.0 / SOFT_CAP))
            th_buf[:, at] = th
            z = SOFT_CAP * th
            ok = base + q * 128 + lanes < vloc
            e_s = jnp.where(ok, jnp.exp(z), 0.0)
            sh = t_stage[:, at] - m_l
            e_t = jnp.where(ok, jnp.exp(sh), 0.0)
            sh = jnp.where(ok, sh, 0.0)
            a_s = a_s + e_s
            a_1 = a_1 + e_t
            a_2 = a_2 + e_t * sh
            a_x = a_x + e_t * jnp.where(ok, z, 0.0)
        acc[0] = a_s
        acc[1] = a_1
        acc[2] = a_2
        acc[3] = a_x

    for i in range(SLOTS):
        e_start(i)

    parts = [col(m_buf, 0)] + [jnp.sum(acc[j], axis=-1, keepdims=True) for j in (1, 2, 3, 0)]
    tile = jnp.zeros((tok, 128), jnp.float32)
    for j, v in enumerate(parts):
        tile = jnp.where(lanes == j, v, tile)
    st_tp[tp_i] = tile

    to_tp(st_tp.at[tp_i], 2)
    got(others(st_tp), rcv_s.at[2])
    t_max = col(st_tp[0], 0)
    for q in range(1, tp_n):
        t_max = jnp.maximum(t_max, col(st_tp[q], 0))
    s_1 = s_2 = s_x = s_s = jnp.zeros((tok, 1), jnp.float32)
    for q in range(tp_n):
        v = st_tp[q]
        shift = col(v, 0) - t_max
        fac = jnp.exp(shift)
        s_1 = s_1 + fac * col(v, 1)
        s_2 = s_2 + fac * (col(v, 2) + shift * col(v, 1))
        s_x = s_x + fac * col(v, 3)
        s_s = s_s + col(v, 4)
    log_1 = jnp.log(s_1)
    kl = (s_2 - s_x) / s_1 - log_1 + jnp.log(s_s)
    lse_t = t_max + log_1
    inv_s = 1.0 / s_s
    tile = jnp.where(lanes == 0, lse_t, jnp.where(lanes == 1, inv_s, jnp.where(lanes == 2, m_loc, 0.0)))
    tile = jnp.concatenate([tile, jnp.zeros((128 - tok, 128), jnp.float32)], axis=0).T
    st_dp[dp_i] = tile[0:8]

    to_plane(st_dp, 4)

    rows_second()

    @pl.loop(0, 8)
    def _(j):
        two_second(j)

    turn(0)

    got(others(mc_dp), rcv_s.at[7])
    m_cnt = jnp.sum(mc_dp[...], axis=0)[0:1, 0:1]
    w_loc = m_loc / m_cnt

    dg_tp[tp_i] = jnp.zeros((tok, dim), jnp.float32)

    @pl.loop(0, n_ch)
    def _(i):
        pl.when(i == n_ch // 3)(rows_sibling)
        pl.when(i == n_ch // 2)(lambda: turn(1))
        pl.when(i == n_ch * 2 // 3)(lambda: turn(3))
        e_wait(i)
        base = pl.multiple_of(i * win, SUB)
        for q in range(win // 128):
            at = pl.ds(pl.multiple_of(base + q * 128, 128), 128)
            th = th_buf[:, at]
            p_s = jnp.exp(SOFT_CAP * th) * inv_s
            p_t = jnp.exp(t_stage[:, at] - lse_t)
            d = (p_s - p_t) * w_loc * (1.0 - th * th)
            ok = base + q * 128 + lanes < vloc
            dr_loc[:, pl.ds(q * 128, 128)] = jnp.where(ok, d, 0.0).astype(jnp.bfloat16)
        dg_tp[tp_i] += lax.dot_general(dr_loc[...], e_slot[i % SLOTS], NN, preferred_element_type=jnp.float32)

        @pl.when(i + SLOTS < n_ch)
        def _():
            e_start(i + SLOTS)

    to_tp(dg_tp.at[tp_i], 5)

    gc_copy.wait()

    def gin_copy(d):
        return pltpu.make_async_copy(gbuf.at[d // 2, d % 2], gin.at[d % 4], gin_sem.at[d % 4])

    for d in range(min(4, dp_n)):
        gin_copy(d).start()

    for d in range(dp_n):
        gin_copy(d).wait()
        gv = (gin[d % 4].reshape(tok, dim) * scale)
        g_all[pl.ds(d * tok, tok), :] = gv.astype(jnp.bfloat16)
        if d + 4 < dp_n:
            gin_copy(d + 4).start()

    for d in range(0, dp_n, 2):
        gv = g_all[pl.ds(d * tok, 2 * tok), :].astype(jnp.float32).T
        for c in range(dp_n):
            gc = gv[c * cols:(c + 1) * cols]
            if cpad != cols:
                gc = jnp.concatenate([gc, jnp.zeros((cpad - cols, 2 * tok), jnp.float32)], axis=0)
            g_t[pl.ds(c * cpad, cpad), pl.ds(d * tok, 2 * tok)] = gc.astype(jnp.bfloat16)

    turn(2)

    got(others(dg_tp), rcv_s.at[5])
    dg = dg_tp[0]
    for q in range(1, tp_n):
        dg = dg + dg_tp[q]
    x = hid[...].astype(jnp.float32)
    inv = lax.rsqrt(jnp.mean(x * x, axis=-1, keepdims=True) + NORM_EPS)
    dxs = dg * scale
    o_dh[...] = (inv * dxs - x * (inv * inv * inv * (jnp.sum(dxs * x, axis=-1, keepdims=True) / dim))).astype(jnp.bfloat16)
    dw = jnp.sum(dg * (x * inv), axis=0, keepdims=True)
    dw_dp[dp_i] = jnp.broadcast_to(jnp.sum(w_loc * kl, axis=0, keepdims=True), (8, 128))
    for j in range(dim // 128):
        dw_dp[dp_i, pl.ds(j, 1), :] = dw[:, j * 128:(j + 1) * 128]

    to_plane(dw_dp, 6)

    got(others(st_dp), rcv_s.at[4])

    @pl.loop(0, dp_n)
    def _(d):
        v = jnp.concatenate([st_dp[d], jnp.zeros((120, 128), jnp.float32)], axis=0).T
        st_all[d] = v[0:tok]

    for o in (0, 1, 3, 2):
        for dc in CORES:
            across_second(o, dc)

    @pl.when(dp_i < last)
    def _():
        sub_copy(win).wait()

    @pl.when(dp_i == last)
    def _():
        sub_copy(tail).wait()

    row_n = 4 * tok

    def de_src(dev, s):
        return de_st.at[s % 2, pl.ds(pl.multiple_of(dev * cpad, 8), cpad)]

    def de_dst(origin, s):
        return o_emb.at[:, pl.ds(pl.multiple_of(origin * win + s * SUB, SUB), SUB)]

    def de_local(s):
        return pltpu.make_async_copy(de_src(dp_i, s), de_dst(dp_i, s), loc_sem.at[s % 2])

    def de_first(s):
        snd = de_snd.at[s % 2]

        @pl.loop(0, 4)
        def _(j):
            for way in CORES:
                dest = dev_ab(2, *halves(j + 4 * way))
                push(de_src(dest, s), e_a.at[way, s, j], snd, ea_rcv.at[way, s], dev_a(way_of(way))).start()

        @pl.loop(0, 8)
        def _(j):
            for o in ODD:
                dest = dev_ab(o, *halves(j))
                src = de_src(dest, s)
                pl.when(j < 2)(lambda: push(src, de_dst(dp_i, s), snd, de_rcv, dest).start())
                pl.when(j >= 2)(lambda: push(src, e_1.at[o, s, j - 2], snd, e1_rcv.at[o, s], dev_a(o)).start())

        push(de_src(sib, s), de_dst(dp_i, s), snd, de_rcv, sib).start()
        de_turn(0, s, snd)
        de_local(s).start()

    def de_turn(o, s, snd):
        @pl.loop(2, 8)
        def _(j):
            db, dc = halves(j)
            dest = dev_ab(0, db, dc)
            src = e_1.at[o, s, j - 2] if o else de_src(dest, s)
            pl.when(db != 2)(lambda: push(src, de_dst(dev_a(-o), s), snd, de_rcv, dest).start())
            pl.when(db == 2)(lambda: push(src, e_b.at[o, dc, s], snd, eb_rcv.at[o, dc, s],
                                          dev_b(way_of(dc))).start())

    def de_two(s):
        for way in CORES:
            sign = way_of(way)
            origin = dev_a(-sign)

            @pl.when(active(origin, s))
            def _():
                got(e_a.at[way, s], ea_rcv.at[way, s])

                @pl.loop(0, 4)
                def _(j):
                    jj = j + 4 * way
                    dest = dev_ab(sign, *halves(jj))
                    src, snd = e_a.at[way, s, j], e2_snd.at[way]
                    pl.when(jj < 2)(lambda: push(src, de_dst(origin, s), snd, de_rcv, dest).start())
                    pl.when(jj >= 2)(lambda: push(src, e_1.at[2, s, jj - 2], snd, e1_rcv.at[2, s],
                                                  dev_a(sign)).start())

    def de_across(o, s):
        @pl.when(active(dev_a(-o), s))
        def _():
            got(e_1.at[o, s], e1_rcv.at[o, s])
            de_turn(o, s, e1_snd.at[o])

    def de_last(o, s):
        for dc in CORES:
            sign = way_of(dc)
            origin = dev_ab(-o, -sign, 0)

            @pl.when(active(origin, s))
            def _():
                src = e_b.at[o, dc, s]
                got(src, eb_rcv.at[o, dc, s])
                push(src, de_dst(origin, s), eb_snd.at[o, dc], de_rcv, dev_ab(0, sign, dc)).start()

    def de_step(k):
        def run(f, s, *o):
            if 0 <= s < n_sub:
                f(*o, s)

        run(de_two, k - 1)
        run(de_across, k - 1, 1)
        run(de_across, k - 1, 3)
        run(de_across, k - 2, 2)
        for o in (0, 1, 3):
            run(de_last, k - 2, o)
        run(de_last, k - 3, 2)

    def de_wait(s):
        @pl.when(active(dp_i, s))
        def _():
            sent(de_st.at[s % 2, pl.ds(0, (dp_n - 1) * cpad)], de_snd.at[s % 2])
            de_local(s).wait()

    pl.when(dp_i <= last)(lambda: got(t_recv.at[pl.ds(0, dp_n - 1)], t_rcv))

    for s in range(n_sub):
        if s >= 2:
            de_wait(s - 2)

        @pl.when(active(dp_i, s))
        def _(s=s):
            @pl.loop(0, dp_n // 4)
            def _(b):
                rows = pl.ds(pl.multiple_of(b * row_n, row_n), row_n)
                r_blk[...] = lax.dot_general(g_all[rows, :], e_sub[pl.ds(s * SUB, SUB), :], NT,
                                             preferred_element_type=jnp.float32)
                for q in range(row_n // 32):
                    d = b * 4 + q * 32 // tok
                    off = q * 32 % tok
                    th = jnp.tanh(r_blk[pl.ds(q * 32, 32), :] * (1.0 / SOFT_CAP))
                    sv = st_all[d, pl.ds(off, 32), :]
                    p_s = jnp.exp(SOFT_CAP * th) * col(sv, 1)
                    p_t = jnp.exp(t_recv[d, pl.ds(off, 32), pl.ds(s * SUB, SUB)] - col(sv, 0))
                    dv = (p_s - p_t) * (col(sv, 2) / m_cnt) * (1.0 - th * th)
                    dr_blk[pl.ds(pl.multiple_of(b * row_n + q * 32, 32), 32), :] = dv.astype(jnp.bfloat16)

            @pl.loop(0, de_st.shape[1] // 256)
            def _(b):
                rows = pl.ds(pl.multiple_of(b * 256, 256), 256)
                de_st[s % 2, rows, :] = lax.dot_general(g_t[rows, :], dr_blk[...], NN,
                                                        preferred_element_type=jnp.float32)

            de_first(s)

        de_step(s)

    for s in range(n_sub, n_sub + 3):
        de_step(s)

    got(others(dw_dp), rcv_s.at[6])
    tot = dw_dp[0]
    for d in range(1, dp_n):
        tot = tot + dw_dp[d]
    o_dw[...] = tot

    sent(a_part, snd_s.at[0])
    for way in CORES:
        sent(gbuf.at[:, 0, 0], b_snd.at[way])
        sent(b_half, b_snd.at[2 + way])
    for buf, ch in ((st_tp, 2), (st_dp, 4), (dg_tp, 5), (dw_dp, 6), (mc_dp, 7)):
        sent(others(buf), snd_s.at[ch])

    one = t_recv.at[0]

    @pl.loop(0, 8)
    def _(j):
        for o in (1, 2, 3):
            pl.when(dev_ab(o, *halves(j)) <= last)(lambda o=o: sent(one, s1_snd.at[m8(o, j)]))
        pl.when(dev_ab(way_of(j // 4), *halves(j)) <= last)(lambda: sent(one, sa_snd.at[j]))

    pl.when(sib <= last)(lambda: sent(one, s1_snd.at[1]))

    @pl.loop(2, 8)
    def _(j):
        for o in range(4):
            pl.when(dev_ab(0, *halves(j)) <= last)(lambda o=o: sent(one, s2_snd.at[m8(o, j)]))

    for o in range(4):
        for dc in CORES:
            pl.when(dev_ab(0, way_of(dc), dc) <= last)(lambda o=o, dc=dc: sent(one, sb_snd.at[m2(o, dc)]))

    def e_sent(origin, part, sem):
        pl.when(origin < last)(lambda: sent(part(n_sub), sem))
        pl.when(origin == last)(lambda: sent(part(tail_n), sem))

    for way in CORES:
        e_sent(dev_ab(2 * way - 1, 0, 0), lambda n, way=way: e_a.at[way, pl.ds(0, n)], e2_snd.at[way])
    for o in range(4):
        if o:
            e_sent(dev_a(-o), lambda n, o=o: e_1.at[o, pl.ds(0, n)], e1_snd.at[o])
        for dc in CORES:
            e_sent(dev_ab(-o, 2 * dc - 1, 0), lambda n, o=o, dc=dc: e_b.at[o, dc, pl.ds(0, n)], eb_snd.at[o, dc])

    for s in range(max(0, n_sub - 2), n_sub):
        de_wait(s)

    total = sum(n_act(s) for s in range(n_sub))

    def de_drain(n):
        got(o_emb.at[:, pl.ds(0, n * SUB)], de_rcv)

    @pl.when(dp_i < last)
    def _():
        de_drain(total - n_sub)

    @pl.when(dp_i == last)
    def _():
        de_drain(total - tail_n)

    @pl.when(dp_i > last)
    def _():
        de_drain(total)


def solution(mesh):
    tp_n, dp_n = mesh.shape['tp'], mesh.shape['dp']
    ny = 4 if dp_n >= 32 else 1

    def device_fn(hid_loc, norm_w, emb_loc, teach_loc, mask_loc):
        tok, dim = hid_loc.shape
        vloc = emb_loc.shape[0]
        win = -(-vloc // (dp_n * SUB)) * SUB
        n_ch = -(-vloc // win)
        cols = dim // dp_n
        cpad = -(-cols // 8) * 8
        rq = tok // tp_n
        f32, bf16 = jnp.float32, jnp.bfloat16
        vm, dma = pltpu.VMEM, pltpu.SemaphoreType.DMA
        any_s, vm_s = pl.BlockSpec(memory_space=pl.ANY), pl.BlockSpec(memory_space=pltpu.VMEM)
        wide = n_ch * win
        n_sub = win // SUB
        o_emb, o_dh, o_dw = pl.pallas_call(
            functools.partial(body, (tp_n, dp_n, ny)),
            out_shape=(jax.ShapeDtypeStruct((cpad, wide), f32), jax.ShapeDtypeStruct((tok, dim), bf16),
                       jax.ShapeDtypeStruct((8, 128), f32),
                       jax.ShapeDtypeStruct((dp_n // 2, 2, tp_n, rq, dim), f32),
                       jax.ShapeDtypeStruct((4, 8, tok, win), f32), jax.ShapeDtypeStruct((8, tok, win), f32),
                       jax.ShapeDtypeStruct((8, tok, win), f32)),
            in_specs=[vm_s, vm_s, vm_s, any_s, any_s],
            out_specs=(any_s, vm_s, vm_s, any_s, any_s, any_s, any_s),
            scratch_shapes=[
                vm((tok, wide), f32), vm((tok, wide), f32), vm((dp_n, tok, win), f32), vm((2, 16, vloc), bf16),
                vm((SLOTS, win, dim), bf16), vm((win, dim), bf16), vm((dp_n * tok, dim), bf16),
                vm((dp_n * cpad, dp_n * tok), bf16), vm((4, tp_n, rq, dim), f32), vm((tok, win), bf16),
                vm((4 * tok, SUB), f32), vm((dp_n * tok, SUB), bf16), vm((2, dp_n * cpad, SUB), f32),
                vm((4, n_sub, 6, cpad, SUB), f32),
                vm((2, n_sub, 4, cpad, SUB), f32), vm((4, 2, n_sub, cpad, SUB), f32), vm((dp_n, 8, 128), f32),
                vm((tok, 128), f32), vm((4, tok, 128), f32), vm((tp_n, tok, 128), f32), vm((8, 128), f32),
                vm((dp_n, 8, 128), f32), vm((dp_n, tok, 128), f32), vm((tp_n, tok, dim), f32),
                vm((dp_n, 8, 128), f32), vm((tp_n, rq, dim), f32), vm((tok, dim), bf16),
                dma((2,)), dma((SLOTS,)), dma, dma, dma((4,)), dma((2,)), dma((8,)), dma((8,)),
                dma, dma((2,)), dma, dma((4,)), dma((4,)), dma((4, n_sub)), dma((2, n_sub)), dma((4, 2, n_sub)), dma((4,)), dma((2,)),
                dma((4, 2)),
                dma((32,)), dma((8,)), dma((8,)), dma((32,)), dma((8,)), dma((32,)), dma((8,)),
            ],
            compiler_params=pltpu.CompilerParams(collective_id=0, has_side_effects=True,
                                                 vmem_limit_bytes=67_000_000),
            name='head',
        )(hid_loc, norm_w.reshape(1, dim), mask_loc.astype(f32).reshape(tok, 1), emb_loc, teach_loc)[:3]
        return o_dw[7, 0], o_dh, o_emb[:cols, :vloc].T, o_dw.reshape(-1)[:dim]

    return jax.shard_map(device_fn, mesh=mesh, in_specs=(P('dp', None), P(None), P('tp', None), P('dp', 'tp'), P('dp')),
                         out_specs=(P(), P('dp', None), P('tp', 'dp'), P(None)), check_vma=False)
```

```python
import functools

import jax
import jax.numpy as jnp
from jax import lax
from jax.experimental import pallas as pl
from jax.experimental.pallas import tpu as pltpu
from jax.sharding import PartitionSpec as P

SOFT_CAP = 30.0
NORM_EPS = 1e-6
SUB = 256
STRIP = 32
ODD = (1, 3)
CORES = (0, 1)
SLOTS = 3
MESH = pl.DeviceIdType.MESH
NT = (((1,), (1,)), ((), ()))
NN = (((1,), (0,)), ((), ()))


def col(v, j):
    return v[:, j:j + 1]


def halves(j):
    return j // 2, j % 2


def way_of(d):
    return 1 - 2 * d


def m8(o, j):
    return o * 8 + j


def m2(o, dc):
    return o * 2 + dc


def body(cfg, hid, nw, mask, emb, teach, o_emb, o_dh, o_dw, gbuf, e_1, e_a, e_b,
         t_stage, th_buf, t_recv, tb, e_slot, g_all, g_t, gin, dr_loc, r_blk, dr_blk,
         w1, r_a, r_b, mc_dp, m_buf, acc, st_tp, st_t, st_dp, st_all, dg_tp, dw_dp, xs_buf, gl_buf,
         tb_sem, es_sem, sub_sem, gl_sem, gin_sem, loc_sem, snd_s, rcv_s, t_rcv, de_snd, de_rcv, b_snd, b_rcv, e1_rcv, ea_rcv, eb_rcv, e1_snd, e2_snd, eb_snd,
         w1_rcv, ra_rcv, rb_rcv, s1_snd, sa_snd, s2_snd, sb_snd):
    tp_n, dp_n, ny = cfg
    tok, dim = hid.shape
    vloc = emb.shape[0]
    win = t_recv.shape[2]
    n_sub = win // SUB
    n_ch = t_stage.shape[1] // win
    tail = vloc - (n_ch - 1) * win
    chips = dp_n // 2
    nz = chips // ny
    rq = tok // tp_n
    cpad = o_emb.shape[0]
    cols = dim // dp_n
    last = n_ch - 1
    tail_n = -(-tail // SUB)
    tp_i = lax.axis_index('tp')
    dp_i = lax.axis_index('dp')
    chip = dp_i // 2
    core = dp_i % 2

    zc, yc = chip // ny, chip % ny
    a_c, b_c = zc + core * (yc - zc), yc + core * (zc - yc)
    sa, sb = ny - core * (ny - 1), 1 + core * (ny - 1)

    def dev_ab(oa, ob, dc):
        return 2 * (((a_c + oa + 4) % 4) * sa + ((b_c + ob + 4) % 4) * sb) + (core + dc) % 2

    def dev_a(oa):
        return dev_ab(oa, 0, 0)

    def dev_b(ob):
        return dev_ab(0, ob, 0)

    def peer(k):
        j = (k // 2 * 5) % chips
        return ((zc + j // ny) % nz * ny + (yc + j % ny) % ny) * 2 + (core + k % 2) % 2

    def active(dev, s):
        return dev * win + s * SUB < vloc

    def n_act(s):
        return sum(1 for d in range(dp_n) if d * win + s * SUB < vloc)

    sib = chip * 2 + (core + 1) % 2

    def push(src, dst, snd, rcv, dev, axis='dp'):
        return pltpu.make_async_remote_copy(src, dst, snd, rcv, device_id={axis: dev}, device_id_type=MESH)

    def got(ref, sem):
        push(ref, ref, gl_sem, sem, dp_i).wait_recv()

    def sent(ref, sem):
        push(ref, ref, sem, gl_sem, dp_i).wait_send()

    def to_plane(buf, ch):
        @pl.loop(1, dp_n)
        def _(k):
            push(buf.at[dp_i], buf.at[dp_i], snd_s.at[ch], rcv_s.at[ch], peer(k)).start()

    def to_tp(ref, ch):
        @pl.loop(1, tp_n)
        def _(k):
            push(ref, ref, snd_s.at[ch], rcv_s.at[ch], (tp_i + k) % tp_n, 'tp').start()

    def others(buf):
        return buf.at[pl.ds(0, buf.shape[0] - 1)]

    barrier = pltpu.get_barrier_semaphore()

    @pl.loop(1, dp_n)
    def _(k):
        pl.semaphore_signal(barrier, inc=1, device_id={'dp': peer(k)}, device_id_type=MESH)

    @pl.loop(1, tp_n)
    def _(k):
        pl.semaphore_signal(barrier, inc=1, device_id={'tp': (tp_i + k) % tp_n}, device_id_type=MESH)

    def tb_copy(r):
        return pltpu.make_async_copy(teach.at[pl.ds(r * 16, 16)], tb.at[r % 2], tb_sem.at[r % 2])

    tb_copy(0).start()
    tb_copy(1).start()

    def e_copy(i, slot, rows):
        return pltpu.make_async_copy(emb.at[pl.ds(pl.multiple_of(i * win, 16), rows)],
                                     e_slot.at[slot, pl.ds(0, rows)], es_sem.at[slot])

    def e_start(i):
        @pl.when(i < last)
        def _():
            e_copy(i, i % SLOTS, win).start()

        @pl.when(i == last)
        def _():
            e_copy(i, i % SLOTS, tail).start()

    def e_wait(i):
        @pl.when(i < last)
        def _():
            e_copy(i, i % SLOTS, win).wait()

        @pl.when(i == last)
        def _():
            e_copy(i, i % SLOTS, tail).wait()

    def sub_copy(rows):
        return pltpu.make_async_copy(emb.at[pl.ds(pl.multiple_of(dp_i * win, 16), rows)],
                                     e_slot.at[0, pl.ds(0, rows)], sub_sem)

    x = hid[...].astype(jnp.float32)
    scale = 1.0 + nw[...].astype(jnp.float32)
    inv = lax.rsqrt(jnp.mean(x * x, axis=-1, keepdims=True) + NORM_EPS)
    xs = x * inv
    xs_buf[...] = xs.reshape(tp_n, rq, dim)
    gl_buf[...] = (xs * scale).astype(jnp.bfloat16)

    own_g = pltpu.make_async_copy(xs_buf.at[tp_i], gbuf.at[chip, core, tp_i], gl_sem)
    own_g.start()

    m_loc = mask[...]
    mc_dp[dp_i] = jnp.broadcast_to(jnp.sum(m_loc, axis=0, keepdims=True), (8, 128))
    pl.semaphore_wait(barrier, dp_n - 1 + tp_n - 1)

    @pl.loop(1, chips)
    def _(k):
        push(xs_buf.at[tp_i], gbuf.at[chip, core, tp_i], snd_s.at[0], rcv_s.at[0], peer(2 * k)).start()


    to_plane(mc_dp, 7)

    pieces = [(c0, min(1024, vloc - c0)) for c0 in range(0, vloc, 1024)]
    full_p = vloc // 1024

    t_stage[:, pl.ds(vloc // 128 * 128, n_ch * win - vloc // 128 * 128)] = jnp.zeros(
        (tok, n_ch * win - vloc // 128 * 128), jnp.float32)
    for r in range(tok // 16):
        tb_copy(r).wait()
        rows = pl.ds(r * 16, 16)

        def conv(c0, width, mx):
            v = tb[r % 2, :, pl.ds(c0, width)].astype(jnp.float32)
            t_stage[rows, pl.ds(c0, width)] = v
            return v

        def step(i, mx):
            v = conv(pl.multiple_of(i * 1024, 128), 1024, mx)
            for q in range(8):
                mx = jnp.maximum(mx, v[:, q * 128:(q + 1) * 128])
            return mx

        mx = lax.fori_loop(0, full_p, step, jnp.full((16, 128), -jnp.inf, jnp.float32))
        m1 = jnp.max(mx, axis=-1, keepdims=True)
        if full_p * 1024 < vloc:
            v = conv(full_p * 1024, vloc - full_p * 1024, None)
            m1 = jnp.maximum(m1, jnp.max(v, axis=-1, keepdims=True))
        m_buf[rows, :] = jnp.broadcast_to(m1, (16, 128))
        if r + 2 < tok // 16:
            tb_copy(r + 2).start()

    for i in range(SLOTS):
        e_start(i)

    def t_win(dev):
        return t_stage.at[:, pl.ds(pl.multiple_of(dev * win, 128), win)]

    def two_first(j):
        dest = dev_ab(2, *halves(j))
        hop = dev_a(way_of(j // 4))
        pl.when(dest <= last)(lambda: push(t_win(dest), r_a.at[j], s1_snd.at[16 + j], ra_rcv.at[j], hop).start())

    def one_first(o, j):
        dest = dev_ab(o, *halves(j))

        @pl.when(dest <= last)
        def _():
            pl.when(j < 2)(lambda: push(t_win(dest), t_recv.at[dp_i], s1_snd.at[m8(o, j)], t_rcv, dest).start())
            pl.when(j >= 2)(lambda: push(t_win(dest), w1.at[o - 1, j - 2], s1_snd.at[m8(o, j)], w1_rcv.at[m8(o, j)],
                                         dev_a(o)).start())

    def two_second(j):
        sign = way_of(j // 4)
        dest = dev_ab(sign, *halves(j))

        @pl.when(dest <= last)
        def _():
            got(r_a.at[j], ra_rcv.at[j])
            pl.when(j < 2)(lambda: push(r_a.at[j], t_recv.at[dev_a(-sign)], sa_snd.at[j], t_rcv, dest).start())
            pl.when(j >= 2)(lambda: push(r_a.at[j], w1.at[1, j - 2], sa_snd.at[j], w1_rcv.at[16 + j],
                                         dev_a(sign)).start())

    def across(o, j):
        db, dc = halves(j)
        dest = dev_ab(0, db, dc)

        @pl.when(dest <= last)
        def _():
            if o == 0:
                src = t_win(dest)
            else:
                src = w1.at[o - 1, j - 2]
                got(src, w1_rcv.at[m8(o, j)])
            pl.when(db != 2)(lambda: push(src, t_recv.at[dev_a(-o)], s2_snd.at[m8(o, j)], t_rcv, dest).start())
            pl.when(db == 2)(lambda: push(src, r_b.at[m2(o, dc)], s2_snd.at[m8(o, j)], rb_rcv.at[m2(o, dc)],
                                          dev_b(way_of(dc))).start())

    def across_second(o, dc):
        sign = way_of(dc)
        dest = dev_ab(0, sign, dc)

        @pl.when(dest <= last)
        def _():
            got(r_b.at[m2(o, dc)], rb_rcv.at[m2(o, dc)])
            push(r_b.at[m2(o, dc)], t_recv.at[dev_ab(-o, -sign, 0)], sb_snd.at[m2(o, dc)], t_rcv, dest).start()

    def turn(o):
        @pl.loop(2, 8)
        def _(j):
            across(o, j)

    def turn_second(o):
        for dc in CORES:
            across_second(o, dc)

    @pl.loop(0, 4)
    def _(j):
        two_first(j)
        two_first(j + 4)

    @pl.loop(0, 8)
    def _(j):
        one_first(1, j)
        one_first(3, j)

    pl.when(sib <= last)(lambda: push(t_win(sib), t_recv.at[dp_i], s1_snd.at[1], t_rcv, sib).start())

    @pl.when(dp_i <= last)
    def _():
        t_recv[dp_i] = t_stage[:, pl.ds(pl.multiple_of(dp_i * win, 128), win)]

    a_part = gbuf.at[pl.ds(0, chips - 1), 0, 0]
    up, down = (tp_i + 1) % tp_n, (tp_i + tp_n - 1) % tp_n
    half = chips // 2

    def rows_first():
        own_g.wait()
        got(a_part, rcv_s.at[0])
        own = gbuf.at[:, core, tp_i]
        push(own, own, b_snd.at[0], b_rcv.at[0], up, 'tp').start()
        push(own, own, b_snd.at[1], b_rcv.at[1], down, 'tp').start()

    def rows_second():
        for way in CORES:
            got(gbuf.at[:, 0, 0], b_rcv.at[way])
        lo, hi = gbuf.at[pl.ds(0, half), core, down], gbuf.at[pl.ds(half, half), core, up]
        push(lo, lo, b_snd.at[2], b_rcv.at[2], up, 'tp').start()
        push(hi, hi, b_snd.at[3], b_rcv.at[3], down, 'tp').start()

    b_half = gbuf.at[pl.ds(0, half), 0, 0]

    def rows_sibling():
        for way in CORES:
            got(b_half, b_rcv.at[2 + way])
        gc_copy.start()

    gc_copy = push(gbuf.at[:, core], gbuf.at[:, core], snd_s.at[3], rcv_s.at[3], sib)

    acc[...] = jnp.zeros_like(acc)
    lanes = lax.broadcasted_iota(jnp.int32, (tok, 128), 1)

    @pl.loop(0, n_ch)
    def _(i):
        pl.when(i == n_ch // 4)(rows_first)
        e_wait(i)
        base = pl.multiple_of(i * win, 128)
        own = pl.ds(pl.multiple_of(i * tok, tok), tok)
        th_buf[own, :] = lax.dot_general(gl_buf[...], e_slot[i % SLOTS], NT,
                                                      preferred_element_type=jnp.float32)

        @pl.when(i + SLOTS < n_ch)
        def _():
            e_start(i + SLOTS)

        m_l = m_buf[...]
        a_s, a_1, a_2, a_x = acc[0], acc[1], acc[2], acc[3]
        for q in range(win // 128):
            at = pl.ds(pl.multiple_of(base + q * 128, 128), 128)
            part = pl.ds(q * 128, 128)
            th = jnp.tanh(th_buf[own, part] * (1.0 / SOFT_CAP))
            th_buf[own, part] = th
            z = SOFT_CAP * th
            ok = base + q * 128 + lanes < vloc
            e_s = jnp.where(ok, jnp.exp(z), 0.0)
            sh = t_stage[:, at] - m_l
            e_t = jnp.where(ok, jnp.exp(sh), 0.0)
            sh = jnp.where(ok, sh, 0.0)
            a_s = a_s + e_s
            a_1 = a_1 + e_t
            a_2 = a_2 + e_t * sh
            a_x = a_x + e_t * jnp.where(ok, z, 0.0)
        acc[0] = a_s
        acc[1] = a_1
        acc[2] = a_2
        acc[3] = a_x

    for i in range(SLOTS):
        e_start(i)

    parts = [col(m_buf, 0)] + [jnp.sum(acc[j], axis=-1, keepdims=True) for j in (1, 2, 3, 0)]
    tile = jnp.zeros((tok, 128), jnp.float32)
    for j, v in enumerate(parts):
        tile = jnp.where(lanes == j, v, tile)
    st_tp[tp_i] = tile

    to_tp(st_tp.at[tp_i], 2)
    got(others(st_tp), rcv_s.at[2])
    t_max = col(st_tp[0], 0)
    for q in range(1, tp_n):
        t_max = jnp.maximum(t_max, col(st_tp[q], 0))
    s_1 = s_2 = s_x = s_s = jnp.zeros((tok, 1), jnp.float32)
    for q in range(tp_n):
        v = st_tp[q]
        shift = col(v, 0) - t_max
        fac = jnp.exp(shift)
        s_1 = s_1 + fac * col(v, 1)
        s_2 = s_2 + fac * (col(v, 2) + shift * col(v, 1))
        s_x = s_x + fac * col(v, 3)
        s_s = s_s + col(v, 4)
    log_1 = jnp.log(s_1)
    kl = (s_2 - s_x) / s_1 - log_1 + jnp.log(s_s)
    lse_t = t_max + log_1
    inv_s = 1.0 / s_s
    tile = jnp.where(lanes == 0, lse_t, jnp.where(lanes == 1, inv_s, jnp.where(lanes == 2, m_loc, 0.0)))
    tile = jnp.concatenate([tile, jnp.zeros((128 - tok, 128), jnp.float32)], axis=0).T
    st_dp[dp_i] = tile[0:8]

    to_plane(st_dp, 4)

    rows_second()

    @pl.loop(0, 8)
    def _(j):
        two_second(j)

    turn(0)

    got(others(mc_dp), rcv_s.at[7])
    m_cnt = jnp.sum(mc_dp[...], axis=0)[0:1, 0:1]
    w_loc = m_loc / m_cnt

    dg_tp[tp_i] = jnp.zeros((tok, dim), jnp.float32)

    @pl.loop(0, n_ch)
    def _(i):
        pl.when(i == n_ch // 3)(rows_sibling)
        pl.when(i == n_ch // 2)(lambda: turn(1))
        pl.when(i == n_ch * 2 // 3)(lambda: turn(3))
        e_wait(i)
        base = pl.multiple_of(i * win, 128)
        own = pl.ds(pl.multiple_of(i * tok, tok), tok)
        for q in range(win // 128):
            at = pl.ds(pl.multiple_of(base + q * 128, 128), 128)
            part = pl.ds(q * 128, 128)
            th = th_buf[own, part]
            p_s = jnp.exp(SOFT_CAP * th) * inv_s
            p_t = jnp.exp(t_stage[:, at] - lse_t)
            d = (p_s - p_t) * w_loc * (1.0 - th * th)
            ok = base + q * 128 + lanes < vloc
            dr_loc[:, part] = jnp.where(ok, d, 0.0).astype(jnp.bfloat16)
        dg_tp[tp_i] += lax.dot_general(dr_loc[...], e_slot[i % SLOTS], NN, preferred_element_type=jnp.float32)

        @pl.when(i + SLOTS < n_ch)
        def _():
            e_start(i + SLOTS)

    @pl.when(dp_i < last)
    def _():
        sub_copy(win).start()

    @pl.when(dp_i == last)
    def _():
        sub_copy(tail).start()

    to_tp(dg_tp.at[tp_i], 5)

    turn(2)
    turn_second(0)

    gc_copy.wait()

    def gin_copy(d):
        return pltpu.make_async_copy(gbuf.at[d // 2, d % 2], gin.at[d % 4], gin_sem.at[d % 4])

    for d in range(min(4, dp_n)):
        gin_copy(d).start()

    for d in range(dp_n):
        gin_copy(d).wait()
        gv = (gin[d % 4].reshape(tok, dim) * scale)
        g_all[pl.ds(d * tok, tok), :] = gv.astype(jnp.bfloat16)
        if d + 4 < dp_n:
            gin_copy(d + 4).start()

    for d in range(0, dp_n, 2):
        gv = g_all[pl.ds(d * tok, 2 * tok), :].astype(jnp.float32).T
        for c in range(dp_n):
            gc = gv[c * cols:(c + 1) * cols]
            if cpad != cols:
                gc = jnp.concatenate([gc, jnp.zeros((cpad - cols, 2 * tok), jnp.float32)], axis=0)
            g_t[pl.ds(c * cpad, cpad), pl.ds(d * tok, 2 * tok)] = gc.astype(jnp.bfloat16)

    for o in ODD:
        turn_second(o)

    got(others(dg_tp), rcv_s.at[5])
    dg = dg_tp[0]
    for q in range(1, tp_n):
        dg = dg + dg_tp[q]
    x = hid[...].astype(jnp.float32)
    inv = lax.rsqrt(jnp.mean(x * x, axis=-1, keepdims=True) + NORM_EPS)
    dxs = dg * scale
    o_dh[...] = (inv * dxs - x * (inv * inv * inv * (jnp.sum(dxs * x, axis=-1, keepdims=True) / dim))).astype(jnp.bfloat16)
    dw = jnp.sum(dg * (x * inv), axis=0, keepdims=True)
    dw_dp[dp_i] = jnp.broadcast_to(jnp.sum(w_loc * kl, axis=0, keepdims=True), (8, 128))
    for j in range(dim // 128):
        dw_dp[dp_i, pl.ds(j, 1), :] = dw[:, j * 128:(j + 1) * 128]

    to_plane(dw_dp, 6)

    got(others(st_dp), rcv_s.at[4])

    @pl.loop(0, dp_n)
    def _(d):
        v = jnp.concatenate([st_dp[d], jnp.zeros((120, 128), jnp.float32)], axis=0).T
        st_all[d] = v[0:tok]

    turn_second(2)

    @pl.when(dp_i < last)
    def _():
        sub_copy(win).wait()

    @pl.when(dp_i == last)
    def _():
        sub_copy(tail).wait()

    row_n = 4 * tok

    def de_src(dev, s):
        return th_buf.at[pl.ds(pl.multiple_of(dev * cpad, 8), cpad), pl.ds(s * SUB, SUB)]

    def de_dst(origin, s):
        return o_emb.at[:, pl.ds(pl.multiple_of(origin * win + s * SUB, 128), SUB)]

    def de_local(s):
        return pltpu.make_async_copy(de_src(dp_i, s), de_dst(dp_i, s), loc_sem.at[s])

    def de_first(s):
        snd = de_snd.at[s]

        @pl.loop(0, 4)
        def _(j):
            for way in CORES:
                dest = dev_ab(2, *halves(j + 4 * way))
                push(de_src(dest, s), e_a.at[way, s, j], snd, ea_rcv.at[way, s], dev_a(way_of(way))).start()

        @pl.loop(0, 8)
        def _(j):
            for o in ODD:
                dest = dev_ab(o, *halves(j))
                src = de_src(dest, s)
                pl.when(j < 2)(lambda: push(src, de_dst(dp_i, s), snd, de_rcv, dest).start())
                pl.when(j >= 2)(lambda: push(src, e_1.at[o, s, j - 2], snd, e1_rcv.at[o, s], dev_a(o)).start())

        push(de_src(sib, s), de_dst(dp_i, s), snd, de_rcv, sib).start()
        de_turn(0, s, snd)
        de_local(s).start()

    def de_turn(o, s, snd):
        @pl.loop(2, 8)
        def _(j):
            db, dc = halves(j)
            dest = dev_ab(0, db, dc)
            src = e_1.at[o, s, j - 2] if o else de_src(dest, s)
            pl.when(db != 2)(lambda: push(src, de_dst(dev_a(-o), s), snd, de_rcv, dest).start())
            pl.when(db == 2)(lambda: push(src, e_b.at[o, dc, s], snd, eb_rcv.at[o, dc, s],
                                          dev_b(way_of(dc))).start())

    def de_two(s):
        for way in CORES:
            sign = way_of(way)
            origin = dev_a(-sign)

            @pl.when(active(origin, s))
            def _():
                got(e_a.at[way, s], ea_rcv.at[way, s])

                @pl.loop(0, 4)
                def _(j):
                    jj = j + 4 * way
                    dest = dev_ab(sign, *halves(jj))
                    src, snd = e_a.at[way, s, j], e2_snd.at[way]
                    pl.when(jj < 2)(lambda: push(src, de_dst(origin, s), snd, de_rcv, dest).start())
                    pl.when(jj >= 2)(lambda: push(src, e_1.at[2, s, jj - 2], snd, e1_rcv.at[2, s],
                                                  dev_a(sign)).start())

    def de_across(o, s):
        @pl.when(active(dev_a(-o), s))
        def _():
            got(e_1.at[o, s], e1_rcv.at[o, s])
            de_turn(o, s, e1_snd.at[o])

    def de_last(o, s):
        for dc in CORES:
            sign = way_of(dc)
            origin = dev_ab(-o, -sign, 0)

            @pl.when(active(origin, s))
            def _():
                src = e_b.at[o, dc, s]
                got(src, eb_rcv.at[o, dc, s])
                push(src, de_dst(origin, s), eb_snd.at[o, dc], de_rcv, dev_ab(0, sign, dc)).start()

    def de_step(k):
        def run(f, s, *o):
            if 0 <= s < n_sub:
                f(*o, s)

        run(de_two, k - 1)
        run(de_across, k - 1, 1)
        run(de_across, k - 1, 3)
        run(de_across, k - 2, 2)
        for o in (0, 1, 3):
            run(de_last, k - 2, o)
        run(de_last, k - 3, 2)

    def de_wait(s):
        @pl.when(active(dp_i, s))
        def _():
            sent(th_buf.at[pl.ds(0, (dp_n - 1) * cpad), pl.ds(0, SUB)], de_snd.at[s])
            de_local(s).wait()

    pl.when(dp_i <= last)(lambda: got(t_recv.at[pl.ds(0, dp_n - 1)], t_rcv))

    for s in range(n_sub):
        @pl.when(active(dp_i, s))
        def _(s=s):
            @pl.loop(0, dp_n // 4)
            def _(b):
                rows = pl.ds(pl.multiple_of(b * row_n, row_n), row_n)
                r_blk[...] = lax.dot_general(g_all[rows, :], e_slot[0, pl.ds(s * SUB, SUB), :], NT,
                                             preferred_element_type=jnp.float32)
                for q in range(row_n // STRIP):
                    d = b * 4 + q * STRIP // tok
                    off = q * STRIP % tok
                    th = jnp.tanh(r_blk[pl.ds(q * STRIP, STRIP), :] * (1.0 / SOFT_CAP))
                    sv = st_all[d, pl.ds(off, STRIP), :]
                    p_s = jnp.exp(SOFT_CAP * th) * col(sv, 1)
                    p_t = jnp.exp(t_recv[d, pl.ds(off, STRIP), pl.ds(s * SUB, SUB)] - col(sv, 0))
                    dv = (p_s - p_t) * (col(sv, 2) / m_cnt) * (1.0 - th * th)
                    dr_blk[pl.ds(pl.multiple_of(b * row_n + q * STRIP, STRIP), STRIP), :] = dv.astype(jnp.bfloat16)

            @pl.loop(0, dp_n * cpad // 256)
            def _(b):
                rows = pl.ds(pl.multiple_of(b * 256, 256), 256)
                th_buf[rows, pl.ds(s * SUB, SUB)] = lax.dot_general(g_t[rows, :], dr_blk[...], NN,
                                                        preferred_element_type=jnp.float32)

            de_first(s)

        de_step(s)

    for s in range(n_sub, n_sub + 3):
        de_step(s)

    got(others(dw_dp), rcv_s.at[6])
    tot = dw_dp[0]
    for d in range(1, dp_n):
        tot = tot + dw_dp[d]
    o_dw[...] = tot

    sent(a_part, snd_s.at[0])
    for way in CORES:
        sent(gbuf.at[:, 0, 0], b_snd.at[way])
        sent(b_half, b_snd.at[2 + way])
    for buf, ch in ((st_tp, 2), (st_dp, 4), (dg_tp, 5), (dw_dp, 6), (mc_dp, 7)):
        sent(others(buf), snd_s.at[ch])

    one = t_recv.at[0]

    @pl.loop(0, 8)
    def _(j):
        for o in (1, 2, 3):
            pl.when(dev_ab(o, *halves(j)) <= last)(lambda o=o: sent(one, s1_snd.at[m8(o, j)]))
        pl.when(dev_ab(way_of(j // 4), *halves(j)) <= last)(lambda: sent(one, sa_snd.at[j]))

    pl.when(sib <= last)(lambda: sent(one, s1_snd.at[1]))

    @pl.loop(2, 8)
    def _(j):
        for o in range(4):
            pl.when(dev_ab(0, *halves(j)) <= last)(lambda o=o: sent(one, s2_snd.at[m8(o, j)]))

    for o in range(4):
        for dc in CORES:
            pl.when(dev_ab(0, way_of(dc), dc) <= last)(lambda o=o, dc=dc: sent(one, sb_snd.at[m2(o, dc)]))

    def e_sent(origin, part, sem):
        pl.when(origin < last)(lambda: sent(part(n_sub), sem))
        pl.when(origin == last)(lambda: sent(part(tail_n), sem))

    for way in CORES:
        e_sent(dev_ab(2 * way - 1, 0, 0), lambda n, way=way: e_a.at[way, pl.ds(0, n)], e2_snd.at[way])
    for o in range(4):
        if o:
            e_sent(dev_a(-o), lambda n, o=o: e_1.at[o, pl.ds(0, n)], e1_snd.at[o])
        for dc in CORES:
            e_sent(dev_ab(-o, 2 * dc - 1, 0), lambda n, o=o, dc=dc: e_b.at[o, dc, pl.ds(0, n)], eb_snd.at[o, dc])

    for s in range(n_sub):
        de_wait(s)

    total = sum(n_act(s) for s in range(n_sub))

    def de_drain(n):
        got(o_emb.at[:, pl.ds(0, n * SUB)], de_rcv)

    @pl.when(dp_i < last)
    def _():
        de_drain(total - n_sub)

    @pl.when(dp_i == last)
    def _():
        de_drain(total - tail_n)

    @pl.when(dp_i > last)
    def _():
        de_drain(total)


def solution(mesh):
    tp_n, dp_n = mesh.shape['tp'], mesh.shape['dp']
    ny = 4 if dp_n >= 32 else 1

    def device_fn(hid_loc, norm_w, emb_loc, teach_loc, mask_loc):
        tok, dim = hid_loc.shape
        vloc = emb_loc.shape[0]
        win = -(-vloc // (dp_n * 128)) * 128
        n_ch = -(-vloc // win)
        cols = dim // dp_n
        cpad = -(-cols // 8) * 8
        rq = tok // tp_n
        f32, bf16 = jnp.float32, jnp.bfloat16
        vm, dma = pltpu.VMEM, pltpu.SemaphoreType.DMA
        any_s, vm_s = pl.BlockSpec(memory_space=pl.ANY), pl.BlockSpec(memory_space=pltpu.VMEM)
        wide = n_ch * win
        n_sub = win // SUB
        o_emb, o_dh, o_dw = pl.pallas_call(
            functools.partial(body, (tp_n, dp_n, ny)),
            out_shape=(jax.ShapeDtypeStruct((cpad, wide), f32), jax.ShapeDtypeStruct((tok, dim), bf16),
                       jax.ShapeDtypeStruct((8, 128), f32),
                       jax.ShapeDtypeStruct((dp_n // 2, 2, tp_n, rq, dim), f32),
                       jax.ShapeDtypeStruct((4, n_sub, 6, cpad, SUB), f32),
                       jax.ShapeDtypeStruct((2, n_sub, 4, cpad, SUB), f32),
                       jax.ShapeDtypeStruct((4, 2, n_sub, cpad, SUB), f32)),
            in_specs=[vm_s, vm_s, vm_s, any_s, any_s],
            out_specs=(any_s, vm_s, vm_s, any_s, any_s, any_s, any_s),
            scratch_shapes=[
                vm((tok, wide), f32), vm((n_ch * tok, win), f32), vm((dp_n, tok, win), f32), vm((2, 16, vloc), bf16),
                vm((SLOTS, win, dim), bf16), vm((dp_n * tok, dim), bf16),
                vm((dp_n * cpad, dp_n * tok), bf16), vm((4, tp_n, rq, dim), f32), vm((tok, win), bf16),
                vm((4 * tok, SUB), f32), vm((dp_n * tok, SUB), bf16),
                vm((3, 6, tok, win), f32), vm((8, tok, win), f32), vm((8, tok, win), f32), vm((dp_n, 8, 128), f32),
                vm((tok, 128), f32), vm((4, tok, 128), f32), vm((tp_n, tok, 128), f32), vm((8, 128), f32),
                vm((dp_n, 8, 128), f32), vm((dp_n, tok, 128), f32), vm((tp_n, tok, dim), f32),
                vm((dp_n, 8, 128), f32), vm((tp_n, rq, dim), f32), vm((tok, dim), bf16),
                dma((2,)), dma((SLOTS,)), dma, dma, dma((4,)), dma((n_sub,)), dma((8,)), dma((8,)),
                dma, dma((n_sub,)), dma, dma((4,)), dma((4,)), dma((4, n_sub)), dma((2, n_sub)), dma((4, 2, n_sub)), dma((4,)), dma((2,)),
                dma((4, 2)),
                dma((32,)), dma((8,)), dma((8,)), dma((32,)), dma((8,)), dma((32,)), dma((8,)),
            ],
            compiler_params=pltpu.CompilerParams(collective_id=0, has_side_effects=True,
                                                 vmem_limit_bytes=67_000_000),
            name='head',
        )(hid_loc, norm_w.reshape(1, dim), mask_loc.astype(f32).reshape(tok, 1), emb_loc, teach_loc)[:3]
        return o_dw[7, 0], o_dh, o_emb[:cols, :vloc].T, o_dw.reshape(-1)[:dim]

    return jax.shard_map(device_fn, mesh=mesh, in_specs=(P('dp', None), P(None), P('tp', None), P('dp', 'tp'), P('dp')),
                         out_specs=(P(), P('dp', None), P('tp', 'dp'), P(None)), check_vma=False)
```

```python
import functools

import jax
import jax.numpy as jnp
from jax import lax
from jax.experimental import pallas as pl
from jax.experimental.pallas import tpu as pltpu
from jax.sharding import PartitionSpec as P

SOFT_CAP = 30.0
NORM_EPS = 1e-6
SUB = 256
STRIP = 32
ODD = (1, 3)
CORES = (0, 1)
SLOTS = 3
MESH = pl.DeviceIdType.MESH
NT = (((1,), (1,)), ((), ()))
NN = (((1,), (0,)), ((), ()))


def col(v, j):
    return v[:, j:j + 1]


def halves(j):
    return j // 2, j % 2


def way_of(d):
    return 1 - 2 * d


def m8(o, j):
    return o * 8 + j


def m2(o, dc):
    return o * 2 + dc


def body(cfg, hid, nw, mask, emb, teach, o_emb, o_dh, o_dw, gbuf, e_1, e_a, e_b,
         t_stage, th_buf, t_recv, tb, e_slot, g_all, g_t, gin, dr_loc, r_blk, dr_blk,
         w1, r_a, r_b, mc_dp, m_buf, acc, st_tp, st_t, st_dp, st_all, dg_tp, dw_dp, xs_buf, gl_buf,
         tb_sem, es_sem, sub_sem, gl_sem, gin_sem, loc_sem, snd_s, rcv_s, t_rcv, de_snd, de_rcv, b_snd, b_rcv, e1_rcv, ea_rcv, eb_rcv, e1_snd, e2_snd, eb_snd,
         w1_rcv, ra_rcv, rb_rcv, s1_snd, sa_snd, s2_snd, sb_snd):
    tp_n, dp_n, ny = cfg
    tok, dim = hid.shape
    vloc = emb.shape[0]
    win = t_recv.shape[2]
    n_sub = win // SUB
    n_ch = t_stage.shape[1] // win
    tail = vloc - (n_ch - 1) * win
    chips = dp_n // 2
    nz = chips // ny
    rq = tok // tp_n
    cpad = o_emb.shape[0]
    cols = dim // dp_n
    last = n_ch - 1
    tail_n = -(-tail // SUB)
    tp_i = lax.axis_index('tp')
    dp_i = lax.axis_index('dp')
    chip = dp_i // 2
    core = dp_i % 2

    zc, yc = chip // ny, chip % ny
    a_c, b_c = zc + core * (yc - zc), yc + core * (zc - yc)
    sa, sb = ny - core * (ny - 1), 1 + core * (ny - 1)

    def dev_ab(oa, ob, dc):
        return 2 * (((a_c + oa + 4) % 4) * sa + ((b_c + ob + 4) % 4) * sb) + (core + dc) % 2

    def dev_a(oa):
        return dev_ab(oa, 0, 0)

    def dev_b(ob):
        return dev_ab(0, ob, 0)

    def peer(k):
        j = (k // 2 * 5) % chips
        return ((zc + j // ny) % nz * ny + (yc + j % ny) % ny) * 2 + (core + k % 2) % 2

    def active(dev, s):
        return dev * win + s * SUB < vloc

    def n_act(s):
        return sum(1 for d in range(dp_n) if d * win + s * SUB < vloc)

    sib = chip * 2 + (core + 1) % 2

    def push(src, dst, snd, rcv, dev, axis='dp'):
        return pltpu.make_async_remote_copy(src, dst, snd, rcv, device_id={axis: dev}, device_id_type=MESH)

    def got(ref, sem):
        push(ref, ref, gl_sem, sem, dp_i).wait_recv()

    def sent(ref, sem):
        push(ref, ref, sem, gl_sem, dp_i).wait_send()

    def to_plane(buf, ch):
        @pl.loop(1, dp_n)
        def _(k):
            push(buf.at[dp_i], buf.at[dp_i], snd_s.at[ch], rcv_s.at[ch], peer(k)).start()

    def to_tp(ref, ch):
        @pl.loop(1, tp_n)
        def _(k):
            push(ref, ref, snd_s.at[ch], rcv_s.at[ch], (tp_i + k) % tp_n, 'tp').start()

    def others(buf):
        return buf.at[pl.ds(0, buf.shape[0] - 1)]

    barrier = pltpu.get_barrier_semaphore()

    @pl.loop(1, dp_n)
    def _(k):
        pl.semaphore_signal(barrier, inc=1, device_id={'dp': peer(k)}, device_id_type=MESH)

    @pl.loop(1, tp_n)
    def _(k):
        pl.semaphore_signal(barrier, inc=1, device_id={'tp': (tp_i + k) % tp_n}, device_id_type=MESH)

    def tb_copy(r):
        return pltpu.make_async_copy(teach.at[pl.ds(r * 16, 16)], tb.at[r % 2], tb_sem.at[r % 2])

    tb_copy(0).start()
    tb_copy(1).start()

    def e_copy(i, slot, rows):
        return pltpu.make_async_copy(emb.at[pl.ds(pl.multiple_of(i * win, 16), rows)],
                                     e_slot.at[slot, pl.ds(0, rows)], es_sem.at[slot])

    def e_start(i):
        @pl.when(i < last)
        def _():
            e_copy(i, i % SLOTS, win).start()

        @pl.when(i == last)
        def _():
            e_copy(i, i % SLOTS, tail).start()

    def e_wait(i):
        @pl.when(i < last)
        def _():
            e_copy(i, i % SLOTS, win).wait()

        @pl.when(i == last)
        def _():
            e_copy(i, i % SLOTS, tail).wait()

    def sub_copy(rows):
        return pltpu.make_async_copy(emb.at[pl.ds(pl.multiple_of(dp_i * win, 16), rows)],
                                     e_slot.at[0, pl.ds(0, rows)], sub_sem)

    x = hid[...].astype(jnp.float32)
    scale = 1.0 + nw[...].astype(jnp.float32).reshape(1, dim)
    inv = lax.rsqrt(jnp.mean(x * x, axis=-1, keepdims=True) + NORM_EPS)
    xs = x * inv
    xs_buf[...] = xs.reshape(tp_n, rq, dim)
    gl_buf[...] = (xs * scale).astype(jnp.bfloat16)

    own_g = pltpu.make_async_copy(xs_buf.at[tp_i], gbuf.at[chip, core, tp_i], gl_sem)
    own_g.start()

    diag = lax.broadcasted_iota(jnp.int32, (tok, tok), 0) == lax.broadcasted_iota(jnp.int32, (tok, tok), 1)
    m_row = mask[...].astype(jnp.float32).reshape(1, tok)
    m_loc = jnp.sum(jnp.where(diag, m_row, 0.0), axis=-1, keepdims=True)
    mc_dp[dp_i] = jnp.broadcast_to(jnp.sum(m_loc, axis=0, keepdims=True), (8, 128))
    pl.semaphore_wait(barrier, dp_n - 1 + tp_n - 1)

    @pl.loop(1, chips)
    def _(k):
        push(xs_buf.at[tp_i], gbuf.at[chip, core, tp_i], snd_s.at[0], rcv_s.at[0], peer(2 * k)).start()


    to_plane(mc_dp, 7)

    pieces = [(c0, min(1024, vloc - c0)) for c0 in range(0, vloc, 1024)]
    full_p = vloc // 1024

    t_stage[:, pl.ds(vloc // 128 * 128, n_ch * win - vloc // 128 * 128)] = jnp.zeros(
        (tok, n_ch * win - vloc // 128 * 128), jnp.float32)
    for r in range(tok // 16):
        tb_copy(r).wait()
        rows = pl.ds(r * 16, 16)

        def conv(c0, width, mx):
            v = tb[r % 2, :, pl.ds(c0, width)].astype(jnp.float32)
            t_stage[rows, pl.ds(c0, width)] = v
            return v

        def step(i, mx):
            v = conv(pl.multiple_of(i * 1024, 128), 1024, mx)
            for q in range(8):
                mx = jnp.maximum(mx, v[:, q * 128:(q + 1) * 128])
            return mx

        mx = lax.fori_loop(0, full_p, step, jnp.full((16, 128), -jnp.inf, jnp.float32))
        m1 = jnp.max(mx, axis=-1, keepdims=True)
        if full_p * 1024 < vloc:
            v = conv(full_p * 1024, vloc - full_p * 1024, None)
            m1 = jnp.maximum(m1, jnp.max(v, axis=-1, keepdims=True))
        m_buf[rows, :] = jnp.broadcast_to(m1, (16, 128))
        if r + 2 < tok // 16:
            tb_copy(r + 2).start()

    for i in range(SLOTS):
        e_start(i)

    def t_win(dev):
        return t_stage.at[:, pl.ds(pl.multiple_of(dev * win, 128), win)]

    def two_first(j):
        dest = dev_ab(2, *halves(j))
        hop = dev_a(way_of(j // 4))
        pl.when(dest <= last)(lambda: push(t_win(dest), r_a.at[j], s1_snd.at[16 + j], ra_rcv.at[j], hop).start())

    def one_first(o, j):
        dest = dev_ab(o, *halves(j))

        @pl.when(dest <= last)
        def _():
            pl.when(j < 2)(lambda: push(t_win(dest), t_recv.at[dp_i], s1_snd.at[m8(o, j)], t_rcv, dest).start())
            pl.when(j >= 2)(lambda: push(t_win(dest), w1.at[o - 1, j - 2], s1_snd.at[m8(o, j)], w1_rcv.at[m8(o, j)],
                                         dev_a(o)).start())

    def two_second(j):
        sign = way_of(j // 4)
        dest = dev_ab(sign, *halves(j))

        @pl.when(dest <= last)
        def _():
            got(r_a.at[j], ra_rcv.at[j])
            pl.when(j < 2)(lambda: push(r_a.at[j], t_recv.at[dev_a(-sign)], sa_snd.at[j], t_rcv, dest).start())
            pl.when(j >= 2)(lambda: push(r_a.at[j], w1.at[1, j - 2], sa_snd.at[j], w1_rcv.at[16 + j],
                                         dev_a(sign)).start())

    def across(o, j):
        db, dc = halves(j)
        dest = dev_ab(0, db, dc)

        @pl.when(dest <= last)
        def _():
            if o == 0:
                src = t_win(dest)
            else:
                src = w1.at[o - 1, j - 2]
                got(src, w1_rcv.at[m8(o, j)])
            pl.when(db != 2)(lambda: push(src, t_recv.at[dev_a(-o)], s2_snd.at[m8(o, j)], t_rcv, dest).start())
            pl.when(db == 2)(lambda: push(src, r_b.at[m2(o, dc)], s2_snd.at[m8(o, j)], rb_rcv.at[m2(o, dc)],
                                          dev_b(way_of(dc))).start())

    def across_second(o, dc):
        sign = way_of(dc)
        dest = dev_ab(0, sign, dc)

        @pl.when(dest <= last)
        def _():
            got(r_b.at[m2(o, dc)], rb_rcv.at[m2(o, dc)])
            push(r_b.at[m2(o, dc)], t_recv.at[dev_ab(-o, -sign, 0)], sb_snd.at[m2(o, dc)], t_rcv, dest).start()

    def turn(o):
        @pl.loop(2, 8)
        def _(j):
            across(o, j)

    def turn_second(o):
        for dc in CORES:
            across_second(o, dc)

    @pl.loop(0, 4)
    def _(j):
        two_first(j)
        two_first(j + 4)

    pl.when(sib <= last)(lambda: push(t_win(sib), t_recv.at[dp_i], s1_snd.at[1], t_rcv, sib).start())

    @pl.when(dp_i <= last)
    def _():
        t_recv[dp_i] = t_stage[:, pl.ds(pl.multiple_of(dp_i * win, 128), win)]

    a_part = gbuf.at[pl.ds(0, chips - 1), 0, 0]
    up, down = (tp_i + 1) % tp_n, (tp_i + tp_n - 1) % tp_n
    half = chips // 2

    def rows_first():
        own_g.wait()
        got(a_part, rcv_s.at[0])
        own = gbuf.at[:, core, tp_i]
        push(own, own, b_snd.at[0], b_rcv.at[0], up, 'tp').start()
        push(own, own, b_snd.at[1], b_rcv.at[1], down, 'tp').start()

    def rows_second():
        for way in CORES:
            got(gbuf.at[:, 0, 0], b_rcv.at[way])
        lo, hi = gbuf.at[pl.ds(0, half), core, down], gbuf.at[pl.ds(half, half), core, up]
        push(lo, lo, b_snd.at[2], b_rcv.at[2], up, 'tp').start()
        push(hi, hi, b_snd.at[3], b_rcv.at[3], down, 'tp').start()

    b_half = gbuf.at[pl.ds(0, half), 0, 0]

    def rows_sibling():
        for way in CORES:
            got(b_half, b_rcv.at[2 + way])
        gc_copy.start()

    gc_copy = push(gbuf.at[:, core], gbuf.at[:, core], snd_s.at[3], rcv_s.at[3], sib)

    acc[...] = jnp.zeros_like(acc)
    lanes = lax.broadcasted_iota(jnp.int32, (tok, 128), 1)

    @pl.loop(0, n_ch)
    def _(i):
        pl.when(i == n_ch // 4)(rows_first)

        @pl.when(i % 3 + i // 24 * 3 == 0)
        def _():
            for o in ODD:
                one_first(o, i // 3)

        e_wait(i)
        base = pl.multiple_of(i * win, 128)
        own = pl.ds(pl.multiple_of(i * tok, tok), tok)
        th_buf[own, :] = lax.dot_general(gl_buf[...], e_slot[i % SLOTS], NT,
                                                      preferred_element_type=jnp.float32)

        @pl.when(i + SLOTS < n_ch)
        def _():
            e_start(i + SLOTS)

        m_l = m_buf[...]
        a_s, a_1, a_2, a_x = acc[0], acc[1], acc[2], acc[3]
        for q in range(win // 128):
            at = pl.ds(pl.multiple_of(base + q * 128, 128), 128)
            part = pl.ds(q * 128, 128)
            th = jnp.tanh(th_buf[own, part] * (1.0 / SOFT_CAP))
            th_buf[own, part] = th
            z = SOFT_CAP * th
            ok = base + q * 128 + lanes < vloc
            e_s = jnp.where(ok, jnp.exp(z), 0.0)
            sh = t_stage[:, at] - m_l
            e_t = jnp.where(ok, jnp.exp(sh), 0.0)
            sh = jnp.where(ok, sh, 0.0)
            a_s = a_s + e_s
            a_1 = a_1 + e_t
            a_2 = a_2 + e_t * sh
            a_x = a_x + e_t * jnp.where(ok, z, 0.0)
        acc[0] = a_s
        acc[1] = a_1
        acc[2] = a_2
        acc[3] = a_x

    for i in range(SLOTS):
        e_start(i)

    parts = [col(m_buf, 0)] + [jnp.sum(acc[j], axis=-1, keepdims=True) for j in (1, 2, 3, 0)]
    tile = jnp.zeros((tok, 128), jnp.float32)
    for j, v in enumerate(parts):
        tile = jnp.where(lanes == j, v, tile)
    st_tp[tp_i] = tile

    to_tp(st_tp.at[tp_i], 2)
    got(others(st_tp), rcv_s.at[2])
    t_max = col(st_tp[0], 0)
    for q in range(1, tp_n):
        t_max = jnp.maximum(t_max, col(st_tp[q], 0))
    s_1 = s_2 = s_x = s_s = jnp.zeros((tok, 1), jnp.float32)
    for q in range(tp_n):
        v = st_tp[q]
        shift = col(v, 0) - t_max
        fac = jnp.exp(shift)
        s_1 = s_1 + fac * col(v, 1)
        s_2 = s_2 + fac * (col(v, 2) + shift * col(v, 1))
        s_x = s_x + fac * col(v, 3)
        s_s = s_s + col(v, 4)
    log_1 = jnp.log(s_1)
    kl = (s_2 - s_x) / s_1 - log_1 + jnp.log(s_s)
    lse_t = t_max + log_1
    inv_s = 1.0 / s_s
    tile = jnp.where(lanes == 0, lse_t, jnp.where(lanes == 1, inv_s, jnp.where(lanes == 2, m_loc, 0.0)))
    tile = jnp.concatenate([tile, jnp.zeros((128 - tok, 128), jnp.float32)], axis=0).T
    st_dp[dp_i] = tile[0:8]

    to_plane(st_dp, 4)

    rows_second()

    @pl.loop(0, 8)
    def _(j):
        two_second(j)

    turn(0)

    got(others(mc_dp), rcv_s.at[7])
    m_cnt = jnp.sum(mc_dp[...], axis=0)[0:1, 0:1]
    w_loc = m_loc / m_cnt

    dg_tp[tp_i] = jnp.zeros((tok, dim), jnp.float32)

    @pl.loop(0, n_ch)
    def _(i):
        pl.when(i == n_ch // 3)(rows_sibling)
        pl.when(i == n_ch // 2)(lambda: turn(1))
        pl.when(i == n_ch * 2 // 3)(lambda: turn(3))
        e_wait(i)
        base = pl.multiple_of(i * win, 128)
        own = pl.ds(pl.multiple_of(i * tok, tok), tok)
        for q in range(win // 128):
            at = pl.ds(pl.multiple_of(base + q * 128, 128), 128)
            part = pl.ds(q * 128, 128)
            th = th_buf[own, part]
            p_s = jnp.exp(SOFT_CAP * th) * inv_s
            p_t = jnp.exp(t_stage[:, at] - lse_t)
            d = (p_s - p_t) * w_loc * (1.0 - th * th)
            ok = base + q * 128 + lanes < vloc
            dr_loc[:, part] = jnp.where(ok, d, 0.0).astype(jnp.bfloat16)
        dg_tp[tp_i] += lax.dot_general(dr_loc[...], e_slot[i % SLOTS], NN, preferred_element_type=jnp.float32)

        @pl.when(i + SLOTS < n_ch)
        def _():
            e_start(i + SLOTS)

    @pl.when(dp_i < last)
    def _():
        sub_copy(win).start()

    @pl.when(dp_i == last)
    def _():
        sub_copy(tail).start()

    to_tp(dg_tp.at[tp_i], 5)

    turn(2)
    turn_second(0)

    gc_copy.wait()

    def gin_copy(d):
        return pltpu.make_async_copy(gbuf.at[d // 2, d % 2], gin.at[d % 4], gin_sem.at[d % 4])

    for d in range(min(4, dp_n)):
        gin_copy(d).start()

    for d in range(dp_n):
        gin_copy(d).wait()
        gv = (gin[d % 4].reshape(tok, dim) * scale)
        g_all[pl.ds(d * tok, tok), :] = gv.astype(jnp.bfloat16)
        if d + 4 < dp_n:
            gin_copy(d + 4).start()

    for d in range(0, dp_n, 2):
        gv = g_all[pl.ds(d * tok, 2 * tok), :].astype(jnp.float32).T
        for c in range(dp_n):
            gc = gv[c * cols:(c + 1) * cols]
            if cpad != cols:
                gc = jnp.concatenate([gc, jnp.zeros((cpad - cols, 2 * tok), jnp.float32)], axis=0)
            g_t[pl.ds(c * cpad, cpad), pl.ds(d * tok, 2 * tok)] = gc.astype(jnp.bfloat16)

    for o in ODD:
        turn_second(o)

    got(others(dg_tp), rcv_s.at[5])
    dg = dg_tp[0]
    for q in range(1, tp_n):
        dg = dg + dg_tp[q]
    x = hid[...].astype(jnp.float32)
    inv = lax.rsqrt(jnp.mean(x * x, axis=-1, keepdims=True) + NORM_EPS)
    dxs = dg * scale
    o_dh[...] = (inv * dxs - x * (inv * inv * inv * (jnp.sum(dxs * x, axis=-1, keepdims=True) / dim))).astype(jnp.bfloat16)
    dw = jnp.sum(dg * (x * inv), axis=0, keepdims=True)
    dw_dp[dp_i] = jnp.broadcast_to(jnp.sum(w_loc * kl, axis=0, keepdims=True), (8, 128))
    for j in range(dim // 128):
        dw_dp[dp_i, pl.ds(j, 1), :] = dw[:, j * 128:(j + 1) * 128]

    to_plane(dw_dp, 6)

    got(others(st_dp), rcv_s.at[4])

    @pl.loop(0, dp_n)
    def _(d):
        v = jnp.concatenate([st_dp[d], jnp.zeros((120, 128), jnp.float32)], axis=0).T
        st_all[d] = v[0:tok]

    turn_second(2)

    @pl.when(dp_i < last)
    def _():
        sub_copy(win).wait()

    @pl.when(dp_i == last)
    def _():
        sub_copy(tail).wait()

    row_n = 4 * tok

    def de_src(dev, s):
        return th_buf.at[pl.ds(pl.multiple_of(dev * cpad, 8), cpad), pl.ds(s * SUB, SUB)]

    def de_dst(origin, s):
        return o_emb.at[:, pl.ds(pl.multiple_of(origin * win + s * SUB, 128), SUB)]

    def de_local(s):
        return pltpu.make_async_copy(de_src(dp_i, s), de_dst(dp_i, s), loc_sem.at[s])

    def de_first(s):
        snd = de_snd.at[s]

        @pl.loop(0, 4)
        def _(j):
            for way in CORES:
                dest = dev_ab(2, *halves(j + 4 * way))
                push(de_src(dest, s), e_a.at[way, s, j], snd, ea_rcv.at[way, s], dev_a(way_of(way))).start()

        @pl.loop(0, 8)
        def _(j):
            for o in ODD:
                dest = dev_ab(o, *halves(j))
                src = de_src(dest, s)
                pl.when(j < 2)(lambda: push(src, de_dst(dp_i, s), snd, de_rcv, dest).start())
                pl.when(j >= 2)(lambda: push(src, e_1.at[o, s, j - 2], snd, e1_rcv.at[o, s], dev_a(o)).start())

        push(de_src(sib, s), de_dst(dp_i, s), snd, de_rcv, sib).start()
        de_turn(0, s, snd)
        de_local(s).start()

    def de_turn(o, s, snd):
        @pl.loop(2, 8)
        def _(j):
            db, dc = halves(j)
            dest = dev_ab(0, db, dc)
            src = e_1.at[o, s, j - 2] if o else de_src(dest, s)
            pl.when(db != 2)(lambda: push(src, de_dst(dev_a(-o), s), snd, de_rcv, dest).start())
            pl.when(db == 2)(lambda: push(src, e_b.at[o, dc, s], snd, eb_rcv.at[o, dc, s],
                                          dev_b(way_of(dc))).start())

    def de_two(s):
        for way in CORES:
            sign = way_of(way)
            origin = dev_a(-sign)

            @pl.when(active(origin, s))
            def _():
                got(e_a.at[way, s], ea_rcv.at[way, s])

                @pl.loop(0, 4)
                def _(j):
                    jj = j + 4 * way
                    dest = dev_ab(sign, *halves(jj))
                    src, snd = e_a.at[way, s, j], e2_snd.at[way]
                    pl.when(jj < 2)(lambda: push(src, de_dst(origin, s), snd, de_rcv, dest).start())
                    pl.when(jj >= 2)(lambda: push(src, e_1.at[2, s, jj - 2], snd, e1_rcv.at[2, s],
                                                  dev_a(sign)).start())

    def de_across(o, s):
        @pl.when(active(dev_a(-o), s))
        def _():
            got(e_1.at[o, s], e1_rcv.at[o, s])
            de_turn(o, s, e1_snd.at[o])

    def de_last(o, s):
        for dc in CORES:
            sign = way_of(dc)
            origin = dev_ab(-o, -sign, 0)

            @pl.when(active(origin, s))
            def _():
                src = e_b.at[o, dc, s]
                got(src, eb_rcv.at[o, dc, s])
                push(src, de_dst(origin, s), eb_snd.at[o, dc], de_rcv, dev_ab(0, sign, dc)).start()

    def de_step(k):
        def run(f, s, *o):
            if 0 <= s < n_sub:
                f(*o, s)

        run(de_two, k - 1)
        run(de_across, k - 1, 1)
        run(de_across, k - 1, 3)
        run(de_across, k - 2, 2)
        for o in (0, 1, 3):
            run(de_last, k - 2, o)
        run(de_last, k - 3, 2)

    def de_wait(s):
        @pl.when(active(dp_i, s))
        def _():
            sent(th_buf.at[pl.ds(0, (dp_n - 1) * cpad), pl.ds(0, SUB)], de_snd.at[s])
            de_local(s).wait()

    pl.when(dp_i <= last)(lambda: got(t_recv.at[pl.ds(0, dp_n - 1)], t_rcv))

    for s in range(n_sub):
        @pl.when(active(dp_i, s))
        def _(s=s):
            @pl.loop(0, dp_n // 4)
            def _(b):
                rows = pl.ds(pl.multiple_of(b * row_n, row_n), row_n)
                r_blk[...] = lax.dot_general(g_all[rows, :], e_slot[0, pl.ds(s * SUB, SUB), :], NT,
                                             preferred_element_type=jnp.float32)
                for q in range(row_n // STRIP):
                    d = b * 4 + q * STRIP // tok
                    off = q * STRIP % tok
                    th = jnp.tanh(r_blk[pl.ds(q * STRIP, STRIP), :] * (1.0 / SOFT_CAP))
                    sv = st_all[d, pl.ds(off, STRIP), :]
                    p_s = jnp.exp(SOFT_CAP * th) * col(sv, 1)
                    p_t = jnp.exp(t_recv[d, pl.ds(off, STRIP), pl.ds(s * SUB, SUB)] - col(sv, 0))
                    dv = (p_s - p_t) * (col(sv, 2) / m_cnt) * (1.0 - th * th)
                    dr_blk[pl.ds(pl.multiple_of(b * row_n + q * STRIP, STRIP), STRIP), :] = dv.astype(jnp.bfloat16)

            @pl.loop(0, dp_n * cpad // 256)
            def _(b):
                rows = pl.ds(pl.multiple_of(b * 256, 256), 256)
                th_buf[rows, pl.ds(s * SUB, SUB)] = lax.dot_general(g_t[rows, :], dr_blk[...], NN,
                                                        preferred_element_type=jnp.float32)

            de_first(s)

        de_step(s)

    for s in range(n_sub, n_sub + 3):
        de_step(s)

    got(others(dw_dp), rcv_s.at[6])
    tot = dw_dp[0]
    for d in range(1, dp_n):
        tot = tot + dw_dp[d]
    o_dw[...] = tot

    sent(a_part, snd_s.at[0])
    for way in CORES:
        sent(gbuf.at[:, 0, 0], b_snd.at[way])
        sent(b_half, b_snd.at[2 + way])
    for buf, ch in ((st_tp, 2), (st_dp, 4), (dg_tp, 5), (dw_dp, 6), (mc_dp, 7)):
        sent(others(buf), snd_s.at[ch])

    one = t_recv.at[0]

    @pl.loop(0, 8)
    def _(j):
        for o in (1, 2, 3):
            pl.when(dev_ab(o, *halves(j)) <= last)(lambda o=o: sent(one, s1_snd.at[m8(o, j)]))
        pl.when(dev_ab(way_of(j // 4), *halves(j)) <= last)(lambda: sent(one, sa_snd.at[j]))

    pl.when(sib <= last)(lambda: sent(one, s1_snd.at[1]))

    @pl.loop(2, 8)
    def _(j):
        for o in range(4):
            pl.when(dev_ab(0, *halves(j)) <= last)(lambda o=o: sent(one, s2_snd.at[m8(o, j)]))

    for o in range(4):
        for dc in CORES:
            pl.when(dev_ab(0, way_of(dc), dc) <= last)(lambda o=o, dc=dc: sent(one, sb_snd.at[m2(o, dc)]))

    def e_sent(origin, part, sem):
        pl.when(origin < last)(lambda: sent(part(n_sub), sem))
        pl.when(origin == last)(lambda: sent(part(tail_n), sem))

    for way in CORES:
        e_sent(dev_ab(2 * way - 1, 0, 0), lambda n, way=way: e_a.at[way, pl.ds(0, n)], e2_snd.at[way])
    for o in range(4):
        if o:
            e_sent(dev_a(-o), lambda n, o=o: e_1.at[o, pl.ds(0, n)], e1_snd.at[o])
        for dc in CORES:
            e_sent(dev_ab(-o, 2 * dc - 1, 0), lambda n, o=o, dc=dc: e_b.at[o, dc, pl.ds(0, n)], eb_snd.at[o, dc])

    for s in range(n_sub):
        de_wait(s)

    total = sum(n_act(s) for s in range(n_sub))

    def de_drain(n):
        got(o_emb.at[:, pl.ds(0, n * SUB)], de_rcv)

    @pl.when(dp_i < last)
    def _():
        de_drain(total - n_sub)

    @pl.when(dp_i == last)
    def _():
        de_drain(total - tail_n)

    @pl.when(dp_i > last)
    def _():
        de_drain(total)


def solution(mesh):
    tp_n, dp_n = mesh.shape['tp'], mesh.shape['dp']
    ny = 4 if dp_n >= 32 else 1

    def device_fn(hid_loc, norm_w, emb_loc, teach_loc, mask_loc):
        tok, dim = hid_loc.shape
        vloc = emb_loc.shape[0]
        win = -(-vloc // (dp_n * 128)) * 128
        n_ch = -(-vloc // win)
        cols = dim // dp_n
        cpad = -(-cols // 8) * 8
        rq = tok // tp_n
        f32, bf16 = jnp.float32, jnp.bfloat16
        vm, dma = pltpu.VMEM, pltpu.SemaphoreType.DMA
        any_s, vm_s = pl.BlockSpec(memory_space=pl.ANY), pl.BlockSpec(memory_space=pltpu.VMEM)
        wide = n_ch * win
        n_sub = win // SUB
        o_emb, o_dh, o_dw = pl.pallas_call(
            functools.partial(body, (tp_n, dp_n, ny)),
            out_shape=(jax.ShapeDtypeStruct((cpad, wide), f32), jax.ShapeDtypeStruct((tok, dim), bf16),
                       jax.ShapeDtypeStruct((8, 128), f32),
                       jax.ShapeDtypeStruct((dp_n // 2, 2, tp_n, rq, dim), f32),
                       jax.ShapeDtypeStruct((4, n_sub, 6, cpad, SUB), f32),
                       jax.ShapeDtypeStruct((2, n_sub, 4, cpad, SUB), f32),
                       jax.ShapeDtypeStruct((4, 2, n_sub, cpad, SUB), f32)),
            in_specs=[vm_s, vm_s, vm_s, any_s, any_s],
            out_specs=(any_s, vm_s, vm_s, any_s, any_s, any_s, any_s),
            scratch_shapes=[
                vm((tok, wide), f32), vm((n_ch * tok, win), f32), vm((dp_n, tok, win), f32), vm((2, 16, vloc), bf16),
                vm((SLOTS, win, dim), bf16), vm((dp_n * tok, dim), bf16),
                vm((dp_n * cpad, dp_n * tok), bf16), vm((4, tp_n, rq, dim), f32), vm((tok, win), bf16),
                vm((4 * tok, SUB), f32), vm((dp_n * tok, SUB), bf16),
                vm((3, 6, tok, win), f32), vm((8, tok, win), f32), vm((8, tok, win), f32), vm((dp_n, 8, 128), f32),
                vm((tok, 128), f32), vm((4, tok, 128), f32), vm((tp_n, tok, 128), f32), vm((8, 128), f32),
                vm((dp_n, 8, 128), f32), vm((dp_n, tok, 128), f32), vm((tp_n, tok, dim), f32),
                vm((dp_n, 8, 128), f32), vm((tp_n, rq, dim), f32), vm((tok, dim), bf16),
                dma((2,)), dma((SLOTS,)), dma, dma, dma((4,)), dma((n_sub,)), dma((8,)), dma((8,)),
                dma, dma((n_sub,)), dma, dma((4,)), dma((4,)), dma((4, n_sub)), dma((2, n_sub)), dma((4, 2, n_sub)), dma((4,)), dma((2,)),
                dma((4, 2)),
                dma((32,)), dma((8,)), dma((8,)), dma((32,)), dma((8,)), dma((32,)), dma((8,)),
            ],
            compiler_params=pltpu.CompilerParams(collective_id=0, has_side_effects=True,
                                                 vmem_limit_bytes=67_000_000),
            name='head',
        )(hid_loc, norm_w, mask_loc, emb_loc, teach_loc)[:3]
        return o_dw[7, 0], o_dh, o_emb[:cols, :vloc].T, o_dw.reshape(-1)[:dim]

    return jax.shard_map(device_fn, mesh=mesh, in_specs=(P('dp', None), P(None), P('tp', None), P('dp', 'tp'), P('dp')),
                         out_specs=(P(), P('dp', None), P('tp', 'dp'), P(None)), check_vma=False)
```

```python
import functools

import jax
import jax.numpy as jnp
from jax import lax
from jax.experimental import pallas as pl
from jax.experimental.pallas import tpu as pltpu
from jax.sharding import PartitionSpec as P

SOFT_CAP = 30.0
NORM_EPS = 1e-6
SUB = 256
STRIP = 32
ODD = (1, 3)
CORES = (0, 1)
SLOTS = 3
MESH = pl.DeviceIdType.MESH
NT = (((1,), (1,)), ((), ()))
NN = (((1,), (0,)), ((), ()))


def col(v, j):
    return v[:, j:j + 1]


def halves(j):
    return j // 2, j % 2


def way_of(d):
    return 1 - 2 * d


def m8(o, j):
    return o * 8 + j


def m2(o, dc):
    return o * 2 + dc


def body(cfg, hid, nw, mask, emb, teach, o_emb, o_dh, o_dw, gbuf, e_1, e_a,
         t_stage, th_buf, t_recv, tb, e_slot, g_all, g_t, gin, dr_loc, r_blk, dr_blk,
         w1, r_a, r_b, e_b, mc_dp, m_buf, acc, st_tp, st_t, st_dp, st_all, dg_tp, dw_dp, xs_buf, gl_buf,
         tb_sem, es_sem, sub_sem, gl_sem, gin_sem, loc_sem, snd_s, rcv_s, t_rcv, de_snd, de_rcv, b_snd, b_rcv, e1_rcv, ea_rcv, eb_rcv, e1_snd, e2_snd, eb_snd,
         w1_rcv, ra_rcv, rb_rcv, s1_snd, sa_snd, s2_snd, sb_snd):
    tp_n, dp_n, ny = cfg
    tok, dim = hid.shape
    vloc = emb.shape[0]
    win = t_recv.shape[2]
    n_sub = win // SUB
    n_ch = t_stage.shape[1] // win
    tail = vloc - (n_ch - 1) * win
    chips = dp_n // 2
    nz = chips // ny
    rq = tok // tp_n
    cpad = o_emb.shape[0]
    cols = dim // dp_n
    last = n_ch - 1
    tail_n = -(-tail // SUB)
    tp_i = lax.axis_index('tp')
    dp_i = lax.axis_index('dp')
    chip = dp_i // 2
    core = dp_i % 2

    zc, yc = chip // ny, chip % ny
    a_c, b_c = zc + core * (yc - zc), yc + core * (zc - yc)
    sa, sb = ny - core * (ny - 1), 1 + core * (ny - 1)

    def dev_ab(oa, ob, dc):
        return 2 * (((a_c + oa + 4) % 4) * sa + ((b_c + ob + 4) % 4) * sb) + (core + dc) % 2

    def dev_a(oa):
        return dev_ab(oa, 0, 0)

    def dev_b(ob):
        return dev_ab(0, ob, 0)

    def peer(k):
        j = (k // 2 * 5) % chips
        return ((zc + j // ny) % nz * ny + (yc + j % ny) % ny) * 2 + (core + k % 2) % 2

    def active(dev, s):
        return dev * win + s * SUB < vloc

    def n_act(s):
        return sum(1 for d in range(dp_n) if d * win + s * SUB < vloc)

    sib = chip * 2 + (core + 1) % 2

    def push(src, dst, snd, rcv, dev, axis='dp'):
        return pltpu.make_async_remote_copy(src, dst, snd, rcv, device_id={axis: dev}, device_id_type=MESH)

    def got(ref, sem):
        push(ref, ref, gl_sem, sem, dp_i).wait_recv()

    def sent(ref, sem):
        push(ref, ref, sem, gl_sem, dp_i).wait_send()

    def to_plane(buf, ch):
        @pl.loop(1, dp_n)
        def _(k):
            push(buf.at[dp_i], buf.at[dp_i], snd_s.at[ch], rcv_s.at[ch], peer(k)).start()

    def to_tp(ref, ch):
        @pl.loop(1, tp_n)
        def _(k):
            push(ref, ref, snd_s.at[ch], rcv_s.at[ch], (tp_i + k) % tp_n, 'tp').start()

    def others(buf):
        return buf.at[pl.ds(0, buf.shape[0] - 1)]

    barrier = pltpu.get_barrier_semaphore()

    @pl.loop(1, dp_n)
    def _(k):
        pl.semaphore_signal(barrier, inc=1, device_id={'dp': peer(k)}, device_id_type=MESH)

    @pl.loop(1, tp_n)
    def _(k):
        pl.semaphore_signal(barrier, inc=1, device_id={'tp': (tp_i + k) % tp_n}, device_id_type=MESH)

    def tb_copy(r):
        return pltpu.make_async_copy(teach.at[pl.ds(r * 16, 16)], tb.at[r % 2], tb_sem.at[r % 2])

    tb_copy(0).start()
    tb_copy(1).start()

    def e_copy(i, slot, rows):
        return pltpu.make_async_copy(emb.at[pl.ds(pl.multiple_of(i * win, 16), rows)],
                                     e_slot.at[slot, pl.ds(0, rows)], es_sem.at[slot])

    def e_start(i):
        @pl.when(i < last)
        def _():
            e_copy(i, i % SLOTS, win).start()

        @pl.when(i == last)
        def _():
            e_copy(i, i % SLOTS, tail).start()

    def e_wait(i):
        @pl.when(i < last)
        def _():
            e_copy(i, i % SLOTS, win).wait()

        @pl.when(i == last)
        def _():
            e_copy(i, i % SLOTS, tail).wait()

    def sub_copy(rows):
        return pltpu.make_async_copy(emb.at[pl.ds(pl.multiple_of(dp_i * win, 16), rows)],
                                     e_slot.at[0, pl.ds(0, rows)], sub_sem)

    x = hid[...].astype(jnp.float32)
    scale = 1.0 + nw[...].astype(jnp.float32).reshape(1, dim)
    inv = lax.rsqrt(jnp.mean(x * x, axis=-1, keepdims=True) + NORM_EPS)
    xs = x * inv
    xs_buf[...] = xs.reshape(tp_n, rq, dim)
    gl_buf[...] = (xs * scale).astype(jnp.bfloat16)

    own_g = pltpu.make_async_copy(xs_buf.at[tp_i], gbuf.at[chip, core, tp_i], gl_sem)
    own_g.start()

    diag = lax.broadcasted_iota(jnp.int32, (tok, tok), 0) == lax.broadcasted_iota(jnp.int32, (tok, tok), 1)
    m_row = mask[...].astype(jnp.float32).reshape(1, tok)
    m_loc = jnp.sum(jnp.where(diag, m_row, 0.0), axis=-1, keepdims=True)
    mc_dp[dp_i] = jnp.broadcast_to(jnp.sum(m_loc, axis=0, keepdims=True), (8, 128))
    pieces = [(c0, min(1024, vloc - c0)) for c0 in range(0, vloc, 1024)]
    full_p = vloc // 1024

    t_stage[:, pl.ds(vloc // 128 * 128, n_ch * win - vloc // 128 * 128)] = jnp.zeros(
        (tok, n_ch * win - vloc // 128 * 128), jnp.float32)
    for r in range(tok // 16):
        tb_copy(r).wait()
        rows = pl.ds(r * 16, 16)

        def conv(c0, width, mx):
            v = tb[r % 2, :, pl.ds(c0, width)].astype(jnp.float32)
            t_stage[rows, pl.ds(c0, width)] = v
            return v

        def step(i, mx):
            v = conv(pl.multiple_of(i * 1024, 128), 1024, mx)
            for q in range(8):
                mx = jnp.maximum(mx, v[:, q * 128:(q + 1) * 128])
            return mx

        mx = lax.fori_loop(0, full_p, step, jnp.full((16, 128), -jnp.inf, jnp.float32))
        m1 = jnp.max(mx, axis=-1, keepdims=True)
        if full_p * 1024 < vloc:
            v = conv(full_p * 1024, vloc - full_p * 1024, None)
            m1 = jnp.maximum(m1, jnp.max(v, axis=-1, keepdims=True))
        m_buf[rows, :] = jnp.broadcast_to(m1, (16, 128))
        if r + 2 < tok // 16:
            tb_copy(r + 2).start()

    for i in range(SLOTS):
        e_start(i)

    pl.semaphore_wait(barrier, dp_n - 1 + tp_n - 1)

    @pl.loop(1, chips)
    def _(k):
        push(xs_buf.at[tp_i], gbuf.at[chip, core, tp_i], snd_s.at[0], rcv_s.at[0], peer(2 * k)).start()


    to_plane(mc_dp, 7)

    def t_win(dev):
        return t_stage.at[:, pl.ds(pl.multiple_of(dev * win, 128), win)]

    def two_first(j):
        dest = dev_ab(2, *halves(j))
        hop = dev_a(way_of(j // 4))
        pl.when(dest <= last)(lambda: push(t_win(dest), r_a.at[j], s1_snd.at[16 + j], ra_rcv.at[j], hop).start())

    def one_first(o, j):
        dest = dev_ab(o, *halves(j))

        @pl.when(dest <= last)
        def _():
            pl.when(j < 2)(lambda: push(t_win(dest), t_recv.at[dp_i], s1_snd.at[m8(o, j)], t_rcv, dest).start())
            pl.when(j >= 2)(lambda: push(t_win(dest), w1.at[o - 1, j - 2], s1_snd.at[m8(o, j)], w1_rcv.at[m8(o, j)],
                                         dev_a(o)).start())

    def two_second(j):
        sign = way_of(j // 4)
        dest = dev_ab(sign, *halves(j))

        @pl.when(dest <= last)
        def _():
            got(r_a.at[j], ra_rcv.at[j])
            pl.when(j < 2)(lambda: push(r_a.at[j], t_recv.at[dev_a(-sign)], sa_snd.at[j], t_rcv, dest).start())
            pl.when(j >= 2)(lambda: push(r_a.at[j], w1.at[1, j - 2], sa_snd.at[j], w1_rcv.at[16 + j],
                                         dev_a(sign)).start())

    def across(o, j):
        db, dc = halves(j)
        dest = dev_ab(0, db, dc)

        @pl.when(dest <= last)
        def _():
            if o == 0:
                src = t_win(dest)
            else:
                src = w1.at[o - 1, j - 2]
                got(src, w1_rcv.at[m8(o, j)])
            pl.when(db != 2)(lambda: push(src, t_recv.at[dev_a(-o)], s2_snd.at[m8(o, j)], t_rcv, dest).start())
            pl.when(db == 2)(lambda: push(src, r_b.at[m2(o, dc)], s2_snd.at[m8(o, j)], rb_rcv.at[m2(o, dc)],
                                          dev_b(way_of(dc))).start())

    def across_second(o, dc):
        sign = way_of(dc)
        dest = dev_ab(0, sign, dc)

        @pl.when(dest <= last)
        def _():
            got(r_b.at[m2(o, dc)], rb_rcv.at[m2(o, dc)])
            push(r_b.at[m2(o, dc)], t_recv.at[dev_ab(-o, -sign, 0)], sb_snd.at[m2(o, dc)], t_rcv, dest).start()

    def turn(o):
        @pl.loop(2, 8)
        def _(j):
            across(o, j)

    def turn_second(o):
        for dc in CORES:
            across_second(o, dc)

    @pl.loop(0, 4)
    def _(j):
        two_first(j)
        two_first(j + 4)

    pl.when(sib <= last)(lambda: push(t_win(sib), t_recv.at[dp_i], s1_snd.at[1], t_rcv, sib).start())

    @pl.when(dp_i <= last)
    def _():
        t_recv[dp_i] = t_stage[:, pl.ds(pl.multiple_of(dp_i * win, 128), win)]

    a_part = gbuf.at[pl.ds(0, chips - 1), 0, 0]
    up, down = (tp_i + 1) % tp_n, (tp_i + tp_n - 1) % tp_n
    half = chips // 2

    def rows_first():
        own_g.wait()
        got(a_part, rcv_s.at[0])
        own = gbuf.at[:, core, tp_i]
        push(own, own, b_snd.at[0], b_rcv.at[0], up, 'tp').start()
        push(own, own, b_snd.at[1], b_rcv.at[1], down, 'tp').start()

    def rows_second():
        for way in CORES:
            got(gbuf.at[:, 0, 0], b_rcv.at[way])
        lo, hi = gbuf.at[pl.ds(0, half), core, down], gbuf.at[pl.ds(half, half), core, up]
        push(lo, lo, b_snd.at[2], b_rcv.at[2], up, 'tp').start()
        push(hi, hi, b_snd.at[3], b_rcv.at[3], down, 'tp').start()

    b_half = gbuf.at[pl.ds(0, half), 0, 0]

    def rows_sibling():
        for way in CORES:
            got(b_half, b_rcv.at[2 + way])
        gc_copy.start()

    gc_copy = push(gbuf.at[:, core], gbuf.at[:, core], snd_s.at[3], rcv_s.at[3], sib)

    acc[...] = jnp.zeros_like(acc)
    lanes = lax.broadcasted_iota(jnp.int32, (tok, 128), 1)

    @pl.loop(0, n_ch)
    def _(i):
        pl.when(i == n_ch // 4)(rows_first)

        @pl.when(i % 3 + i // 24 * 3 == 0)
        def _():
            for o in ODD:
                one_first(o, i // 3)

        e_wait(i)
        base = pl.multiple_of(i * win, 128)
        own = pl.ds(pl.multiple_of(i * tok, tok), tok)
        th_buf[own, :] = lax.dot_general(gl_buf[...], e_slot[i % SLOTS], NT,
                                                      preferred_element_type=jnp.float32)

        @pl.when(i + SLOTS < n_ch)
        def _():
            e_start(i + SLOTS)

        m_l = m_buf[...]
        a_s, a_1, a_2, a_x = acc[0], acc[1], acc[2], acc[3]
        for q in range(win // 128):
            at = pl.ds(pl.multiple_of(base + q * 128, 128), 128)
            part = pl.ds(q * 128, 128)
            th = jnp.tanh(th_buf[own, part] * (1.0 / SOFT_CAP))
            th_buf[own, part] = th
            z = SOFT_CAP * th
            ok = base + q * 128 + lanes < vloc
            e_s = jnp.where(ok, jnp.exp(z), 0.0)
            sh = t_stage[:, at] - m_l
            e_t = jnp.where(ok, jnp.exp(sh), 0.0)
            sh = jnp.where(ok, sh, 0.0)
            a_s = a_s + e_s
            a_1 = a_1 + e_t
            a_2 = a_2 + e_t * sh
            a_x = a_x + e_t * jnp.where(ok, z, 0.0)
        acc[0] = a_s
        acc[1] = a_1
        acc[2] = a_2
        acc[3] = a_x

    for i in range(SLOTS):
        e_start(i)

    parts = [col(m_buf, 0)] + [jnp.sum(acc[j], axis=-1, keepdims=True) for j in (1, 2, 3, 0)]
    tile = jnp.zeros((tok, 128), jnp.float32)
    for j, v in enumerate(parts):
        tile = jnp.where(lanes == j, v, tile)
    st_tp[tp_i] = tile

    to_tp(st_tp.at[tp_i], 2)
    got(others(st_tp), rcv_s.at[2])
    t_max = col(st_tp[0], 0)
    for q in range(1, tp_n):
        t_max = jnp.maximum(t_max, col(st_tp[q], 0))
    s_1 = s_2 = s_x = s_s = jnp.zeros((tok, 1), jnp.float32)
    for q in range(tp_n):
        v = st_tp[q]
        shift = col(v, 0) - t_max
        fac = jnp.exp(shift)
        s_1 = s_1 + fac * col(v, 1)
        s_2 = s_2 + fac * (col(v, 2) + shift * col(v, 1))
        s_x = s_x + fac * col(v, 3)
        s_s = s_s + col(v, 4)
    log_1 = jnp.log(s_1)
    kl = (s_2 - s_x) / s_1 - log_1 + jnp.log(s_s)
    lse_t = t_max + log_1
    inv_s = 1.0 / s_s
    tile = jnp.where(lanes == 0, lse_t, jnp.where(lanes == 1, inv_s, jnp.where(lanes == 2, m_loc, 0.0)))
    tile = jnp.concatenate([tile, jnp.zeros((128 - tok, 128), jnp.float32)], axis=0).T
    st_dp[dp_i] = tile[0:8]

    to_plane(st_dp, 4)

    rows_second()

    @pl.loop(0, 8)
    def _(j):
        two_second(j)

    turn(0)

    got(others(mc_dp), rcv_s.at[7])
    m_cnt = jnp.sum(mc_dp[...], axis=0)[0:1, 0:1]
    w_loc = m_loc / m_cnt

    dg_tp[tp_i] = jnp.zeros((tok, dim), jnp.float32)

    @pl.loop(0, n_ch)
    def _(i):
        pl.when(i == n_ch // 3)(rows_sibling)
        pl.when(i == n_ch // 2)(lambda: turn(1))
        pl.when(i == n_ch * 2 // 3)(lambda: turn(3))
        e_wait(i)
        base = pl.multiple_of(i * win, 128)
        own = pl.ds(pl.multiple_of(i * tok, tok), tok)
        for q in range(win // 128):
            at = pl.ds(pl.multiple_of(base + q * 128, 128), 128)
            part = pl.ds(q * 128, 128)
            th = th_buf[own, part]
            p_s = jnp.exp(SOFT_CAP * th) * inv_s
            p_t = jnp.exp(t_stage[:, at] - lse_t)
            d = (p_s - p_t) * w_loc * (1.0 - th * th)
            ok = base + q * 128 + lanes < vloc
            dr_loc[:, part] = jnp.where(ok, d, 0.0).astype(jnp.bfloat16)
        dg_tp[tp_i] += lax.dot_general(dr_loc[...], e_slot[i % SLOTS], NN, preferred_element_type=jnp.float32)

        @pl.when(i + SLOTS < n_ch)
        def _():
            e_start(i + SLOTS)

    @pl.when(dp_i < last)
    def _():
        sub_copy(win).start()

    @pl.when(dp_i == last)
    def _():
        sub_copy(tail).start()

    to_tp(dg_tp.at[tp_i], 5)

    turn(2)
    turn_second(0)

    gc_copy.wait()

    def gin_copy(d):
        return pltpu.make_async_copy(gbuf.at[d // 2, d % 2], gin.at[d % 4], gin_sem.at[d % 4])

    for d in range(min(4, dp_n)):
        gin_copy(d).start()

    for d in range(dp_n):
        gin_copy(d).wait()
        gv = (gin[d % 4].reshape(tok, dim) * scale)
        g_all[pl.ds(d * tok, tok), :] = gv.astype(jnp.bfloat16)
        if d + 4 < dp_n:
            gin_copy(d + 4).start()

    for d in range(0, dp_n, 2):
        gv = g_all[pl.ds(d * tok, 2 * tok), :].astype(jnp.float32).T
        for c in range(dp_n):
            gc = gv[c * cols:(c + 1) * cols]
            if cpad != cols:
                gc = jnp.concatenate([gc, jnp.zeros((cpad - cols, 2 * tok), jnp.float32)], axis=0)
            g_t[pl.ds(c * cpad, cpad), pl.ds(d * tok, 2 * tok)] = gc.astype(jnp.bfloat16)

    for o in ODD:
        turn_second(o)

    got(others(dg_tp), rcv_s.at[5])
    dg = dg_tp[0]
    for q in range(1, tp_n):
        dg = dg + dg_tp[q]
    x = hid[...].astype(jnp.float32)
    inv = lax.rsqrt(jnp.mean(x * x, axis=-1, keepdims=True) + NORM_EPS)
    dxs = dg * scale
    o_dh[...] = (inv * dxs - x * (inv * inv * inv * (jnp.sum(dxs * x, axis=-1, keepdims=True) / dim))).astype(jnp.bfloat16)
    dw = jnp.sum(dg * (x * inv), axis=0, keepdims=True)
    dw_dp[dp_i] = jnp.broadcast_to(jnp.sum(w_loc * kl, axis=0, keepdims=True), (8, 128))
    for j in range(dim // 128):
        dw_dp[dp_i, pl.ds(j, 1), :] = dw[:, j * 128:(j + 1) * 128]

    to_plane(dw_dp, 6)

    got(others(st_dp), rcv_s.at[4])

    @pl.loop(0, dp_n)
    def _(d):
        v = jnp.concatenate([st_dp[d], jnp.zeros((120, 128), jnp.float32)], axis=0).T
        st_all[d] = v[0:tok]

    turn_second(2)

    @pl.when(dp_i < last)
    def _():
        sub_copy(win).wait()

    @pl.when(dp_i == last)
    def _():
        sub_copy(tail).wait()

    row_n = 4 * tok

    def de_src(dev, s):
        return th_buf.at[pl.ds(pl.multiple_of(dev * cpad, 8), cpad), pl.ds(s * SUB, SUB)]

    def de_dst(origin, s):
        return o_emb.at[:, pl.ds(pl.multiple_of(origin * win + s * SUB, 128), SUB)]

    def de_local(s):
        return pltpu.make_async_copy(de_src(dp_i, s), de_dst(dp_i, s), loc_sem.at[s])

    def de_first(s):
        snd = de_snd.at[s]

        @pl.loop(0, 4)
        def _(j):
            for way in CORES:
                dest = dev_ab(2, *halves(j + 4 * way))
                push(de_src(dest, s), e_a.at[way, s, j], snd, ea_rcv.at[way, s], dev_a(way_of(way))).start()

        @pl.loop(0, 8)
        def _(j):
            for o in ODD:
                dest = dev_ab(o, *halves(j))
                src = de_src(dest, s)
                pl.when(j < 2)(lambda: push(src, de_dst(dp_i, s), snd, de_rcv, dest).start())
                pl.when(j >= 2)(lambda: push(src, e_1.at[o, s, j - 2], snd, e1_rcv.at[o, s], dev_a(o)).start())

        push(de_src(sib, s), de_dst(dp_i, s), snd, de_rcv, sib).start()
        de_turn(0, s, snd)
        de_local(s).start()

    def de_turn(o, s, snd):
        @pl.loop(2, 8)
        def _(j):
            db, dc = halves(j)
            dest = dev_ab(0, db, dc)
            src = e_1.at[o, s, j - 2] if o else de_src(dest, s)
            pl.when(db != 2)(lambda: push(src, de_dst(dev_a(-o), s), snd, de_rcv, dest).start())
            pl.when(db == 2)(lambda: push(src, e_b.at[o, dc, s], snd, eb_rcv.at[o, dc, s],
                                          dev_b(way_of(dc))).start())

    def de_two(s):
        for way in CORES:
            sign = way_of(way)
            origin = dev_a(-sign)

            @pl.when(active(origin, s))
            def _():
                got(e_a.at[way, s], ea_rcv.at[way, s])

                @pl.loop(0, 4)
                def _(j):
                    jj = j + 4 * way
                    dest = dev_ab(sign, *halves(jj))
                    src, snd = e_a.at[way, s, j], e2_snd.at[way]
                    pl.when(jj < 2)(lambda: push(src, de_dst(origin, s), snd, de_rcv, dest).start())
                    pl.when(jj >= 2)(lambda: push(src, e_1.at[2, s, jj - 2], snd, e1_rcv.at[2, s],
                                                  dev_a(sign)).start())

    def de_across(o, s):
        @pl.when(active(dev_a(-o), s))
        def _():
            got(e_1.at[o, s], e1_rcv.at[o, s])
            de_turn(o, s, e1_snd.at[o])

    def de_last(o, s):
        for dc in CORES:
            sign = way_of(dc)
            origin = dev_ab(-o, -sign, 0)

            @pl.when(active(origin, s))
            def _():
                src = e_b.at[o, dc, s]
                got(src, eb_rcv.at[o, dc, s])
                push(src, de_dst(origin, s), eb_snd.at[o, dc], de_rcv, dev_ab(0, sign, dc)).start()

    def de_step(k):
        def run(f, s, *o):
            if 0 <= s < n_sub:
                f(*o, s)

        run(de_two, k - 1)
        run(de_across, k - 1, 1)
        run(de_across, k - 1, 3)
        run(de_across, k - 2, 2)
        for o in (0, 1, 3):
            run(de_last, k - 2, o)
        run(de_last, k - 3, 2)

    def de_wait(s):
        @pl.when(active(dp_i, s))
        def _():
            sent(th_buf.at[pl.ds(0, (dp_n - 1) * cpad), pl.ds(0, SUB)], de_snd.at[s])
            de_local(s).wait()

    pl.when(dp_i <= last)(lambda: got(t_recv.at[pl.ds(0, dp_n - 1)], t_rcv))

    for s in range(n_sub):
        @pl.when(active(dp_i, s))
        def _(s=s):
            @pl.loop(0, dp_n // 4)
            def _(b):
                rows = pl.ds(pl.multiple_of(b * row_n, row_n), row_n)
                r_blk[...] = lax.dot_general(g_all[rows, :], e_slot[0, pl.ds(s * SUB, SUB), :], NT,
                                             preferred_element_type=jnp.float32)
                for q in range(row_n // STRIP):
                    d = b * 4 + q * STRIP // tok
                    off = q * STRIP % tok
                    th = jnp.tanh(r_blk[pl.ds(q * STRIP, STRIP), :] * (1.0 / SOFT_CAP))
                    sv = st_all[d, pl.ds(off, STRIP), :]
                    p_s = jnp.exp(SOFT_CAP * th) * col(sv, 1)
                    p_t = jnp.exp(t_recv[d, pl.ds(off, STRIP), pl.ds(s * SUB, SUB)] - col(sv, 0))
                    dv = (p_s - p_t) * (col(sv, 2) / m_cnt) * (1.0 - th * th)
                    dr_blk[pl.ds(pl.multiple_of(b * row_n + q * STRIP, STRIP), STRIP), :] = dv.astype(jnp.bfloat16)

            @pl.loop(0, dp_n * cpad // 256)
            def _(b):
                rows = pl.ds(pl.multiple_of(b * 256, 256), 256)
                th_buf[rows, pl.ds(s * SUB, SUB)] = lax.dot_general(g_t[rows, :], dr_blk[...], NN,
                                                        preferred_element_type=jnp.float32)

            de_first(s)

        de_step(s)

    for s in range(n_sub, n_sub + 3):
        de_step(s)

    got(others(dw_dp), rcv_s.at[6])
    tot = dw_dp[0]
    for d in range(1, dp_n):
        tot = tot + dw_dp[d]
    o_dw[...] = tot

    sent(a_part, snd_s.at[0])
    for way in CORES:
        sent(gbuf.at[:, 0, 0], b_snd.at[way])
        sent(b_half, b_snd.at[2 + way])
    for buf, ch in ((st_tp, 2), (st_dp, 4), (dg_tp, 5), (dw_dp, 6), (mc_dp, 7)):
        sent(others(buf), snd_s.at[ch])

    one = t_recv.at[0]

    @pl.loop(0, 8)
    def _(j):
        for o in (1, 2, 3):
            pl.when(dev_ab(o, *halves(j)) <= last)(lambda o=o: sent(one, s1_snd.at[m8(o, j)]))
        pl.when(dev_ab(way_of(j // 4), *halves(j)) <= last)(lambda: sent(one, sa_snd.at[j]))

    pl.when(sib <= last)(lambda: sent(one, s1_snd.at[1]))

    @pl.loop(2, 8)
    def _(j):
        for o in range(4):
            pl.when(dev_ab(0, *halves(j)) <= last)(lambda o=o: sent(one, s2_snd.at[m8(o, j)]))

    for o in range(4):
        for dc in CORES:
            pl.when(dev_ab(0, way_of(dc), dc) <= last)(lambda o=o, dc=dc: sent(one, sb_snd.at[m2(o, dc)]))

    def e_sent(origin, part, sem):
        pl.when(origin < last)(lambda: sent(part(n_sub), sem))
        pl.when(origin == last)(lambda: sent(part(tail_n), sem))

    for way in CORES:
        e_sent(dev_ab(2 * way - 1, 0, 0), lambda n, way=way: e_a.at[way, pl.ds(0, n)], e2_snd.at[way])
    for o in range(4):
        if o:
            e_sent(dev_a(-o), lambda n, o=o: e_1.at[o, pl.ds(0, n)], e1_snd.at[o])
        for dc in CORES:
            e_sent(dev_ab(-o, 2 * dc - 1, 0), lambda n, o=o, dc=dc: e_b.at[o, dc, pl.ds(0, n)], eb_snd.at[o, dc])

    for s in range(n_sub):
        de_wait(s)

    total = sum(n_act(s) for s in range(n_sub))

    def de_drain(n):
        got(o_emb.at[:, pl.ds(0, n * SUB)], de_rcv)

    @pl.when(dp_i < last)
    def _():
        de_drain(total - n_sub)

    @pl.when(dp_i == last)
    def _():
        de_drain(total - tail_n)

    @pl.when(dp_i > last)
    def _():
        de_drain(total)


def solution(mesh):
    tp_n, dp_n = mesh.shape['tp'], mesh.shape['dp']
    ny = 4 if dp_n >= 32 else 1

    def device_fn(hid_loc, norm_w, emb_loc, teach_loc, mask_loc):
        tok, dim = hid_loc.shape
        vloc = emb_loc.shape[0]
        win = -(-vloc // (dp_n * 128)) * 128
        n_ch = -(-vloc // win)
        cols = dim // dp_n
        cpad = -(-cols // 8) * 8
        rq = tok // tp_n
        f32, bf16 = jnp.float32, jnp.bfloat16
        vm, dma = pltpu.VMEM, pltpu.SemaphoreType.DMA
        any_s, vm_s = pl.BlockSpec(memory_space=pl.ANY), pl.BlockSpec(memory_space=pltpu.VMEM)
        wide = n_ch * win
        n_sub = win // SUB
        o_emb, o_dh, o_dw = pl.pallas_call(
            functools.partial(body, (tp_n, dp_n, ny)),
            out_shape=(jax.ShapeDtypeStruct((cpad, wide), f32), jax.ShapeDtypeStruct((tok, dim), bf16),
                       jax.ShapeDtypeStruct((8, 128), f32),
                       jax.ShapeDtypeStruct((dp_n // 2, 2, tp_n, rq, dim), f32),
                       jax.ShapeDtypeStruct((4, n_sub, 6, cpad, SUB), f32),
                       jax.ShapeDtypeStruct((2, n_sub, 4, cpad, SUB), f32)),
            in_specs=[vm_s, vm_s, vm_s, any_s, any_s],
            out_specs=(any_s, vm_s, vm_s, any_s, any_s, any_s),
            scratch_shapes=[
                vm((tok, wide), f32), vm((n_ch * tok, win), f32), vm((dp_n, tok, win), f32), vm((2, 16, vloc), bf16),
                vm((SLOTS, win, dim), bf16), vm((dp_n * tok, dim), bf16),
                vm((dp_n * cpad, dp_n * tok), bf16), vm((4, tp_n, rq, dim), f32), vm((tok, win), bf16),
                vm((4 * tok, SUB), f32), vm((dp_n * tok, SUB), bf16),
                vm((3, 6, tok, win), f32), vm((8, tok, win), f32), vm((8, tok, win), f32),
                vm((4, 2, n_sub, cpad, SUB), f32), vm((dp_n, 8, 128), f32),
                vm((tok, 128), f32), vm((4, tok, 128), f32), vm((tp_n, tok, 128), f32), vm((8, 128), f32),
                vm((dp_n, 8, 128), f32), vm((dp_n, tok, 128), f32), vm((tp_n, tok, dim), f32),
                vm((dp_n, 8, 128), f32), vm((tp_n, rq, dim), f32), vm((tok, dim), bf16),
                dma((2,)), dma((SLOTS,)), dma, dma, dma((4,)), dma((n_sub,)), dma((8,)), dma((8,)),
                dma, dma((n_sub,)), dma, dma((4,)), dma((4,)), dma((4, n_sub)), dma((2, n_sub)), dma((4, 2, n_sub)), dma((4,)), dma((2,)),
                dma((4, 2)),
                dma((32,)), dma((8,)), dma((8,)), dma((32,)), dma((8,)), dma((32,)), dma((8,)),
            ],
            compiler_params=pltpu.CompilerParams(collective_id=0, has_side_effects=True,
                                                 vmem_limit_bytes=67_000_000),
            name='head',
        )(hid_loc, norm_w, mask_loc, emb_loc, teach_loc)[:3]
        return o_dw[7, 0], o_dh, o_emb[:cols, :vloc].T, o_dw.reshape(-1)[:dim]

    return jax.shard_map(device_fn, mesh=mesh, in_specs=(P('dp', None), P(None), P('tp', None), P('dp', 'tp'), P('dp')),
                         out_specs=(P(), P('dp', None), P('tp', 'dp'), P(None)), check_vma=False)
```
